32 devices in a mesh: groups: 2 (over x), mp: 8 (over z, y), psg: 2 (over core).
Axes of the slice: x: 2, y: 2, z: 4, core: 2. Of those that a mesh axis runs over, the one named last changes fastest.
Arguments:
- tokens: bfloat16 [512, 1024], P(('groups', 'mp', 'psg')), parts along dimension 0, may hold values from -6 to 6
- enc_gain: float32 [1024], replicated, may hold values from 0.25 to 1.75
- w_in: bfloat16 [1024, 32768], P(None, 'mp'), may hold values from -0.1875 to 0.1875
- w_out: bfloat16 [32768, 1024], P('mp'), may hold values from -0.046875 to 0.046875
- final_gain: float32 [1024], replicated, may hold values from 0.25 to 1.75
- w_keyval: bfloat16 [1024, 2, 16384], P(None, None, 'mp'), may hold values from -0.1875 to 0.1875
- answer_states: bfloat16 [256, 1024], P('groups'), parts along dimension 0, may hold values from -6 to 6
- dec_gain: float32 [1024], replicated, may hold values from 0.25 to 1.75
- w_query: bfloat16 [1024, 16384], P(None, 'mp')
- w_attn_out: bfloat16 [16384, 1024], P('mp'), may hold values from -0.046875 to 0.046875
- passage_lengths: int32 [32], P('groups'), parts along dimension 0, may hold values from 1 to 16
- passage_owner: int32 [32], P('groups'), parts along dimension 0, may hold values from 0 to 3, as said below
- answer_lengths: int32 [8], P('groups'), parts along dimension 0, may hold values from 1 to 64, 128 in all
Outputs:
- encoded: bfloat16 [512, 1024], P(('groups', 'mp', 'psg')), parts along dimension 0
- answer: bfloat16 [256, 1024], P(('groups', 'mp')), parts along dimension 0
The draws below stay inside these ranges and needn't reach their ends.
There are 2 independent parts, one for each index of `groups`. The reference program is written for one: setup_inputs(seed, part) draws one part's arguments, and reference() takes and returns one part's arrays. A program takes and returns all parts, laid end to end along the dimension named above; an argument that names none is the same for every part. Nothing has to cross between parts.
Inputs may be any that keep to these rules, and one draw needn't show every extreme that they name: `passage_owner`: every one of the 4 questions owns at least one passage.
All inputs are finite; a program needn't handle non-finite values.
Results may differ from the reference program's by a relative error of at most 0.028.
Values may be sent and summed in bfloat16 or wider, within the bound.
No kernel may reach another device: no remote copies, remote signals or barrier semaphores. Data moves between devices by JAX's collectives and lax.ppermute only.
A program may use at most 128 MiB of HBM per device.

```python
import math
import jax
import jax.numpy as jnp
import numpy as np
from jax import lax

D = 1024
FF = 32768
HEADS = 128
DH = 128
P_SLOT = 16
NQ = 4
ANS = 128
INNER = 16384
TOKENS = 256
NPASS = 16


def draw_w_query(key, part):
    base_key = jax.random.fold_in(jax.random.fold_in(key, 11), 0)
    base = jax.random.normal(base_key, (D, INNER), jnp.float32)
    return (base * D ** (-0.5)).astype(jnp.bfloat16)


def draw_passage_owner(key, part):
    count = TOKENS // P_SLOT
    owner_key, order_key = jax.random.split(jax.random.fold_in(key, 7))
    owners = jax.random.randint(owner_key, (count,), 0, NQ, dtype=jnp.int32)
    order = jax.random.permutation(order_key, count)
    owners = owners.at[order[:NQ]].set(jnp.arange(NQ, dtype=jnp.int32))
    return owners


def touch_ends(drawn, stream_key, smallest, top_value):
    index_at = [jax.random.randint(jax.random.fold_in(stream_key, axis), (), 0, length) for axis, length in enumerate(drawn.shape)]
    longest = drawn.shape.index(max(drawn.shape))
    next_to = index_at[:longest] + [(index_at[longest] + 1) % drawn.shape[longest]] + index_at[longest + 1:]
    return drawn.at[tuple(index_at)].set(smallest).at[tuple(next_to)].set(top_value)


def shard_levels(key, extent, cuts, low, largest):
    def one(axis_at, shards_of):
        draws = jax.random.uniform(jax.random.fold_in(jax.random.fold_in(key, 6), axis_at), (shards_of,), jnp.float32, low / len(cuts), largest / len(cuts))
        return jnp.repeat(jnp.exp(draws), extent[axis_at] // shards_of).reshape((-1,) + (1,) * (len(extent) - axis_at - 1))

    level = one(*cuts[0])
    for cut in cuts[1:]:
        level = level * one(*cut)
    return level


def split_up(count, total, most, skew):
    loads = [(1 << 20) // math.isqrt(standing ** skew) + 1 for standing in range(2, count + 1)]
    rest, given = total - most - (count - 1), [1] * (count - 1)
    while rest > 0:
        free = [i for i in range(count - 1) if given[i] < most]
        pool, remaining = sum([loads[i] for i in free]), rest
        for i in free:
            more = min(most - given[i], max(1, remaining * loads[i] // pool), rest)
            given[i] = given[i] + more
            rest = rest - more
    return np.array([most] + given)


def ragged(own_key, count, total, most, slope):
    if count == 2:
        one = jax.random.randint(own_key, (), max(1, total - most), min(most, total - 1) + 1)
        return jnp.stack([one, total - one])
    lengths = jnp.asarray(split_up(count, total, most, slope), jnp.int32)
    couples = (count - 1) // 2
    donor, taker = lengths[1:1 + 2 * couples:2], lengths[2:2 + 2 * couples:2]
    slack = jnp.minimum(donor - 1, most - taker)
    passed = jax.random.randint(jax.random.fold_in(own_key, 1), (couples,), 0, 1 << 20) % (slack + 1)
    lengths = lengths.at[1:1 + 2 * couples:2].set(donor - passed).at[2:2 + 2 * couples:2].set(taker + passed)
    return lengths[jax.random.permutation(jax.random.fold_in(own_key, 2), count)]


def bell_draw(key, shape, width, limit, shards=(), held_as=jnp.bfloat16):
    drawn = width * jax.random.normal(key, shape, jnp.float32)
    if shards:
        drawn = drawn * shard_levels(key, shape, shards, -0.22, 0.18)
    return jnp.clip(drawn, -limit, limit).astype(held_as)


def setup_inputs(seed: int = 0, part: int = 0) -> dict:
    key_list = jax.random.split(jax.random.key(seed), 14)
    own_keys = jax.random.split(jax.random.fold_in(key_list[13], part), 14)
    tokens = bell_draw(own_keys[0], (TOKENS, D), 1.0, 6.0, ((0, 16),))
    enc_gain = jnp.clip(1.0 + 0.15 * jax.random.normal(key_list[1], (D,), jnp.float32), 0.25, 1.75)
    w_in = bell_draw(key_list[2], (D, FF), D ** -0.5, 0.1875, ((1, 8),))
    w_out = bell_draw(key_list[3], (FF, D), (FF // 2) ** -0.5, 0.046875, ((0, 8),))
    final_gain = jnp.clip(1.0 + 0.15 * jax.random.normal(key_list[4], (D,), jnp.float32), 0.25, 1.75)
    w_keyval = bell_draw(key_list[5], (D, 2, INNER), D ** -0.5, 0.1875, ((2, 8),))
    answer_states = bell_draw(own_keys[6], (ANS, D), 1.0, 6.0)
    dec_gain = jnp.clip(1.0 + 0.15 * jax.random.normal(key_list[7], (D,), jnp.float32), 0.25, 1.75)
    w_query = draw_w_query(jax.random.fold_in(key_list[13], 71), part)
    w_attn_out = bell_draw(key_list[9], (INNER, D), INNER ** -0.5, 0.046875, ((0, 8),))
    passage_lengths = touch_ends(jax.random.randint(own_keys[10], (NPASS,), 1, P_SLOT + 1), jax.random.fold_in(own_keys[10], 1), 1, P_SLOT).astype(jnp.int32)
    passage_owner = draw_passage_owner(jax.random.fold_in(jax.random.fold_in(key_list[13], part), 71), part)
    answer_lengths = ragged(own_keys[12], NQ, ANS, ANS // 2, 1).astype(jnp.int32)
    return dict(tokens=tokens, enc_gain=enc_gain, w_in=w_in, w_out=w_out, final_gain=final_gain, w_keyval=w_keyval, answer_states=answer_states, dec_gain=dec_gain, w_query=w_query, w_attn_out=w_attn_out, passage_lengths=passage_lengths, passage_owner=passage_owner, answer_lengths=answer_lengths)


eps = 1e-06

def norm_rows(states, gain):
    wide = states.astype(jnp.float32)
    factor = lax.rsqrt(lax.optimization_barrier(jnp.mean(wide * wide, axis=-1, keepdims=True)) + eps)
    return wide * factor * gain

def key_mask(token_index, passage_lengths, passage_owner, answer_lengths, answer_count):
    passage = token_index // P_SLOT
    place = token_index % P_SLOT
    count = passage_lengths.shape[0]
    match = passage[:, None] == jnp.arange(count, dtype=jnp.int32)[None, :]
    token_length = lax.optimization_barrier(jnp.sum(jnp.where(match, passage_lengths[None, :], 0), axis=1))
    token_owner = lax.optimization_barrier(jnp.sum(jnp.where(match, passage_owner[None, :], 0), axis=1))
    ends = jnp.cumsum(answer_lengths).astype(jnp.int32)
    answer_index = jnp.arange(answer_count, dtype=jnp.int32)
    question = lax.optimization_barrier(jnp.sum((answer_index[:, None] >= ends[None, :]).astype(jnp.int32), axis=1))
    return (place < token_length)[None, :] & (token_owner[None, :] == question[:, None])

def reference(tokens, enc_gain, w_in, w_out, final_gain, w_keyval, answer_states, dec_gain, w_query, w_attn_out, passage_lengths, passage_owner, answer_lengths):
    normed = norm_rows(tokens, enc_gain).astype(jnp.bfloat16)
    blocks = normed.reshape(TOKENS // P_SLOT, P_SLOT, D)

    def feed(block):
        hidden = jnp.maximum(jnp.dot(block, w_in, preferred_element_type=jnp.float32), 0.0).astype(jnp.bfloat16)
        return jnp.dot(hidden, w_out, preferred_element_type=jnp.float32)
    ffn = lax.map(feed, blocks).reshape(TOKENS, D)
    encoded = (tokens.astype(jnp.float32) + ffn).astype(jnp.bfloat16)
    memory = norm_rows(encoded, final_gain).astype(jnp.bfloat16)
    joined = jnp.dot(memory, w_keyval.reshape(D, 2 * INNER), preferred_element_type=jnp.float32).astype(jnp.bfloat16)
    keys = joined[:, :INNER].reshape(TOKENS, HEADS, DH).transpose(1, 0, 2)
    values = joined[:, INNER:].reshape(TOKENS, HEADS, DH).transpose(1, 0, 2)
    normed_answer = norm_rows(answer_states, dec_gain).astype(jnp.bfloat16)
    query = jnp.dot(normed_answer, w_query, preferred_element_type=jnp.float32).astype(jnp.bfloat16)
    query = query.reshape(ANS, HEADS, DH).transpose(1, 0, 2)
    allowed = key_mask(jnp.arange(TOKENS, dtype=jnp.int32), passage_lengths, passage_owner, answer_lengths, ANS)

    def attend(operands):
        head_query, head_keys, head_values = operands
        scores = jnp.dot(head_query, head_keys.T, preferred_element_type=jnp.float32) * DH ** (-0.5)
        scores = jnp.where(allowed, scores, -1e+30)
        top = lax.optimization_barrier(jnp.max(scores, axis=1, keepdims=True))
        weights = jnp.where(allowed, jnp.exp(scores - top), 0.0)
        total = lax.optimization_barrier(jnp.sum(weights, axis=1, keepdims=True))
        summed = jnp.dot(weights.astype(jnp.bfloat16), head_values, preferred_element_type=jnp.float32)
        return (summed / total).astype(jnp.bfloat16)
    context = lax.map(attend, (query, keys, values)).transpose(1, 0, 2).reshape(ANS, INNER)
    answer = (answer_states.astype(jnp.float32) + jnp.dot(context, w_attn_out, preferred_element_type=jnp.float32)).astype(jnp.bfloat16)
    return (encoded, answer)
```

```python
import jax
import jax.numpy as jnp
from jax import lax
from jax.sharding import PartitionSpec as P

DH = 128
P_SLOT = 16


eps = 1e-06


def norm_rows(states, gain):
    wide = states.astype(jnp.float32)
    factor = lax.rsqrt(jnp.mean(wide * wide, axis=-1, keepdims=True) + eps)
    return wide * factor * gain


def key_mask(token_index, passage_lengths, passage_owner, answer_lengths, answer_count):
    passage = token_index // P_SLOT
    place = token_index % P_SLOT
    count = passage_lengths.shape[0]
    match = passage[:, None] == jnp.arange(count, dtype=jnp.int32)[None, :]
    token_length = jnp.sum(jnp.where(match, passage_lengths[None, :], 0), axis=1)
    token_owner = jnp.sum(jnp.where(match, passage_owner[None, :], 0), axis=1)
    number = answer_lengths.shape[0]
    order = jnp.arange(number, dtype=jnp.int32)
    ends = jnp.sum(jnp.where(order[:, None] <= order[None, :], answer_lengths[:, None], 0), axis=0)
    answer_index = jnp.arange(answer_count, dtype=jnp.int32)
    question = jnp.sum((answer_index[:, None] >= ends[None, :]).astype(jnp.int32), axis=1)
    return (place < token_length)[None, :] & (token_owner[None, :] == question[:, None])


def gather_mp(x, count):
    return lax.all_to_all(jnp.broadcast_to(x[None], (count,) + x.shape), "mp", 0, 0)


def swap_psg(x):
    return lax.ppermute(x, "psg", [(0, 1), (1, 0)])


def per_device(
    tokens,
    enc_gain,
    w_in,
    w_out,
    final_gain,
    w_keyval,
    answer_states,
    dec_gain,
    w_query,
    w_attn_out,
    passage_lengths,
    passage_owner,
    answer_lengths,
):
    row_count = tokens.shape[0]
    width = tokens.shape[1]
    answer_count = answer_states.shape[0]
    mp = lax.axis_size("mp")
    psg = lax.axis_size("psg")
    mp_index = lax.axis_index("mp")
    psg_index = lax.axis_index("psg")
    heads = w_query.shape[1] // DH // psg
    inner = heads * DH

    everyone = gather_mp(tokens, mp).reshape(mp * row_count, width)
    normed = norm_rows(everyone, enc_gain).astype(jnp.bfloat16)
    hidden = jnp.maximum(jnp.dot(normed, w_in, preferred_element_type=jnp.float32), 0.0).astype(
        jnp.bfloat16
    )
    partial_sums = jnp.dot(hidden, w_out, preferred_element_type=jnp.float32).astype(jnp.bfloat16)
    parts = lax.all_to_all(partial_sums.reshape(mp, row_count, width), "mp", 0, 0)
    summed_rows = jnp.sum(parts.astype(jnp.float32), axis=0)
    encoded = (tokens.astype(jnp.float32) + summed_rows).astype(jnp.bfloat16)
    memory = norm_rows(encoded, final_gain).astype(jnp.bfloat16)
    mine = gather_mp(memory, mp).reshape(mp * row_count, width)
    theirs = swap_psg(mine)
    both = jnp.concatenate([mine, theirs], axis=0)
    key_rows = both.shape[0]

    start = psg_index * inner
    w_kv = lax.dynamic_slice_in_dim(w_keyval, start, inner, 2)
    w_q = lax.dynamic_slice_in_dim(w_query, start, inner, 1)
    w_o = lax.dynamic_slice_in_dim(w_attn_out, start, inner, 0)
    keys = jnp.dot(both, w_kv[:, 0], preferred_element_type=jnp.float32).astype(jnp.bfloat16)
    values = jnp.dot(both, w_kv[:, 1], preferred_element_type=jnp.float32).astype(jnp.bfloat16)
    keys = keys.reshape(key_rows, heads, DH)
    values = values.reshape(key_rows, heads, DH)
    normed_answer = norm_rows(answer_states, dec_gain).astype(jnp.bfloat16)
    query = jnp.dot(normed_answer, w_q, preferred_element_type=jnp.float32).astype(jnp.bfloat16)
    query = query.reshape(answer_count, heads, DH)

    local = jnp.arange(key_rows, dtype=jnp.int32)
    half = local // (mp * row_count)
    block = (local % (mp * row_count)) // row_count
    core = jnp.where(half == 0, psg_index, 1 - psg_index)
    token_index = (block * psg + core) * row_count + local % row_count
    allowed = key_mask(token_index, passage_lengths, passage_owner, answer_lengths, answer_count)
    scores = jnp.einsum("qhd,khd->hqk", query, keys, preferred_element_type=jnp.float32) * DH ** (
        -0.5
    )
    scores = jnp.where(allowed[None], scores, -1e30)
    top = jnp.max(scores, axis=2, keepdims=True)
    weights = jnp.where(allowed[None], jnp.exp(scores - top), 0.0)
    total = jnp.sum(weights, axis=2, keepdims=True)
    summed = jnp.einsum(
        "hqk,khd->hqd", weights.astype(jnp.bfloat16), values, preferred_element_type=jnp.float32
    )
    context = (summed / total).astype(jnp.bfloat16)
    context = context.transpose(1, 0, 2).reshape(answer_count, inner)
    partial_answer = jnp.dot(context, w_o, preferred_element_type=jnp.float32)

    out_count = answer_count // mp
    small = out_count // psg
    halves = partial_answer.reshape(mp, psg, small, width)
    keep = lax.dynamic_index_in_dim(halves, psg_index, 1, False)
    give = lax.dynamic_index_in_dim(halves, 1 - psg_index, 1, False)
    chip_sum = (keep + swap_psg(give)).astype(jnp.bfloat16)
    answer_parts = lax.all_to_all(chip_sum, "mp", 0, 0)
    own_start = mp_index * out_count + psg_index * small
    own_answer = lax.dynamic_slice_in_dim(answer_states, own_start, small, 0).astype(jnp.float32)
    piece = (own_answer + jnp.sum(answer_parts.astype(jnp.float32), axis=0)).astype(jnp.bfloat16)
    other = swap_psg(piece)
    first = jnp.where(psg_index == 0, piece, other)
    second = jnp.where(psg_index == 0, other, piece)
    return (encoded, jnp.concatenate([first, second], axis=0))


def solution(mesh):
    placed = (
        P(("groups", "mp", "psg"), None),
        P(),
        P(None, "mp"),
        P("mp", None),
        P(),
        P(None, None, "mp"),
        P("groups", None),
        P(),
        P(None, "mp"),
        P("mp", None),
        P("groups"),
        P("groups"),
        P("groups"),
    )
    return jax.shard_map(
        per_device,
        mesh=mesh,
        in_specs=placed,
        out_specs=(P(("groups", "mp", "psg"), None), P(("groups", "mp"), None)),
        check_vma=False,
    )
```

```python
import jax
import jax.numpy as jnp
from jax import lax
from jax.experimental import pallas as pl
from jax.experimental.pallas import tpu as pltpu
from jax.sharding import PartitionSpec as P

DH = 128
P_SLOT = 16


eps = 1e-06


def norm_rows(states, gain):
    wide = states.astype(jnp.float32)
    factor = lax.rsqrt(jnp.mean(wide * wide, axis=-1, keepdims=True) + eps)
    return wide * factor * gain


def key_mask(token_index, passage_lengths, passage_owner, answer_lengths, answer_count):
    passage = token_index // P_SLOT
    place = token_index % P_SLOT
    count = passage_lengths.shape[0]
    match = passage[:, None] == jnp.arange(count, dtype=jnp.int32)[None, :]
    token_length = jnp.sum(jnp.where(match, passage_lengths[None, :], 0), axis=1)
    token_owner = jnp.sum(jnp.where(match, passage_owner[None, :], 0), axis=1)
    number = answer_lengths.shape[0]
    order = jnp.arange(number, dtype=jnp.int32)
    ends = jnp.sum(jnp.where(order[:, None] <= order[None, :], answer_lengths[:, None], 0), axis=0)
    answer_index = jnp.arange(answer_count, dtype=jnp.int32)
    question = jnp.sum((answer_index[:, None] >= ends[None, :]).astype(jnp.int32), axis=1)
    return (place < token_length)[None, :] & (token_owner[None, :] == question[:, None])


def gather_mp(x, count):
    return lax.all_to_all(jnp.broadcast_to(x[None], (count,) + x.shape), "mp", 0, 0)


def swap_psg(x):
    return lax.ppermute(x, "psg", [(0, 1), (1, 0)])


BF16 = jnp.bfloat16
F32 = jnp.float32
SMEM_SPEC = pl.BlockSpec(memory_space=pltpu.SMEM)
VMEM_SPEC = pl.BlockSpec(memory_space=pltpu.VMEM)
HBM_SPEC = pl.BlockSpec(memory_space=pltpu.HBM)


def limit(mib):
    return pltpu.CompilerParams(vmem_limit_bytes=mib << 20)


def prepare_kernel(half, states, gain, w_query, w_keyval, query, wkv, scr_q, scr_kv, sems):
    width = states.shape[1]
    inner = query.shape[1]
    strips = inner // 128
    start = pl.multiple_of(half[0] * inner, 128)
    q_copy = pltpu.make_async_copy(w_query.at[:, pl.ds(start, inner)], scr_q, sems.at[strips])
    copies = [
        pltpu.make_async_copy(
            w_keyval.at[:, :, pl.ds(pl.multiple_of(start + s * 128, 128), 128)],
            scr_kv.at[s],
            sems.at[s],
        )
        for s in range(strips)
    ]
    q_copy.start()
    for copy in copies:
        copy.start()
    normed = norm_rows(states[...], gain[...]).astype(BF16)
    q_copy.wait()
    for c in range(inner // 256):
        columns = pl.ds(c * 256, 256)
        query[:, columns] = jnp.dot(
            normed, scr_q[:, columns], preferred_element_type=F32
        ).astype(BF16)
    row = lax.broadcasted_iota(jnp.int32, (256, 256), 0)
    column = lax.broadcasted_iota(jnp.int32, (256, 256), 1)
    source = jnp.where(row < 128, 2 * row, 2 * (row - 128) + 1)
    pick = jnp.where(column == source, 1.0, 0.0).astype(BF16)
    for s in range(0, strips, 2):
        copies[s].wait()
        copies[s + 1].wait()
        for b in range(width // 128):
            rows = pl.ds(b * 128, 128)
            mixed = jnp.concatenate(
                [scr_kv[s, rows].reshape(256, 128), scr_kv[s + 1, rows].reshape(256, 128)], axis=1
            )
            apart = jnp.dot(pick, mixed, preferred_element_type=F32).astype(BF16)
            wkv[0, rows, pl.ds(s * 128, 256)] = apart[:128]
            wkv[1, rows, pl.ds(s * 128, 256)] = apart[128:]


def prepare(half, states, gain, w_query, w_keyval, inner):
    count, width = states.shape
    strips = inner // 128
    return pl.pallas_call(
        prepare_kernel,
        out_shape=(
            jax.ShapeDtypeStruct((count, inner), BF16),
            jax.ShapeDtypeStruct((2, width, inner), BF16),
        ),
        in_specs=[SMEM_SPEC, VMEM_SPEC, VMEM_SPEC, HBM_SPEC, HBM_SPEC],
        out_specs=(VMEM_SPEC, VMEM_SPEC),
        scratch_shapes=[
            pltpu.VMEM((width, inner), BF16),
            pltpu.VMEM((strips, width, 2, 128), BF16),
            pltpu.SemaphoreType.DMA((strips + 1,)),
        ],
        compiler_params=limit(52),
        cost_estimate=pl.CostEstimate(
            flops=2 * count * width * inner + 4 * width * 256 * inner,
            bytes_accessed=10 * width * inner,
            transcendentals=0,
        ),
        name="prepare",
    )(half, states, gain.reshape(1, width), w_query, w_keyval)


def feed_kernel(everyone, gain, w_in, w_out, out, scr_in, scr_out, acc, sems):
    chunks, _, size = scr_in.shape
    copies = []
    for c in range(chunks):
        copies.append(
            (
                pltpu.make_async_copy(w_in.at[:, pl.ds(c * size, size)], scr_in.at[c], sems.at[0, c]),
                pltpu.make_async_copy(w_out.at[pl.ds(c * size, size)], scr_out.at[c], sems.at[1, c]),
            )
        )
    for first, second in copies:
        first.start()
        second.start()
    normed = norm_rows(everyone[...], gain[...]).astype(BF16)
    for c in range(chunks):
        copies[c][0].wait()
        hidden = jnp.maximum(
            jnp.dot(normed, scr_in[c], preferred_element_type=F32), 0.0
        ).astype(BF16)
        copies[c][1].wait()
        part = jnp.dot(hidden, scr_out[c], preferred_element_type=F32)
        if c > 0:
            part = part + acc[...]
        if c < chunks - 1:
            acc[...] = part
        else:
            out[...] = part.astype(BF16)


def feed(everyone, gain, w_in, w_out):
    rows, width = everyone.shape
    units = w_in.shape[1]
    size = min(512, units)
    chunks = units // size
    return pl.pallas_call(
        feed_kernel,
        out_shape=jax.ShapeDtypeStruct((rows, width), BF16),
        in_specs=[VMEM_SPEC, VMEM_SPEC, HBM_SPEC, HBM_SPEC],
        out_specs=VMEM_SPEC,
        scratch_shapes=[
            pltpu.VMEM((chunks, width, size), BF16),
            pltpu.VMEM((chunks, size, width), BF16),
            pltpu.VMEM((rows, width), F32),
            pltpu.SemaphoreType.DMA((2, chunks)),
        ],
        compiler_params=limit(52),
        cost_estimate=pl.CostEstimate(
            flops=4 * rows * width * units, bytes_accessed=4 * width * units, transcendentals=0
        ),
        name="feed",
    )(everyone, gain.reshape(1, width), w_in, w_out)


def settle_kernel(parts, tokens, gain, encoded, spread):
    total = tokens[...].astype(F32)
    for k in range(parts.shape[0]):
        total = total + parts[k].astype(F32)
    rounded = total.astype(BF16)
    encoded[...] = rounded
    memory = norm_rows(rounded, gain[...]).astype(BF16)
    for k in range(spread.shape[0]):
        spread[k] = memory


def settle(parts, tokens, gain):
    count, rows, width = parts.shape
    return pl.pallas_call(
        settle_kernel,
        out_shape=(
            jax.ShapeDtypeStruct((rows, width), BF16),
            jax.ShapeDtypeStruct((count, rows, width), BF16),
        ),
        in_specs=[VMEM_SPEC] * 3,
        out_specs=(VMEM_SPEC, VMEM_SPEC),
        compiler_params=limit(8),
        name="settle",
    )(parts, tokens, gain.reshape(1, width))


def attend_kernel(half, mine, theirs, query, allowed, wkv, w_out, out, scr_k, scr_v, scr_o, context, sems):
    chunks, _, size = scr_k.shape
    inner = chunks * size
    width = out.shape[1]
    start = pl.multiple_of(half[0] * inner, 128)
    copies = []
    for c in range(chunks):
        columns = pl.ds(c * size, size)
        copies.append(
            (
                pltpu.make_async_copy(wkv.at[0, :, columns], scr_k.at[c], sems.at[0, c]),
                pltpu.make_async_copy(wkv.at[1, :, columns], scr_v.at[c], sems.at[1, c]),
            )
        )
    o_copy = pltpu.make_async_copy(w_out.at[pl.ds(start, inner)], scr_o, sems.at[2, 0])
    for first, second in copies:
        first.start()
        second.start()
    o_copy.start()
    live = allowed[...] > 0
    both = jnp.concatenate([mine[...], theirs[...]], axis=0)
    for c in range(chunks):
        copies[c][0].wait()
        keys = jnp.dot(both, scr_k[c], preferred_element_type=F32).astype(BF16)
        copies[c][1].wait()
        values = jnp.dot(both, scr_v[c], preferred_element_type=F32).astype(BF16)
        for h in range(size // DH):
            lanes = slice(h * DH, (h + 1) * DH)
            columns = pl.ds(c * size + h * DH, DH)
            scores = lax.dot_general(
                query[:, columns],
                keys[:, lanes],
                (((1,), (1,)), ((), ())),
                preferred_element_type=F32,
            ) * DH ** (-0.5)
            scores = jnp.where(live, scores, -1e30)
            top = jnp.max(scores, axis=1, keepdims=True)
            weights = jnp.where(live, jnp.exp(scores - top), 0.0)
            total = jnp.sum(weights, axis=1, keepdims=True)
            summed = jnp.dot(weights.astype(BF16), values[:, lanes], preferred_element_type=F32)
            context[:, columns] = (summed / total).astype(BF16)
    o_copy.wait()
    for c in range(width // 256):
        columns = pl.ds(c * 256, 256)
        out[:, columns] = jnp.dot(context[...], scr_o[:, columns], preferred_element_type=F32)


def attend(half, mine, theirs, query, allowed, wkv, w_attn_out):
    rows, width = mine.shape
    count, inner = query.shape
    size = min(256, inner)
    chunks = inner // size
    keys = 2 * rows
    return pl.pallas_call(
        attend_kernel,
        out_shape=jax.ShapeDtypeStruct((count, width), F32),
        in_specs=[SMEM_SPEC] + [VMEM_SPEC] * 4 + [HBM_SPEC] * 2,
        out_specs=VMEM_SPEC,
        scratch_shapes=[
            pltpu.VMEM((chunks, width, size), BF16),
            pltpu.VMEM((chunks, width, size), BF16),
            pltpu.VMEM((inner, width), BF16),
            pltpu.VMEM((count, inner), BF16),
            pltpu.SemaphoreType.DMA((3, chunks)),
        ],
        compiler_params=limit(52),
        cost_estimate=pl.CostEstimate(
            flops=4 * keys * width * inner + 4 * count * keys * inner + 2 * count * inner * width,
            bytes_accessed=6 * width * inner,
            transcendentals=count * keys * inner // DH,
        ),
        name="attend",
    )(half, mine, theirs, query, allowed, wkv, w_attn_out)


def per_device(
    tokens,
    enc_gain,
    w_in,
    w_out,
    final_gain,
    w_keyval,
    answer_states,
    dec_gain,
    w_query,
    w_attn_out,
    passage_lengths,
    passage_owner,
    answer_lengths,
):
    row_count = tokens.shape[0]
    width = tokens.shape[1]
    answer_count = answer_states.shape[0]
    mp = lax.axis_size("mp")
    psg = lax.axis_size("psg")
    mp_index = lax.axis_index("mp")
    psg_index = lax.axis_index("psg")
    heads = w_query.shape[1] // DH // psg
    inner = heads * DH

    half = jnp.reshape(psg_index, (1,)).astype(jnp.int32)
    everyone = gather_mp(tokens, mp).reshape(mp * row_count, width)
    query, wkv = prepare(half, answer_states, dec_gain, w_query, w_keyval, inner)
    partial_sums = feed(everyone, enc_gain, w_in, w_out)
    parts = lax.all_to_all(partial_sums.reshape(mp, row_count, width), "mp", 0, 0)
    encoded, spread = settle(parts, tokens, final_gain)
    mine = lax.all_to_all(spread, "mp", 0, 0).reshape(mp * row_count, width)
    theirs = swap_psg(mine)
    key_rows = 2 * mp * row_count

    local = jnp.arange(key_rows, dtype=jnp.int32)
    far = local // (mp * row_count)
    block = (local % (mp * row_count)) // row_count
    core = jnp.where(far == 0, psg_index, 1 - psg_index)
    token_index = (block * psg + core) * row_count + local % row_count
    allowed = key_mask(token_index, passage_lengths, passage_owner, answer_lengths, answer_count)
    partial_answer = attend(
        half, mine, theirs, query, allowed.astype(jnp.int32), wkv, w_attn_out
    )

    out_count = answer_count // mp
    small = out_count // psg
    halves = partial_answer.reshape(mp, psg, small, width)
    keep = lax.dynamic_index_in_dim(halves, psg_index, 1, False)
    give = lax.dynamic_index_in_dim(halves, 1 - psg_index, 1, False)
    chip_sum = (keep + swap_psg(give)).astype(jnp.bfloat16)
    answer_parts = lax.all_to_all(chip_sum, "mp", 0, 0)
    own_start = mp_index * out_count + psg_index * small
    own_answer = lax.dynamic_slice_in_dim(answer_states, own_start, small, 0).astype(jnp.float32)
    piece = (own_answer + jnp.sum(answer_parts.astype(jnp.float32), axis=0)).astype(jnp.bfloat16)
    other = swap_psg(piece)
    first = jnp.where(psg_index == 0, piece, other)
    second = jnp.where(psg_index == 0, other, piece)
    return (encoded, jnp.concatenate([first, second], axis=0))


def solution(mesh):
    placed = (
        P(("groups", "mp", "psg"), None),
        P(),
        P(None, "mp"),
        P("mp", None),
        P(),
        P(None, None, "mp"),
        P("groups", None),
        P(),
        P(None, "mp"),
        P("mp", None),
        P("groups"),
        P("groups"),
        P("groups"),
    )
    return jax.shard_map(
        per_device,
        mesh=mesh,
        in_specs=placed,
        out_specs=(P(("groups", "mp", "psg"), None), P(("groups", "mp"), None)),
        check_vma=False,
    )
```

```python
import functools

import jax
import jax.numpy as jnp
from jax import lax
from jax.experimental import pallas as pl
from jax.experimental.pallas import tpu as pltpu
from jax.sharding import PartitionSpec as P

DH = 128
P_SLOT = 16


eps = 1e-06


def norm_rows(states, gain):
    wide = states.astype(jnp.float32)
    factor = lax.rsqrt(jnp.mean(wide * wide, axis=-1, keepdims=True) + eps)
    return wide * factor * gain


def key_mask(token_index, passage_lengths, passage_owner, answer_lengths, answer_count):
    passage = token_index // P_SLOT
    place = token_index % P_SLOT
    count = passage_lengths.shape[0]
    match = passage[:, None] == jnp.arange(count, dtype=jnp.int32)[None, :]
    token_length = jnp.sum(jnp.where(match, passage_lengths[None, :], 0), axis=1)
    token_owner = jnp.sum(jnp.where(match, passage_owner[None, :], 0), axis=1)
    number = answer_lengths.shape[0]
    order = jnp.arange(number, dtype=jnp.int32)
    ends = jnp.sum(jnp.where(order[:, None] <= order[None, :], answer_lengths[:, None], 0), axis=0)
    answer_index = jnp.arange(answer_count, dtype=jnp.int32)
    question = jnp.sum((answer_index[:, None] >= ends[None, :]).astype(jnp.int32), axis=1)
    return (place < token_length)[None, :] & (token_owner[None, :] == question[:, None])


def gather_mp(x, count):
    return lax.all_to_all(jnp.broadcast_to(x[None], (count,) + x.shape), "mp", 0, 0)


def swap_psg(x):
    return lax.ppermute(x, "psg", [(0, 1), (1, 0)])


BF16 = jnp.bfloat16
F32 = jnp.float32
SMEM_SPEC = pl.BlockSpec(memory_space=pltpu.SMEM)
VMEM_SPEC = pl.BlockSpec(memory_space=pltpu.VMEM)
HBM_SPEC = pl.BlockSpec(memory_space=pltpu.HBM)


def limit(mib):
    return pltpu.CompilerParams(vmem_limit_bytes=mib << 20)


def prepare_kernel(half, states, gain, w_query, w_keyval, query, wkv, scr_q, scr_kv, sems):
    width = states.shape[1]
    inner = query.shape[1]
    strips = inner // 128
    start = pl.multiple_of(half[0] * inner, 128)
    q_copy = pltpu.make_async_copy(w_query.at[:, pl.ds(start, inner)], scr_q, sems.at[strips])
    copies = [
        pltpu.make_async_copy(
            w_keyval.at[:, :, pl.ds(pl.multiple_of(start + s * 128, 128), 128)],
            scr_kv.at[s],
            sems.at[s],
        )
        for s in range(strips)
    ]
    q_copy.start()
    for copy in copies:
        copy.start()
    normed = norm_rows(states[...], gain[...]).astype(BF16)
    q_copy.wait()
    for c in range(inner // 256):
        columns = pl.ds(c * 256, 256)
        query[:, columns] = jnp.dot(
            normed, scr_q[:, columns], preferred_element_type=F32
        ).astype(BF16)
    row = lax.broadcasted_iota(jnp.int32, (256, 256), 0)
    column = lax.broadcasted_iota(jnp.int32, (256, 256), 1)
    source = jnp.where(row < 128, 2 * row, 2 * (row - 128) + 1)
    pick = jnp.where(column == source, 1.0, 0.0).astype(BF16)
    for s in range(0, strips, 2):
        copies[s].wait()
        copies[s + 1].wait()
        for b in range(width // 128):
            rows = pl.ds(b * 128, 128)
            mixed = jnp.concatenate(
                [scr_kv[s, rows].reshape(256, 128), scr_kv[s + 1, rows].reshape(256, 128)], axis=1
            )
            apart = jnp.dot(pick, mixed, preferred_element_type=F32).astype(BF16)
            wkv[0, rows, pl.ds(s * 128, 256)] = apart[:128]
            wkv[1, rows, pl.ds(s * 128, 256)] = apart[128:]


def prepare(half, states, gain, w_query, w_keyval, inner):
    count, width = states.shape
    strips = inner // 128
    return pl.pallas_call(
        prepare_kernel,
        out_shape=(
            jax.ShapeDtypeStruct((count, inner), BF16),
            jax.ShapeDtypeStruct((2, width, inner), BF16),
        ),
        in_specs=[SMEM_SPEC, VMEM_SPEC, VMEM_SPEC, HBM_SPEC, HBM_SPEC],
        out_specs=(VMEM_SPEC, VMEM_SPEC),
        scratch_shapes=[
            pltpu.VMEM((width, inner), BF16),
            pltpu.VMEM((strips, width, 2, 128), BF16),
            pltpu.SemaphoreType.DMA((strips + 1,)),
        ],
        compiler_params=limit(52),
        cost_estimate=pl.CostEstimate(
            flops=2 * count * width * inner + 4 * width * 256 * inner,
            bytes_accessed=10 * width * inner,
            transcendentals=0,
        ),
        name="prepare",
    )(half, states, gain.reshape(1, width), w_query, w_keyval)


def stage_kernel(after, whole, out, sems, *, axis, start):
    del after
    size = out.shape[axis]
    number = sems.shape[0]
    step = size // number
    copies = []
    for k in range(number):
        if axis == 0:
            source = whole.at[pl.ds(start + k * step, step)]
            target = out.at[pl.ds(k * step, step)]
        else:
            source = whole.at[:, pl.ds(start + k * step, step)]
            target = out.at[:, pl.ds(k * step, step)]
        copies.append(pltpu.make_async_copy(source, target, sems.at[k]))
    for copy in copies:
        copy.start()
    for copy in copies:
        copy.wait()


def stage(after, whole, axis, part, parts):
    shape = list(whole.shape)
    shape[axis] //= parts
    return pl.pallas_call(
        functools.partial(stage_kernel, axis=axis, start=part * shape[axis]),
        out_shape=jax.ShapeDtypeStruct(tuple(shape), BF16),
        in_specs=[SMEM_SPEC if after.size == 1 else HBM_SPEC, HBM_SPEC],
        out_specs=VMEM_SPEC,
        scratch_shapes=[pltpu.SemaphoreType.DMA((4,))],
        compiler_params=limit(44),
        cost_estimate=pl.CostEstimate(
            flops=1 << 30, bytes_accessed=4 * shape[0] * shape[1], transcendentals=0
        ),
        name="stage",
    )(after, whole)


def feed_kernel(index, mine, theirs, gain, *refs, patterns):
    *weights, out, normed, acc = refs
    half = len(weights) // 2
    pairs, rows, width = mine.shape
    units = weights[0].shape[1]
    size = min(512, units)
    weight = gain[...]
    for k in range(2 * pairs):
        place = pl.multiple_of((index[0] ^ patterns[k]) * rows, rows)
        states = mine[k] if k < pairs else theirs[k - pairs]
        normed[pl.ds(place, rows)] = norm_rows(states, weight).astype(BF16)
    first = True
    for w_in, w_out in zip(weights[:half], weights[half:]):
        for c in range(units // size):
            columns = pl.ds(c * size, size)
            hidden = jnp.maximum(
                jnp.dot(normed[...], w_in[:, columns], preferred_element_type=F32), 0.0
            ).astype(BF16)
            part = jnp.dot(hidden, w_out[columns], preferred_element_type=F32)
            acc[...] = part if first else part + acc[...]
            first = False
    out[...] = acc[...].astype(BF16)


def feed(index, mine, theirs, gain, weights, patterns):
    pairs, rows, width = mine.shape
    count = 2 * pairs * rows
    units = weights[0].shape[1] * len(weights) // 2
    return pl.pallas_call(
        functools.partial(feed_kernel, patterns=patterns),
        out_shape=jax.ShapeDtypeStruct((count, width), BF16),
        in_specs=[SMEM_SPEC] + [VMEM_SPEC] * (3 + len(weights)),
        out_specs=VMEM_SPEC,
        scratch_shapes=[pltpu.VMEM((count, width), BF16), pltpu.VMEM((count, width), F32)],
        compiler_params=limit(24),
        cost_estimate=pl.CostEstimate(
            flops=4 * count * width * units, bytes_accessed=4 * width * units, transcendentals=0
        ),
        name="feed",
    )(index, mine, theirs, gain.reshape(1, width), *weights)


def settle_kernel(parts, tokens, gain, encoded, spread):
    total = tokens[...].astype(F32)
    for k in range(parts.shape[0]):
        total = total + parts[k].astype(F32)
    rounded = total.astype(BF16)
    encoded[...] = rounded
    memory = norm_rows(rounded, gain[...]).astype(BF16)
    for k in range(spread.shape[0]):
        spread[k] = memory


def settle(parts, tokens, gain):
    count, rows, width = parts.shape
    return pl.pallas_call(
        settle_kernel,
        out_shape=(
            jax.ShapeDtypeStruct((rows, width), BF16),
            jax.ShapeDtypeStruct((count, rows, width), BF16),
        ),
        in_specs=[VMEM_SPEC] * 3,
        out_specs=(VMEM_SPEC, VMEM_SPEC),
        compiler_params=limit(8),
        name="settle",
    )(parts, tokens, gain.reshape(1, width))


def attend_kernel(half, mine, theirs, query, allowed, wkv, w_out, out, scr_k, scr_v, scr_o, context, sems):
    chunks, _, size = scr_k.shape
    inner = chunks * size
    width = out.shape[1]
    start = pl.multiple_of(half[0] * inner, 128)
    copies = []
    for c in range(chunks):
        columns = pl.ds(c * size, size)
        copies.append(
            (
                pltpu.make_async_copy(wkv.at[0, :, columns], scr_k.at[c], sems.at[0, c]),
                pltpu.make_async_copy(wkv.at[1, :, columns], scr_v.at[c], sems.at[1, c]),
            )
        )
    o_copy = pltpu.make_async_copy(w_out.at[pl.ds(start, inner)], scr_o, sems.at[2, 0])
    for first, second in copies:
        first.start()
        second.start()
    o_copy.start()
    live = allowed[...] > 0
    both = jnp.concatenate([mine[...], theirs[...]], axis=0)
    for c in range(chunks):
        copies[c][0].wait()
        keys = jnp.dot(both, scr_k[c], preferred_element_type=F32).astype(BF16)
        copies[c][1].wait()
        values = jnp.dot(both, scr_v[c], preferred_element_type=F32).astype(BF16)
        for h in range(size // DH):
            lanes = slice(h * DH, (h + 1) * DH)
            columns = pl.ds(c * size + h * DH, DH)
            scores = lax.dot_general(
                query[:, columns],
                keys[:, lanes],
                (((1,), (1,)), ((), ())),
                preferred_element_type=F32,
            ) * DH ** (-0.5)
            scores = jnp.where(live, scores, -1e30)
            top = jnp.max(scores, axis=1, keepdims=True)
            weights = jnp.where(live, jnp.exp(scores - top), 0.0)
            total = jnp.sum(weights, axis=1, keepdims=True)
            summed = jnp.dot(weights.astype(BF16), values[:, lanes], preferred_element_type=F32)
            context[:, columns] = (summed / total).astype(BF16)
    o_copy.wait()
    for c in range(width // 256):
        columns = pl.ds(c * 256, 256)
        out[:, columns] = jnp.dot(context[...], scr_o[:, columns], preferred_element_type=F32)


def attend(half, mine, theirs, query, allowed, wkv, w_attn_out):
    rows, width = mine.shape
    count, inner = query.shape
    size = min(256, inner)
    chunks = inner // size
    keys = 2 * rows
    return pl.pallas_call(
        attend_kernel,
        out_shape=jax.ShapeDtypeStruct((count, width), F32),
        in_specs=[SMEM_SPEC] + [VMEM_SPEC] * 4 + [HBM_SPEC] * 2,
        out_specs=VMEM_SPEC,
        scratch_shapes=[
            pltpu.VMEM((chunks, width, size), BF16),
            pltpu.VMEM((chunks, width, size), BF16),
            pltpu.VMEM((inner, width), BF16),
            pltpu.VMEM((count, inner), BF16),
            pltpu.SemaphoreType.DMA((3, chunks)),
        ],
        compiler_params=limit(52),
        cost_estimate=pl.CostEstimate(
            flops=4 * keys * width * inner + 4 * count * keys * inner + 2 * count * inner * width,
            bytes_accessed=6 * width * inner,
            transcendentals=count * keys * inner // DH,
        ),
        name="attend",
    )(half, mine, theirs, query, allowed, wkv, w_attn_out)


def per_device(
    tokens,
    enc_gain,
    w_in,
    w_out,
    final_gain,
    w_keyval,
    answer_states,
    dec_gain,
    w_query,
    w_attn_out,
    passage_lengths,
    passage_owner,
    answer_lengths,
):
    row_count = tokens.shape[0]
    width = tokens.shape[1]
    answer_count = answer_states.shape[0]
    mp = lax.axis_size("mp")
    psg = lax.axis_size("psg")
    mp_index = lax.axis_index("mp")
    psg_index = lax.axis_index("psg")
    heads = w_query.shape[1] // DH // psg
    inner = heads * DH

    half = jnp.reshape(psg_index, (1,)).astype(jnp.int32)
    index = jnp.reshape(mp_index, (1,)).astype(jnp.int32)
    patterns = [0]
    held = tokens[None]
    weights = []
    step = mp // 2
    while step > 0:
        got = lax.ppermute(held, "mp", [(j, j ^ step) for j in range(mp)])
        after = index if step == mp // 2 else held
        if step == mp // 2:
            weights.append(stage(after, w_in, 1, 0, 2))
        elif step == mp // 4:
            weights.append(stage(after, w_in, 1, 1, 2))
        elif step == 1:
            weights.append(stage(after, w_out, 0, 0, 2))
            weights.append(stage(after, w_out, 0, 1, 2))
        patterns = patterns + [p ^ step for p in patterns]
        if step > 1:
            held = jnp.concatenate([held, got], axis=0)
        step //= 2
    query, wkv = prepare(half, answer_states, dec_gain, w_query, w_keyval, inner)
    partial_sums = feed(index, held, got, enc_gain, weights, patterns)
    parts = lax.all_to_all(partial_sums.reshape(mp, row_count, width), "mp", 0, 0)
    encoded, spread = settle(parts, tokens, final_gain)
    mine = lax.all_to_all(spread, "mp", 0, 0).reshape(mp * row_count, width)
    theirs = swap_psg(mine)
    key_rows = 2 * mp * row_count

    local = jnp.arange(key_rows, dtype=jnp.int32)
    far = local // (mp * row_count)
    block = (local % (mp * row_count)) // row_count
    core = jnp.where(far == 0, psg_index, 1 - psg_index)
    token_index = (block * psg + core) * row_count + local % row_count
    allowed = key_mask(token_index, passage_lengths, passage_owner, answer_lengths, answer_count)
    partial_answer = attend(
        half, mine, theirs, query, allowed.astype(jnp.int32), wkv, w_attn_out
    )

    out_count = answer_count // mp
    small = out_count // psg
    halves = partial_answer.reshape(mp, psg, small, width)
    keep = lax.dynamic_index_in_dim(halves, psg_index, 1, False)
    give = lax.dynamic_index_in_dim(halves, 1 - psg_index, 1, False)
    chip_sum = (keep + swap_psg(give)).astype(jnp.bfloat16)
    answer_parts = lax.all_to_all(chip_sum, "mp", 0, 0)
    own_start = mp_index * out_count + psg_index * small
    own_answer = lax.dynamic_slice_in_dim(answer_states, own_start, small, 0).astype(jnp.float32)
    piece = (own_answer + jnp.sum(answer_parts.astype(jnp.float32), axis=0)).astype(jnp.bfloat16)
    other = swap_psg(piece)
    first = jnp.where(psg_index == 0, piece, other)
    second = jnp.where(psg_index == 0, other, piece)
    return (encoded, jnp.concatenate([first, second], axis=0))


def solution(mesh):
    placed = (
        P(("groups", "mp", "psg"), None),
        P(),
        P(None, "mp"),
        P("mp", None),
        P(),
        P(None, None, "mp"),
        P("groups", None),
        P(),
        P(None, "mp"),
        P("mp", None),
        P("groups"),
        P("groups"),
        P("groups"),
    )
    return jax.shard_map(
        per_device,
        mesh=mesh,
        in_specs=placed,
        out_specs=(P(("groups", "mp", "psg"), None), P(("groups", "mp"), None)),
        check_vma=False,
    )
```

```python
import functools

import jax
import jax.numpy as jnp
from jax import lax
from jax.experimental import pallas as pl
from jax.experimental.pallas import tpu as pltpu
from jax.sharding import PartitionSpec as P

DH = 128
P_SLOT = 16


eps = 1e-06


def norm_rows(states, gain):
    wide = states.astype(jnp.float32)
    factor = lax.rsqrt(jnp.mean(wide * wide, axis=-1, keepdims=True) + eps)
    return wide * factor * gain


def key_mask(token_index, passage_lengths, passage_owner, answer_lengths, answer_count):
    passage = token_index // P_SLOT
    place = token_index % P_SLOT
    count = passage_lengths.shape[0]
    match = passage[:, None] == jnp.arange(count, dtype=jnp.int32)[None, :]
    token_length = jnp.sum(jnp.where(match, passage_lengths[None, :], 0), axis=1)
    token_owner = jnp.sum(jnp.where(match, passage_owner[None, :], 0), axis=1)
    number = answer_lengths.shape[0]
    order = jnp.arange(number, dtype=jnp.int32)
    ends = jnp.sum(jnp.where(order[:, None] <= order[None, :], answer_lengths[:, None], 0), axis=0)
    answer_index = jnp.arange(answer_count, dtype=jnp.int32)
    question = jnp.sum((answer_index[:, None] >= ends[None, :]).astype(jnp.int32), axis=1)
    return (place < token_length)[None, :] & (token_owner[None, :] == question[:, None])


def gather_mp(x, count):
    return lax.all_to_all(jnp.broadcast_to(x[None], (count,) + x.shape), "mp", 0, 0)


def swap_psg(x):
    return lax.ppermute(x, "psg", [(0, 1), (1, 0)])


BF16 = jnp.bfloat16
F32 = jnp.float32
SMEM_SPEC = pl.BlockSpec(memory_space=pltpu.SMEM)
VMEM_SPEC = pl.BlockSpec(memory_space=pltpu.VMEM)
HBM_SPEC = pl.BlockSpec(memory_space=pltpu.HBM)


def limit(mib):
    return pltpu.CompilerParams(vmem_limit_bytes=mib << 20)


def prepare_kernel(half, states, gain, w_query, w_keyval, query, w_key, wkv, scr_q, scr_kv, sems):
    width = states.shape[1]
    inner = query.shape[1]
    strips = inner // 128
    start = pl.multiple_of(half[0] * inner, 128)
    q_copy = pltpu.make_async_copy(w_query.at[:, pl.ds(start, inner)], scr_q, sems.at[strips])
    copies = [
        pltpu.make_async_copy(
            w_keyval.at[:, :, pl.ds(pl.multiple_of(start + s * 128, 128), 128)],
            scr_kv.at[s],
            sems.at[s],
        )
        for s in range(strips)
    ]
    q_copy.start()
    for copy in copies:
        copy.start()
    normed = norm_rows(states[...], gain[...]).astype(BF16)
    q_copy.wait()
    for c in range(inner // 256):
        columns = pl.ds(c * 256, 256)
        query[:, columns] = jnp.dot(
            normed, scr_q[:, columns], preferred_element_type=F32
        ).astype(BF16)
    row = lax.broadcasted_iota(jnp.int32, (256, 256), 0)
    column = lax.broadcasted_iota(jnp.int32, (256, 256), 1)
    source = jnp.where(row < 128, 2 * row, 2 * (row - 128) + 1)
    pick = jnp.where(column == source, 1.0, 0.0).astype(BF16)
    for s in range(0, strips, 2):
        copies[s].wait()
        copies[s + 1].wait()
        for b in range(width // 128):
            rows = pl.ds(b * 128, 128)
            mixed = jnp.concatenate(
                [scr_kv[s, rows].reshape(256, 128), scr_kv[s + 1, rows].reshape(256, 128)], axis=1
            )
            apart = jnp.dot(pick, mixed, preferred_element_type=F32).astype(BF16)
            w_key[rows, pl.ds(s * 128, 256)] = apart[:128]
            wkv[0, rows, pl.ds(s * 128, 256)] = apart[:128]
            wkv[1, rows, pl.ds(s * 128, 256)] = apart[128:]


def prepare(half, states, gain, w_query, w_keyval, inner):
    count, width = states.shape
    strips = inner // 128
    return pl.pallas_call(
        prepare_kernel,
        out_shape=(
            jax.ShapeDtypeStruct((count, inner), BF16),
            jax.ShapeDtypeStruct((width, inner), BF16),
            jax.ShapeDtypeStruct((2, width, inner), BF16),
        ),
        in_specs=[SMEM_SPEC, VMEM_SPEC, VMEM_SPEC, HBM_SPEC, HBM_SPEC],
        out_specs=(VMEM_SPEC,) * 3,
        scratch_shapes=[
            pltpu.VMEM((width, inner), BF16),
            pltpu.VMEM((strips, width, 2, 128), BF16),
            pltpu.SemaphoreType.DMA((strips + 1,)),
        ],
        compiler_params=limit(51),
        cost_estimate=pl.CostEstimate(
            flops=2 * count * width * inner + 4 * width * 256 * inner,
            bytes_accessed=10 * width * inner,
            transcendentals=0,
        ),
        name="prepare",
    )(half, states, gain.reshape(1, width), w_query, w_keyval)


def stage_kernel(after, whole, out, sems, *, axis, start):
    del after
    size = out.shape[axis]
    number = sems.shape[0]
    step = size // number
    copies = []
    for k in range(number):
        if axis == 0:
            source = whole.at[pl.ds(start + k * step, step)]
            target = out.at[pl.ds(k * step, step)]
        else:
            source = whole.at[:, pl.ds(start + k * step, step)]
            target = out.at[:, pl.ds(k * step, step)]
        copies.append(pltpu.make_async_copy(source, target, sems.at[k]))
    for copy in copies:
        copy.start()
    for copy in copies:
        copy.wait()


def stage(after, whole, axis, part, parts, room=44):
    shape = list(whole.shape)
    shape[axis] //= parts
    return pl.pallas_call(
        functools.partial(stage_kernel, axis=axis, start=part * shape[axis]),
        out_shape=jax.ShapeDtypeStruct(tuple(shape), BF16),
        in_specs=[SMEM_SPEC if after.size == 1 else HBM_SPEC, HBM_SPEC],
        out_specs=VMEM_SPEC,
        scratch_shapes=[pltpu.SemaphoreType.DMA((4,))],
        compiler_params=limit(room),
        cost_estimate=pl.CostEstimate(
            flops=1 << 30, bytes_accessed=4 * shape[0] * shape[1], transcendentals=0
        ),
        name="stage",
    )(after, whole)


def feed_kernel(index, mine, theirs, gain, *refs, patterns):
    *weights, out, normed, hidden = refs
    half = len(weights) // 2
    pairs, rows, width = mine.shape
    units = weights[0].shape[1]
    size = min(256, units)
    weight = gain[...]
    for k in range(2 * pairs):
        place = pl.multiple_of((index[0] ^ patterns[k]) * rows, rows)
        states = mine[k] if k < pairs else theirs[k - pairs]
        normed[pl.ds(place, rows)] = norm_rows(states, weight).astype(BF16)
    for part in range(half):
        for c in range(units // size):
            columns = pl.ds(c * size, size)
            hidden[part, :, columns] = jnp.maximum(
                jnp.dot(normed[...], weights[part][:, columns], preferred_element_type=F32), 0.0
            ).astype(BF16)
    for c in range(width // 256):
        columns = pl.ds(c * 256, 256)
        total = jnp.dot(hidden[0], weights[half][:, columns], preferred_element_type=F32)
        for part in range(1, half):
            total = total + jnp.dot(
                hidden[part], weights[half + part][:, columns], preferred_element_type=F32
            )
        out[:, columns] = total.astype(BF16)


def feed(index, mine, theirs, gain, weights, patterns):
    pairs, rows, width = mine.shape
    count = 2 * pairs * rows
    units = weights[0].shape[1] * len(weights) // 2
    return pl.pallas_call(
        functools.partial(feed_kernel, patterns=patterns),
        out_shape=jax.ShapeDtypeStruct((count, width), BF16),
        in_specs=[SMEM_SPEC] + [VMEM_SPEC] * (3 + len(weights)),
        out_specs=VMEM_SPEC,
        scratch_shapes=[
            pltpu.VMEM((count, width), BF16),
            pltpu.VMEM((len(weights) // 2, count, weights[0].shape[1]), BF16),
        ],
        compiler_params=limit(24),
        cost_estimate=pl.CostEstimate(
            flops=4 * count * width * units, bytes_accessed=4 * width * units, transcendentals=0
        ),
        name="feed",
    )(index, mine, theirs, gain.reshape(1, width), *weights)


def settle_kernel(parts, tokens, gain, after, encoded, spread):
    del after
    total = tokens[...].astype(F32)
    for k in range(parts.shape[0]):
        total = total + parts[k].astype(F32)
    rounded = total.astype(BF16)
    encoded[...] = rounded
    memory = norm_rows(rounded, gain[...]).astype(BF16)
    for k in range(spread.shape[0]):
        spread[k] = memory


def settle(parts, tokens, gain, after):
    count, rows, width = parts.shape
    return pl.pallas_call(
        settle_kernel,
        out_shape=(
            jax.ShapeDtypeStruct((rows, width), BF16),
            jax.ShapeDtypeStruct((count, rows, width), BF16),
        ),
        in_specs=[VMEM_SPEC] * 3 + [HBM_SPEC],
        out_specs=(VMEM_SPEC, VMEM_SPEC),
        compiler_params=limit(8),
        name="settle",
    )(parts, tokens, gain.reshape(1, width), after)


def project_kernel(half, mine, w_key, wkv, w_out, keys, values, w_value, w_last, sems):
    inner = keys.shape[1]
    size = min(256, inner)
    start = pl.multiple_of(half[0] * inner, 128)
    chunks = inner // size
    copies = [
        pltpu.make_async_copy(
            wkv.at[1, :, pl.ds(c * size, size)], w_value.at[:, pl.ds(c * size, size)], sems.at[c]
        )
        for c in range(chunks)
    ]
    last = pltpu.make_async_copy(w_out.at[pl.ds(start, inner)], w_last, sems.at[chunks])
    for copy in copies:
        copy.start()
    last.start()
    for c in range(chunks):
        columns = pl.ds(c * size, size)
        keys[:, columns] = jnp.dot(
            mine[...], w_key[:, columns], preferred_element_type=F32
        ).astype(BF16)
    for c in range(chunks):
        columns = pl.ds(c * size, size)
        copies[c].wait()
        values[:, columns] = jnp.dot(
            mine[...], w_value[:, columns], preferred_element_type=F32
        ).astype(BF16)
    last.wait()


def project(half, mine, w_key, wkv, w_attn_out):
    rows, width = mine.shape
    inner = w_key.shape[1]
    return pl.pallas_call(
        project_kernel,
        out_shape=(
            jax.ShapeDtypeStruct((rows, inner), BF16),
            jax.ShapeDtypeStruct((rows, inner), BF16),
            jax.ShapeDtypeStruct((width, inner), BF16),
            jax.ShapeDtypeStruct((inner, width), BF16),
        ),
        in_specs=[SMEM_SPEC, VMEM_SPEC, VMEM_SPEC, HBM_SPEC, HBM_SPEC],
        out_specs=(VMEM_SPEC,) * 4,
        scratch_shapes=[pltpu.SemaphoreType.DMA((inner // min(256, inner) + 1,))],
        compiler_params=limit(45),
        cost_estimate=pl.CostEstimate(
            flops=4 * rows * width * inner, bytes_accessed=6 * width * inner, transcendentals=0
        ),
        name="project",
    )(half, mine, w_key, wkv, w_attn_out)


def attend_kernel(near_keys, near_values, theirs, query, allowed, w_key, w_value, w_last, out, context):
    rows, inner = near_keys.shape
    width = out.shape[1]
    size = min(256, inner)
    near = allowed[:, :rows] > 0
    far = allowed[:, rows:] > 0
    for c in range(inner // size):
        columns = pl.ds(c * size, size)
        far_keys = jnp.dot(theirs[...], w_key[:, columns], preferred_element_type=F32).astype(BF16)
        far_values = jnp.dot(
            theirs[...], w_value[:, columns], preferred_element_type=F32
        ).astype(BF16)
        keys = jnp.concatenate([near_keys[:, columns], far_keys], axis=0)
        values = jnp.concatenate([near_values[:, columns], far_values], axis=0)
        for h in range(size // DH):
            lanes = slice(h * DH, (h + 1) * DH)
            place = pl.ds(c * size + h * DH, DH)
            scores = lax.dot_general(
                query[:, place],
                keys[:, lanes],
                (((1,), (1,)), ((), ())),
                preferred_element_type=F32,
            ) * DH ** (-0.5)
            near_scores = jnp.where(near, scores[:, :rows], -1e30)
            far_scores = jnp.where(far, scores[:, rows:], -1e30)
            top = jnp.max(jnp.maximum(near_scores, far_scores), axis=1, keepdims=True)
            near_weights = jnp.where(near, jnp.exp(near_scores - top), 0.0)
            far_weights = jnp.where(far, jnp.exp(far_scores - top), 0.0)
            total = jnp.sum(near_weights + far_weights, axis=1, keepdims=True)
            weights = jnp.concatenate([near_weights, far_weights], axis=1).astype(BF16)
            summed = jnp.dot(weights, values[:, lanes], preferred_element_type=F32)
            context[:, place] = (summed * (1.0 / total)).astype(BF16)
    for c in range(width // 256):
        columns = pl.ds(c * 256, 256)
        out[:, columns] = jnp.dot(context[...], w_last[:, columns], preferred_element_type=F32)


def attend(near_keys, near_values, theirs, query, allowed, w_key, w_value, w_last):
    rows, width = theirs.shape
    count, inner = query.shape
    return pl.pallas_call(
        attend_kernel,
        out_shape=jax.ShapeDtypeStruct((count, width), F32),
        in_specs=[VMEM_SPEC] * 8,
        out_specs=VMEM_SPEC,
        scratch_shapes=[pltpu.VMEM((count, inner), BF16)],
        compiler_params=limit(24),
        cost_estimate=pl.CostEstimate(
            flops=4 * rows * width * inner + 8 * count * rows * inner + 2 * count * inner * width,
            bytes_accessed=6 * width * inner,
            transcendentals=2 * count * rows * inner // DH,
        ),
        name="attend",
    )(near_keys, near_values, theirs, query, allowed, w_key, w_value, w_last)


def per_device(
    tokens,
    enc_gain,
    w_in,
    w_out,
    final_gain,
    w_keyval,
    answer_states,
    dec_gain,
    w_query,
    w_attn_out,
    passage_lengths,
    passage_owner,
    answer_lengths,
):
    row_count = tokens.shape[0]
    width = tokens.shape[1]
    answer_count = answer_states.shape[0]
    mp = lax.axis_size("mp")
    psg = lax.axis_size("psg")
    mp_index = lax.axis_index("mp")
    psg_index = lax.axis_index("psg")
    heads = w_query.shape[1] // DH // psg
    inner = heads * DH

    half = jnp.reshape(psg_index, (1,)).astype(jnp.int32)
    index = jnp.reshape(mp_index, (1,)).astype(jnp.int32)
    patterns = [0]
    held = tokens[None]
    weights = []
    step = mp // 2
    while step > 0:
        got = lax.ppermute(held, "mp", [(j, j ^ step) for j in range(mp)])
        after = index if step == mp // 2 else held
        if step == mp // 2:
            weights.append(stage(after, w_in, 1, 0, 2))
        elif step == mp // 4:
            weights.append(stage(after, w_in, 1, 1, 2))
        elif step == 1:
            weights.append(stage(after, w_out, 0, 0, 2))
            weights.append(stage(after, w_out, 0, 1, 2))
        patterns = patterns + [p ^ step for p in patterns]
        if step > 1:
            held = jnp.concatenate([held, got], axis=0)
        step //= 2
    query, w_key, wkv = prepare(half, answer_states, dec_gain, w_query, w_keyval, inner)
    partial_sums = feed(index, held, got, enc_gain, weights, patterns)
    parts = lax.all_to_all(partial_sums.reshape(mp, row_count, width), "mp", 0, 0)
    encoded, spread = settle(parts, tokens, final_gain, query)
    mine = lax.all_to_all(spread, "mp", 0, 0).reshape(mp * row_count, width)
    theirs = swap_psg(mine)
    key_rows = 2 * mp * row_count

    local = jnp.arange(key_rows, dtype=jnp.int32)
    far = local // (mp * row_count)
    block = (local % (mp * row_count)) // row_count
    core = jnp.where(far == 0, psg_index, 1 - psg_index)
    token_index = (block * psg + core) * row_count + local % row_count
    allowed = key_mask(token_index, passage_lengths, passage_owner, answer_lengths, answer_count)
    near_keys, near_values, w_value, w_last = project(half, mine, w_key, wkv, w_attn_out)
    partial_answer = attend(
        near_keys, near_values, theirs, query, allowed.astype(jnp.int32), w_key, w_value, w_last
    )

    out_count = answer_count // mp
    small = out_count // psg
    halves = partial_answer.reshape(mp, psg, small, width)
    keep = lax.dynamic_index_in_dim(halves, psg_index, 1, False)
    give = lax.dynamic_index_in_dim(halves, 1 - psg_index, 1, False)
    chip_sum = (keep + swap_psg(give)).astype(jnp.bfloat16)
    answer_parts = lax.all_to_all(chip_sum, "mp", 0, 0)
    own_start = mp_index * out_count + psg_index * small
    own_answer = lax.dynamic_slice_in_dim(answer_states, own_start, small, 0).astype(jnp.float32)
    piece = (own_answer + jnp.sum(answer_parts.astype(jnp.float32), axis=0)).astype(jnp.bfloat16)
    other = swap_psg(piece)
    first = jnp.where(psg_index == 0, piece, other)
    second = jnp.where(psg_index == 0, other, piece)
    return (encoded, jnp.concatenate([first, second], axis=0))


def solution(mesh):
    placed = (
        P(("groups", "mp", "psg"), None),
        P(),
        P(None, "mp"),
        P("mp", None),
        P(),
        P(None, None, "mp"),
        P("groups", None),
        P(),
        P(None, "mp"),
        P("mp", None),
        P("groups"),
        P("groups"),
        P("groups"),
    )
    return jax.shard_map(
        per_device,
        mesh=mesh,
        in_specs=placed,
        out_specs=(P(("groups", "mp", "psg"), None), P(("groups", "mp"), None)),
        check_vma=False,
    )
```

```python
import functools

import jax
import jax.numpy as jnp
from jax import lax
from jax.experimental import pallas as pl
from jax.experimental.pallas import tpu as pltpu
from jax.sharding import PartitionSpec as P


DH = 128
P_SLOT = 16


eps = 1e-06


def norm_rows(states, gain):
    wide = states.astype(jnp.float32)
    factor = lax.rsqrt(jnp.mean(wide * wide, axis=-1, keepdims=True) + eps)
    return wide * factor * gain


def key_mask(token_index, passage_lengths, passage_owner, answer_lengths, answer_count):
    passage = token_index // P_SLOT
    place = token_index % P_SLOT
    count = passage_lengths.shape[0]
    match = passage[:, None] == jnp.arange(count, dtype=jnp.int32)[None, :]
    token_length = jnp.sum(jnp.where(match, passage_lengths[None, :], 0), axis=1)
    token_owner = jnp.sum(jnp.where(match, passage_owner[None, :], 0), axis=1)
    number = answer_lengths.shape[0]
    order = jnp.arange(number, dtype=jnp.int32)
    ends = jnp.sum(jnp.where(order[:, None] <= order[None, :], answer_lengths[:, None], 0), axis=0)
    answer_index = jnp.arange(answer_count, dtype=jnp.int32)
    question = jnp.sum((answer_index[:, None] >= ends[None, :]).astype(jnp.int32), axis=1)
    return (place < token_length)[None, :] & (token_owner[None, :] == question[:, None])


def swap_psg(x):
    return lax.ppermute(x, "psg", [(0, 1), (1, 0)])


BF16 = jnp.bfloat16
F32 = jnp.float32
SMEM_SPEC = pl.BlockSpec(memory_space=pltpu.SMEM)
VMEM_SPEC = pl.BlockSpec(memory_space=pltpu.VMEM)
HBM_SPEC = pl.BlockSpec(memory_space=pltpu.HBM)


def limit(mib):
    return pltpu.CompilerParams(vmem_limit_bytes=mib << 20)


def ask_kernel(half, states, gain, w_query, query, scr, sems):
    inner = query.shape[1]
    size = scr.shape[2]
    start = pl.multiple_of(half[0] * inner, 128)
    copies = [
        pltpu.make_async_copy(
            w_query.at[:, pl.ds(pl.multiple_of(start + c * size, 128), size)],
            scr.at[c],
            sems.at[c],
        )
        for c in range(inner // size)
    ]
    for copy in copies:
        copy.start()
    normed = norm_rows(states[...], gain[...]).astype(BF16)
    for c in range(inner // size):
        copies[c].wait()
        query[:, pl.ds(c * size, size)] = jnp.dot(
            normed, scr[c], preferred_element_type=F32
        ).astype(BF16)


def ask(half, states, gain, w_query, inner):
    count, width = states.shape
    size = min(256, inner)
    return pl.pallas_call(
        ask_kernel,
        out_shape=jax.ShapeDtypeStruct((count, inner), BF16),
        in_specs=[SMEM_SPEC, VMEM_SPEC, VMEM_SPEC, HBM_SPEC],
        out_specs=VMEM_SPEC,
        scratch_shapes=[
            pltpu.VMEM((inner // size, width, size), BF16),
            pltpu.SemaphoreType.DMA((inner // size,)),
        ],
        compiler_params=limit(52),
        cost_estimate=pl.CostEstimate(
            flops=1 << 30, bytes_accessed=2 * width * inner, transcendentals=0
        ),
        name="ask",
    )(half, states, gain.reshape(1, width), w_query)


def prepare_kernel(half, w_keyval, first_key, last_key, w_value, scr, sems):
    inner = w_value.shape[1]
    blocks = scr.shape[0]
    start = pl.multiple_of(half[0] * inner, 128)
    copies = [
        pltpu.make_async_copy(
            w_keyval.at[pl.ds(b * 128, 128), :, pl.ds(start, inner)], scr.at[b], sems.at[b]
        )
        for b in range(blocks)
    ]
    for copy in copies:
        copy.start()
    row = lax.broadcasted_iota(jnp.int32, (256, 256), 0)
    column = lax.broadcasted_iota(jnp.int32, (256, 256), 1)
    source = jnp.where(row < 128, 2 * row, 2 * (row - 128) + 1)
    pick = jnp.where(column == source, 1.0, 0.0).astype(BF16)
    for b in range(blocks):
        rows = pl.ds(b * 128, 128)
        copies[b].wait()
        for s in range(0, inner, 128):
            mixed = scr[b, :, :, pl.ds(s, 128)].reshape(256, 128)
            apart = jnp.dot(pick, mixed, preferred_element_type=F32).astype(BF16)
            if s < inner // 2:
                first_key[rows, pl.ds(s, 128)] = apart[:128]
            else:
                last_key[rows, pl.ds(s - inner // 2, 128)] = apart[:128]
            w_value[rows, pl.ds(s, 128)] = apart[128:]


def prepare(half, w_keyval, inner):
    width = w_keyval.shape[0]
    return pl.pallas_call(
        prepare_kernel,
        out_shape=(
            jax.ShapeDtypeStruct((width, inner // 2), BF16),
            jax.ShapeDtypeStruct((width, inner // 2), BF16),
            jax.ShapeDtypeStruct((width, inner), BF16),
        ),
        in_specs=[SMEM_SPEC, HBM_SPEC],
        out_specs=(VMEM_SPEC,) * 3,
        scratch_shapes=[
            pltpu.VMEM((width // 128, 128, 2, inner), BF16),
            pltpu.SemaphoreType.DMA((width // 128,)),
        ],
        compiler_params=limit(51),
        cost_estimate=pl.CostEstimate(
            flops=4 * width * 256 * inner, bytes_accessed=8 * width * inner, transcendentals=0
        ),
        name="prepare",
    )(half, w_keyval)


def stage_kernel(after, whole, out, sems, *, axis, start):
    del after
    size = out.shape[axis]
    number = sems.shape[0]
    step = size // number
    copies = []
    for k in range(number):
        if axis == 0:
            source = whole.at[pl.ds(start + k * step, step)]
            target = out.at[pl.ds(k * step, step)]
        else:
            source = whole.at[:, pl.ds(start + k * step, step)]
            target = out.at[:, pl.ds(k * step, step)]
        copies.append(pltpu.make_async_copy(source, target, sems.at[k]))
    for copy in copies:
        copy.start()
    for copy in copies:
        copy.wait()


def stage(after, whole, axis, part, parts):
    shape = list(whole.shape)
    shape[axis] //= parts
    return pl.pallas_call(
        functools.partial(stage_kernel, axis=axis, start=part * shape[axis]),
        out_shape=jax.ShapeDtypeStruct(tuple(shape), BF16),
        in_specs=[SMEM_SPEC, HBM_SPEC],
        out_specs=VMEM_SPEC,
        scratch_shapes=[pltpu.SemaphoreType.DMA((4,))],
        compiler_params=limit(44),
        cost_estimate=pl.CostEstimate(
            flops=1 << 30, bytes_accessed=4 * shape[0] * shape[1], transcendentals=0
        ),
        name="stage",
    )(after, whole)


def feed_kernel(index, mine, theirs, gain, first_in, last_in, first_out, w_out, out, normed, hidden, last_out, sems, *, patterns):
    pairs, rows, width = mine.shape
    units = first_in.shape[1]
    number = sems.shape[0]
    step = width // number
    copies = [
        pltpu.make_async_copy(
            w_out.at[pl.ds(units, units), pl.ds(k * step, step)],
            last_out.at[:, pl.ds(k * step, step)],
            sems.at[k],
        )
        for k in range(number)
    ]
    for copy in copies:
        copy.start()
    size = min(256, units)
    weight = gain[...]
    for k in range(2 * pairs):
        place = pl.multiple_of((index[0] ^ patterns[k]) * rows, rows)
        states = mine[k] if k < pairs else theirs[k - pairs]
        normed[pl.ds(place, rows)] = norm_rows(states, weight).astype(BF16)
    for part, w_in in enumerate((first_in, last_in)):
        for c in range(units // size):
            columns = pl.ds(c * size, size)
            hidden[part, :, columns] = jnp.maximum(
                jnp.dot(normed[...], w_in[:, columns], preferred_element_type=F32), 0.0
            ).astype(BF16)
    for c in range(number):
        columns = pl.ds(c * step, step)
        total = jnp.dot(hidden[0], first_out[:, columns], preferred_element_type=F32)
        copies[c].wait()
        total = total + jnp.dot(hidden[1], last_out[:, columns], preferred_element_type=F32)
        out[:, columns] = total.astype(BF16)


def feed(index, mine, theirs, gain, first_in, last_in, first_out, w_out, patterns):
    pairs, rows, width = mine.shape
    count = 2 * pairs * rows
    units = first_in.shape[1]
    return pl.pallas_call(
        functools.partial(feed_kernel, patterns=patterns),
        out_shape=jax.ShapeDtypeStruct((count, width), BF16),
        in_specs=[SMEM_SPEC] + [VMEM_SPEC] * 6 + [HBM_SPEC],
        out_specs=VMEM_SPEC,
        scratch_shapes=[
            pltpu.VMEM((count, width), BF16),
            pltpu.VMEM((2, count, units), BF16),
            pltpu.VMEM((units, width), BF16),
            pltpu.SemaphoreType.DMA((width // 256,)),
        ],
        compiler_params=limit(37),
        cost_estimate=pl.CostEstimate(
            flops=8 * count * width * units, bytes_accessed=8 * width * units, transcendentals=0
        ),
        name="feed",
    )(index, mine, theirs, gain.reshape(1, width), first_in, last_in, first_out, w_out)


def settle_kernel(parts, tokens, gain, encoded, spread):
    total = tokens[...].astype(F32)
    for k in range(parts.shape[0]):
        total = total + parts[k].astype(F32)
    rounded = total.astype(BF16)
    encoded[...] = rounded
    memory = norm_rows(rounded, gain[...]).astype(BF16)
    for k in range(spread.shape[0]):
        spread[k] = memory


def settle(parts, tokens, gain):
    count, rows, width = parts.shape
    return pl.pallas_call(
        settle_kernel,
        out_shape=(
            jax.ShapeDtypeStruct((rows, width), BF16),
            jax.ShapeDtypeStruct((count, rows, width), BF16),
        ),
        in_specs=[VMEM_SPEC] * 3,
        out_specs=(VMEM_SPEC, VMEM_SPEC),
        compiler_params=limit(8),
        name="settle",
    )(parts, tokens, gain.reshape(1, width))


def project_kernel(half, mine, first_key, last_key, value, w_out, keys, values, first_value, last_value, w_last, sems):
    inner = keys.shape[1]
    part = inner // 2
    start = pl.multiple_of(half[0] * inner, 128)
    copies = [
        pltpu.make_async_copy(value.at[:, pl.ds(0, part)], first_value, sems.at[0]),
        pltpu.make_async_copy(value.at[:, pl.ds(part, part)], last_value, sems.at[1]),
    ]
    last = pltpu.make_async_copy(w_out.at[pl.ds(start, inner)], w_last, sems.at[2])
    for copy in copies:
        copy.start()
    last.start()
    size = min(256, part)
    for k, w_key in enumerate((first_key, last_key)):
        for c in range(part // size):
            keys[:, pl.ds(k * part + c * size, size)] = jnp.dot(
                mine[...], w_key[:, pl.ds(c * size, size)], preferred_element_type=F32
            ).astype(BF16)
    for k, w_value in enumerate((first_value, last_value)):
        copies[k].wait()
        for c in range(part // size):
            values[:, pl.ds(k * part + c * size, size)] = jnp.dot(
                mine[...], w_value[:, pl.ds(c * size, size)], preferred_element_type=F32
            ).astype(BF16)
    last.wait()


def project(half, mine, first_key, last_key, value, w_attn_out):
    rows, width = mine.shape
    inner = value.shape[1]
    return pl.pallas_call(
        project_kernel,
        out_shape=(
            jax.ShapeDtypeStruct((rows, inner), BF16),
            jax.ShapeDtypeStruct((rows, inner), BF16),
            jax.ShapeDtypeStruct((width, inner // 2), BF16),
            jax.ShapeDtypeStruct((width, inner // 2), BF16),
            jax.ShapeDtypeStruct((inner, width), BF16),
        ),
        in_specs=[SMEM_SPEC] + [VMEM_SPEC] * 3 + [HBM_SPEC, HBM_SPEC],
        out_specs=(VMEM_SPEC,) * 5,
        scratch_shapes=[pltpu.SemaphoreType.DMA((3,))],
        compiler_params=limit(46),
        cost_estimate=pl.CostEstimate(
            flops=4 * rows * width * inner, bytes_accessed=6 * width * inner, transcendentals=0
        ),
        name="project",
    )(half, mine, first_key, last_key, value, w_attn_out)


def attend_kernel(near_keys, near_values, theirs, query, allowed, first_key, last_key, first_value, last_value, w_last, out, context):
    rows, inner = near_keys.shape
    width = out.shape[1]
    part = inner // 2
    size = min(256, part)
    near = allowed[:, :rows] > 0
    far = allowed[:, rows:] > 0
    for c in range(inner // size):
        columns = pl.ds(c * size, size)
        w_key = first_key if c * size < part else last_key
        w_value = first_value if c * size < part else last_value
        local = pl.ds(c * size % part, size)
        far_keys = jnp.dot(theirs[...], w_key[:, local], preferred_element_type=F32).astype(BF16)
        far_values = jnp.dot(
            theirs[...], w_value[:, local], preferred_element_type=F32
        ).astype(BF16)
        keys = jnp.concatenate([near_keys[:, columns], far_keys], axis=0)
        values = jnp.concatenate([near_values[:, columns], far_values], axis=0)
        for h in range(size // DH):
            lanes = slice(h * DH, (h + 1) * DH)
            place = pl.ds(c * size + h * DH, DH)
            scores = lax.dot_general(
                query[:, place],
                keys[:, lanes],
                (((1,), (1,)), ((), ())),
                preferred_element_type=F32,
            ) * DH ** (-0.5)
            near_scores = jnp.where(near, scores[:, :rows], -1e30)
            far_scores = jnp.where(far, scores[:, rows:], -1e30)
            top = jnp.max(jnp.maximum(near_scores, far_scores), axis=1, keepdims=True)
            near_weights = jnp.where(near, jnp.exp(near_scores - top), 0.0)
            far_weights = jnp.where(far, jnp.exp(far_scores - top), 0.0)
            total = jnp.sum(near_weights + far_weights, axis=1, keepdims=True)
            weights = jnp.concatenate([near_weights, far_weights], axis=1).astype(BF16)
            summed = jnp.dot(weights, values[:, lanes], preferred_element_type=F32)
            context[:, place] = (summed * (1.0 / total)).astype(BF16)
    for c in range(width // 256):
        columns = pl.ds(c * 256, 256)
        out[:, columns] = jnp.dot(context[...], w_last[:, columns], preferred_element_type=F32)


def attend(near_keys, near_values, theirs, query, allowed, weights, w_last):
    rows, width = theirs.shape
    count, inner = query.shape
    return pl.pallas_call(
        attend_kernel,
        out_shape=jax.ShapeDtypeStruct((count, width), F32),
        in_specs=[VMEM_SPEC] * 10,
        out_specs=VMEM_SPEC,
        scratch_shapes=[pltpu.VMEM((count, inner), BF16)],
        compiler_params=limit(24),
        cost_estimate=pl.CostEstimate(
            flops=4 * rows * width * inner + 8 * count * rows * inner + 2 * count * inner * width,
            bytes_accessed=6 * width * inner,
            transcendentals=2 * count * rows * inner // DH,
        ),
        name="attend",
    )(near_keys, near_values, theirs, query, allowed, *weights, w_last)


def per_device(
    tokens,
    enc_gain,
    w_in,
    w_out,
    final_gain,
    w_keyval,
    answer_states,
    dec_gain,
    w_query,
    w_attn_out,
    passage_lengths,
    passage_owner,
    answer_lengths,
):
    row_count = tokens.shape[0]
    width = tokens.shape[1]
    answer_count = answer_states.shape[0]
    mp = lax.axis_size("mp")
    psg = lax.axis_size("psg")
    mp_index = lax.axis_index("mp")
    psg_index = lax.axis_index("psg")
    heads = w_query.shape[1] // DH // psg
    inner = heads * DH

    half = jnp.reshape(psg_index, (1,)).astype(jnp.int32)
    index = jnp.reshape(mp_index, (1,)).astype(jnp.int32)
    patterns = [0]
    held = tokens[None]
    step = mp // 2
    while step > 0:
        got = lax.ppermute(held, "mp", [(j, j ^ step) for j in range(mp)])
        patterns = patterns + [p ^ step for p in patterns]
        if step > 1:
            held = jnp.concatenate([held, got], axis=0)
        step //= 2
    first_in = stage(index, w_in, 1, 0, 2)
    last_in = stage(index, w_in, 1, 1, 2)
    first_out = stage(index, w_out, 0, 0, 2)
    query = ask(half, answer_states, dec_gain, w_query, inner)
    first_key, last_key, value = prepare(half, w_keyval, inner)
    partial_sums = feed(index, held, got, enc_gain, first_in, last_in, first_out, w_out, patterns)
    parts = lax.all_to_all(partial_sums.reshape(mp, row_count, width), "mp", 0, 0)
    encoded, spread = settle(parts, tokens, final_gain)
    mine = lax.all_to_all(spread, "mp", 0, 0)
    mine = mine.reshape(mp * row_count, width)
    theirs = swap_psg(mine)
    key_rows = 2 * mp * row_count

    local = jnp.arange(key_rows, dtype=jnp.int32)
    far = local // (mp * row_count)
    block = (local % (mp * row_count)) // row_count
    core = jnp.where(far == 0, psg_index, 1 - psg_index)
    token_index = (block * psg + core) * row_count + local % row_count
    allowed = key_mask(token_index, passage_lengths, passage_owner, answer_lengths, answer_count)
    near_keys, near_values, first_value, last_value, w_last = project(
        half, mine, first_key, last_key, value, w_attn_out
    )
    partial_answer = attend(
        near_keys,
        near_values,
        theirs,
        query,
        allowed.astype(jnp.int32),
        (first_key, last_key, first_value, last_value),
        w_last,
    )

    out_count = answer_count // mp
    small = out_count // psg
    halves = partial_answer.reshape(mp, psg, small, width)
    keep = lax.dynamic_index_in_dim(halves, psg_index, 1, False)
    give = lax.dynamic_index_in_dim(halves, 1 - psg_index, 1, False)
    chip_sum = (keep + swap_psg(give)).astype(jnp.bfloat16)
    answer_parts = lax.all_to_all(chip_sum, "mp", 0, 0)
    own_start = mp_index * out_count + psg_index * small
    own_answer = lax.dynamic_slice_in_dim(answer_states, own_start, small, 0).astype(jnp.float32)
    piece = (own_answer + jnp.sum(answer_parts.astype(jnp.float32), axis=0)).astype(jnp.bfloat16)
    other = swap_psg(piece)
    first = jnp.where(psg_index == 0, piece, other)
    second = jnp.where(psg_index == 0, other, piece)
    return (encoded, jnp.concatenate([first, second], axis=0))


def solution(mesh):
    placed = (
        P(("groups", "mp", "psg"), None),
        P(),
        P(None, "mp"),
        P("mp", None),
        P(),
        P(None, None, "mp"),
        P("groups", None),
        P(),
        P(None, "mp"),
        P("mp", None),
        P("groups"),
        P("groups"),
        P("groups"),
    )
    return jax.shard_map(
        per_device,
        mesh=mesh,
        in_specs=placed,
        out_specs=(P(("groups", "mp", "psg"), None), P(("groups", "mp"), None)),
        check_vma=False,
    )
```

```python
import functools

import jax
import jax.numpy as jnp
from jax import lax
from jax.experimental import pallas as pl
from jax.experimental.pallas import tpu as pltpu
from jax.sharding import PartitionSpec as P


DH = 128
P_SLOT = 16


eps = 1e-06


def norm_rows(states, gain):
    wide = states.astype(jnp.float32)
    factor = lax.rsqrt(jnp.mean(wide * wide, axis=-1, keepdims=True) + eps)
    return wide * factor * gain


def key_mask(token_index, passage_lengths, passage_owner, answer_lengths, answer_count):
    passage = token_index // P_SLOT
    place = token_index % P_SLOT
    count = passage_lengths.shape[0]
    match = passage[:, None] == jnp.arange(count, dtype=jnp.int32)[None, :]
    token_length = jnp.sum(jnp.where(match, passage_lengths[None, :], 0), axis=1)
    token_owner = jnp.sum(jnp.where(match, passage_owner[None, :], 0), axis=1)
    number = answer_lengths.shape[0]
    order = jnp.arange(number, dtype=jnp.int32)
    ends = jnp.sum(jnp.where(order[:, None] <= order[None, :], answer_lengths[:, None], 0), axis=0)
    answer_index = jnp.arange(answer_count, dtype=jnp.int32)
    question = jnp.sum((answer_index[:, None] >= ends[None, :]).astype(jnp.int32), axis=1)
    return (place < token_length)[None, :] & (token_owner[None, :] == question[:, None])


def swap_psg(x):
    return lax.ppermute(x, "psg", [(0, 1), (1, 0)])


BF16 = jnp.bfloat16
F32 = jnp.float32
SMEM_SPEC = pl.BlockSpec(memory_space=pltpu.SMEM)
VMEM_SPEC = pl.BlockSpec(memory_space=pltpu.VMEM)
HBM_SPEC = pl.BlockSpec(memory_space=pltpu.HBM)


def limit(mib):
    return pltpu.CompilerParams(vmem_limit_bytes=mib << 20)


def ask_kernel(half, states, gain, w_query, query, scr, sems):
    inner = query.shape[1]
    size = scr.shape[2]
    start = pl.multiple_of(half[0] * inner, 128)
    copies = [
        pltpu.make_async_copy(
            w_query.at[:, pl.ds(pl.multiple_of(start + c * size, 128), size)],
            scr.at[c],
            sems.at[c],
        )
        for c in range(inner // size)
    ]
    for copy in copies:
        copy.start()
    normed = norm_rows(states[...], gain[...]).astype(BF16)
    for c in range(inner // size):
        copies[c].wait()
        query[:, pl.ds(c * size, size)] = jnp.dot(
            normed, scr[c], preferred_element_type=F32
        ).astype(BF16)


def ask(half, states, gain, w_query, inner):
    count, width = states.shape
    size = min(256, inner)
    return pl.pallas_call(
        ask_kernel,
        out_shape=jax.ShapeDtypeStruct((count, inner), BF16),
        in_specs=[SMEM_SPEC, VMEM_SPEC, VMEM_SPEC, HBM_SPEC],
        out_specs=VMEM_SPEC,
        scratch_shapes=[
            pltpu.VMEM((inner // size, width, size), BF16),
            pltpu.SemaphoreType.DMA((inner // size,)),
        ],
        compiler_params=limit(52),
        cost_estimate=pl.CostEstimate(
            flops=1 << 30, bytes_accessed=2 * width * inner, transcendentals=0
        ),
        name="ask",
    )(half, states, gain.reshape(1, width), w_query)


def prepare_kernel(half, w_keyval, first_key, last_key, w_value, scr, sems):
    inner = w_value.shape[1]
    blocks = scr.shape[0]
    start = pl.multiple_of(half[0] * inner, 128)
    copies = [
        pltpu.make_async_copy(
            w_keyval.at[pl.ds(b * 128, 128), :, pl.ds(start, inner)], scr.at[b], sems.at[b]
        )
        for b in range(blocks)
    ]
    for copy in copies:
        copy.start()
    row = lax.broadcasted_iota(jnp.int32, (256, 256), 0)
    column = lax.broadcasted_iota(jnp.int32, (256, 256), 1)
    source = jnp.where(row < 128, 2 * row, 2 * (row - 128) + 1)
    pick = jnp.where(column == source, 1.0, 0.0).astype(BF16)
    for b in range(blocks):
        rows = pl.ds(b * 128, 128)
        copies[b].wait()
        for s in range(0, inner, 128):
            mixed = scr[b, :, :, pl.ds(s, 128)].reshape(256, 128)
            apart = jnp.dot(pick, mixed, preferred_element_type=F32).astype(BF16)
            if s < inner // 2:
                first_key[rows, pl.ds(s, 128)] = apart[:128]
            else:
                last_key[rows, pl.ds(s - inner // 2, 128)] = apart[:128]
            w_value[rows, pl.ds(s, 128)] = apart[128:]


def prepare(half, w_keyval, inner):
    width = w_keyval.shape[0]
    return pl.pallas_call(
        prepare_kernel,
        out_shape=(
            jax.ShapeDtypeStruct((width, inner // 2), BF16),
            jax.ShapeDtypeStruct((width, inner // 2), BF16),
            jax.ShapeDtypeStruct((width, inner), BF16),
        ),
        in_specs=[SMEM_SPEC, HBM_SPEC],
        out_specs=(VMEM_SPEC,) * 3,
        scratch_shapes=[
            pltpu.VMEM((width // 128, 128, 2, inner), BF16),
            pltpu.SemaphoreType.DMA((width // 128,)),
        ],
        compiler_params=limit(51),
        cost_estimate=pl.CostEstimate(
            flops=4 * width * 256 * inner, bytes_accessed=8 * width * inner, transcendentals=0
        ),
        name="prepare",
    )(half, w_keyval)


def stage_kernel(after, whole, first, last, sems, *, axis):
    del after
    size = first.shape[axis]
    number = sems.shape[0] // 2
    step = size // number
    copies = []
    for half, out in enumerate((first, last)):
        for k in range(number):
            if axis == 0:
                source = whole.at[pl.ds(half * size + k * step, step)]
                target = out.at[pl.ds(k * step, step)]
            else:
                source = whole.at[:, pl.ds(half * size + k * step, step)]
                target = out.at[:, pl.ds(k * step, step)]
            copies.append(pltpu.make_async_copy(source, target, sems.at[half * number + k]))
    for copy in copies:
        copy.start()
    for copy in copies:
        copy.wait()


def stage(after, whole, axis):
    shape = list(whole.shape)
    shape[axis] //= 2
    part = jax.ShapeDtypeStruct(tuple(shape), BF16)
    return pl.pallas_call(
        functools.partial(stage_kernel, axis=axis),
        out_shape=(part, part),
        in_specs=[SMEM_SPEC, HBM_SPEC],
        out_specs=(VMEM_SPEC, VMEM_SPEC),
        scratch_shapes=[pltpu.SemaphoreType.DMA((8,))],
        compiler_params=limit(42),
        cost_estimate=pl.CostEstimate(
            flops=1 << 30, bytes_accessed=8 * shape[0] * shape[1], transcendentals=0
        ),
        name="stage",
    )(after, whole)


def feed_kernel(index, mine, theirs, gain, *refs, patterns):
    *weights, out, normed, hidden = refs
    half = len(weights) // 2
    pairs, rows, width = mine.shape
    units = weights[0].shape[1]
    size = min(256, units)
    weight = gain[...]
    for k in range(2 * pairs):
        place = pl.multiple_of((index[0] ^ patterns[k]) * rows, rows)
        states = mine[k] if k < pairs else theirs[k - pairs]
        normed[pl.ds(place, rows)] = norm_rows(states, weight).astype(BF16)
    for part in range(half):
        for c in range(units // size):
            columns = pl.ds(c * size, size)
            hidden[part, :, columns] = jnp.maximum(
                jnp.dot(normed[...], weights[part][:, columns], preferred_element_type=F32), 0.0
            ).astype(BF16)
    for c in range(width // 256):
        columns = pl.ds(c * 256, 256)
        total = jnp.dot(hidden[0], weights[half][:, columns], preferred_element_type=F32)
        for part in range(1, half):
            total = total + jnp.dot(
                hidden[part], weights[half + part][:, columns], preferred_element_type=F32
            )
        out[:, columns] = total.astype(BF16)


def feed(index, mine, theirs, gain, weights, patterns):
    pairs, rows, width = mine.shape
    count = 2 * pairs * rows
    units = weights[0].shape[1] * len(weights) // 2
    return pl.pallas_call(
        functools.partial(feed_kernel, patterns=patterns),
        out_shape=jax.ShapeDtypeStruct((count, width), BF16),
        in_specs=[SMEM_SPEC] + [VMEM_SPEC] * (3 + len(weights)),
        out_specs=VMEM_SPEC,
        scratch_shapes=[
            pltpu.VMEM((count, width), BF16),
            pltpu.VMEM((len(weights) // 2, count, weights[0].shape[1]), BF16),
        ],
        compiler_params=limit(24),
        cost_estimate=pl.CostEstimate(
            flops=4 * count * width * units, bytes_accessed=4 * width * units, transcendentals=0
        ),
        name="feed",
    )(index, mine, theirs, gain.reshape(1, width), *weights)


def settle_kernel(parts, tokens, gain, encoded, spread):
    total = tokens[...].astype(F32)
    for k in range(parts.shape[0]):
        total = total + parts[k].astype(F32)
    rounded = total.astype(BF16)
    encoded[...] = rounded
    memory = norm_rows(rounded, gain[...]).astype(BF16)
    for k in range(spread.shape[0]):
        spread[k] = memory


def settle(parts, tokens, gain):
    count, rows, width = parts.shape
    return pl.pallas_call(
        settle_kernel,
        out_shape=(
            jax.ShapeDtypeStruct((rows, width), BF16),
            jax.ShapeDtypeStruct((count, rows, width), BF16),
        ),
        in_specs=[VMEM_SPEC] * 3,
        out_specs=(VMEM_SPEC, VMEM_SPEC),
        compiler_params=limit(8),
        name="settle",
    )(parts, tokens, gain.reshape(1, width))


def project_kernel(half, mine, first_key, last_key, value, w_out, keys, values, first_value, last_value, w_last, sems):
    inner = keys.shape[1]
    part = inner // 2
    start = pl.multiple_of(half[0] * inner, 128)
    copies = [
        pltpu.make_async_copy(value.at[:, pl.ds(0, part)], first_value, sems.at[0]),
        pltpu.make_async_copy(value.at[:, pl.ds(part, part)], last_value, sems.at[1]),
    ]
    last = pltpu.make_async_copy(w_out.at[pl.ds(start, inner)], w_last, sems.at[2])
    for copy in copies:
        copy.start()
    last.start()
    size = min(256, part)
    for k, w_key in enumerate((first_key, last_key)):
        for c in range(part // size):
            keys[:, pl.ds(k * part + c * size, size)] = jnp.dot(
                mine[...], w_key[:, pl.ds(c * size, size)], preferred_element_type=F32
            ).astype(BF16)
    for k, w_value in enumerate((first_value, last_value)):
        copies[k].wait()
        for c in range(part // size):
            values[:, pl.ds(k * part + c * size, size)] = jnp.dot(
                mine[...], w_value[:, pl.ds(c * size, size)], preferred_element_type=F32
            ).astype(BF16)
    last.wait()


def project(half, mine, first_key, last_key, value, w_attn_out):
    rows, width = mine.shape
    inner = value.shape[1]
    return pl.pallas_call(
        project_kernel,
        out_shape=(
            jax.ShapeDtypeStruct((rows, inner), BF16),
            jax.ShapeDtypeStruct((rows, inner), BF16),
            jax.ShapeDtypeStruct((width, inner // 2), BF16),
            jax.ShapeDtypeStruct((width, inner // 2), BF16),
            jax.ShapeDtypeStruct((inner, width), BF16),
        ),
        in_specs=[SMEM_SPEC] + [VMEM_SPEC] * 3 + [HBM_SPEC, HBM_SPEC],
        out_specs=(VMEM_SPEC,) * 5,
        scratch_shapes=[pltpu.SemaphoreType.DMA((3,))],
        compiler_params=limit(46),
        cost_estimate=pl.CostEstimate(
            flops=4 * rows * width * inner, bytes_accessed=6 * width * inner, transcendentals=0
        ),
        name="project",
    )(half, mine, first_key, last_key, value, w_attn_out)


def attend_kernel(near_keys, near_values, theirs, query, allowed, first_key, last_key, first_value, last_value, w_last, out, context):
    rows, inner = near_keys.shape
    width = out.shape[1]
    part = inner // 2
    size = min(256, part)
    near = allowed[:, :rows] > 0
    far = allowed[:, rows:] > 0
    for c in range(inner // size):
        columns = pl.ds(c * size, size)
        w_key = first_key if c * size < part else last_key
        w_value = first_value if c * size < part else last_value
        local = pl.ds(c * size % part, size)
        far_keys = jnp.dot(theirs[...], w_key[:, local], preferred_element_type=F32).astype(BF16)
        far_values = jnp.dot(
            theirs[...], w_value[:, local], preferred_element_type=F32
        ).astype(BF16)
        keys = jnp.concatenate([near_keys[:, columns], far_keys], axis=0)
        values = jnp.concatenate([near_values[:, columns], far_values], axis=0)
        for h in range(size // DH):
            lanes = slice(h * DH, (h + 1) * DH)
            place = pl.ds(c * size + h * DH, DH)
            scores = lax.dot_general(
                query[:, place],
                keys[:, lanes],
                (((1,), (1,)), ((), ())),
                preferred_element_type=F32,
            ) * DH ** (-0.5)
            near_scores = jnp.where(near, scores[:, :rows], -1e30)
            far_scores = jnp.where(far, scores[:, rows:], -1e30)
            top = jnp.max(jnp.maximum(near_scores, far_scores), axis=1, keepdims=True)
            near_weights = jnp.where(near, jnp.exp(near_scores - top), 0.0)
            far_weights = jnp.where(far, jnp.exp(far_scores - top), 0.0)
            total = jnp.sum(near_weights + far_weights, axis=1, keepdims=True)
            weights = jnp.concatenate([near_weights, far_weights], axis=1).astype(BF16)
            summed = jnp.dot(weights, values[:, lanes], preferred_element_type=F32)
            context[:, place] = (summed * (1.0 / total)).astype(BF16)
    for c in range(width // 256):
        columns = pl.ds(c * 256, 256)
        out[:, columns] = jnp.dot(context[...], w_last[:, columns], preferred_element_type=F32)


def attend(near_keys, near_values, theirs, query, allowed, weights, w_last):
    rows, width = theirs.shape
    count, inner = query.shape
    return pl.pallas_call(
        attend_kernel,
        out_shape=jax.ShapeDtypeStruct((count, width), F32),
        in_specs=[VMEM_SPEC] * 10,
        out_specs=VMEM_SPEC,
        scratch_shapes=[pltpu.VMEM((count, inner), BF16)],
        compiler_params=limit(24),
        cost_estimate=pl.CostEstimate(
            flops=4 * rows * width * inner + 8 * count * rows * inner + 2 * count * inner * width,
            bytes_accessed=6 * width * inner,
            transcendentals=2 * count * rows * inner // DH,
        ),
        name="attend",
    )(near_keys, near_values, theirs, query, allowed, *weights, w_last)


def per_device(
    tokens,
    enc_gain,
    w_in,
    w_out,
    final_gain,
    w_keyval,
    answer_states,
    dec_gain,
    w_query,
    w_attn_out,
    passage_lengths,
    passage_owner,
    answer_lengths,
):
    row_count = tokens.shape[0]
    width = tokens.shape[1]
    answer_count = answer_states.shape[0]
    mp = lax.axis_size("mp")
    psg = lax.axis_size("psg")
    mp_index = lax.axis_index("mp")
    psg_index = lax.axis_index("psg")
    heads = w_query.shape[1] // DH // psg
    inner = heads * DH

    half = jnp.reshape(psg_index, (1,)).astype(jnp.int32)
    index = jnp.reshape(mp_index, (1,)).astype(jnp.int32)
    quarter = mp // 4
    patterns = [0]
    blocks = [tokens[None]]
    for k in (3, 2, 1):
        blocks.append(lax.ppermute(tokens[None], "mp", [(j, j ^ (k * quarter)) for j in range(mp)]))
        patterns.append(k * quarter)
    held = jnp.concatenate(blocks, axis=0)
    step = quarter // 2
    while step > 0:
        got = lax.ppermute(held, "mp", [(j, j ^ step) for j in range(mp)])
        patterns = patterns + [p ^ step for p in patterns]
        if step > 1:
            held = jnp.concatenate([held, got], axis=0)
        step //= 2
    first_in, last_in = stage(index, w_in, 1)
    first_out, last_out = stage(index, w_out, 0)
    query = ask(half, answer_states, dec_gain, w_query, inner)
    first_key, last_key, value = prepare(half, w_keyval, inner)
    partial_sums = feed(
        index, held, got, enc_gain, [first_in, last_in, first_out, last_out], patterns
    )
    parts = lax.all_to_all(partial_sums.reshape(mp, row_count, width), "mp", 0, 0)
    encoded, spread = settle(parts, tokens, final_gain)
    mine = lax.all_to_all(spread, "mp", 0, 0)
    mine = mine.reshape(mp * row_count, width)
    theirs = swap_psg(mine)
    key_rows = 2 * mp * row_count

    local = jnp.arange(key_rows, dtype=jnp.int32)
    far = local // (mp * row_count)
    block = (local % (mp * row_count)) // row_count
    core = jnp.where(far == 0, psg_index, 1 - psg_index)
    token_index = (block * psg + core) * row_count + local % row_count
    allowed = key_mask(token_index, passage_lengths, passage_owner, answer_lengths, answer_count)
    near_keys, near_values, first_value, last_value, w_last = project(
        half, mine, first_key, last_key, value, w_attn_out
    )
    partial_answer = attend(
        near_keys,
        near_values,
        theirs,
        query,
        allowed.astype(jnp.int32),
        (first_key, last_key, first_value, last_value),
        w_last,
    )

    out_count = answer_count // mp
    small = out_count // psg
    halves = partial_answer.reshape(mp, psg, small, width)
    keep = lax.dynamic_index_in_dim(halves, psg_index, 1, False)
    give = lax.dynamic_index_in_dim(halves, 1 - psg_index, 1, False)
    chip_sum = (keep + swap_psg(give)).astype(jnp.bfloat16)
    answer_parts = lax.all_to_all(chip_sum, "mp", 0, 0)
    own_start = mp_index * out_count + psg_index * small
    own_answer = lax.dynamic_slice_in_dim(answer_states, own_start, small, 0).astype(jnp.float32)
    piece = (own_answer + jnp.sum(answer_parts.astype(jnp.float32), axis=0)).astype(jnp.bfloat16)
    other = swap_psg(piece)
    first = jnp.where(psg_index == 0, piece, other)
    second = jnp.where(psg_index == 0, other, piece)
    return (encoded, jnp.concatenate([first, second], axis=0))


def solution(mesh):
    placed = (
        P(("groups", "mp", "psg"), None),
        P(),
        P(None, "mp"),
        P("mp", None),
        P(),
        P(None, None, "mp"),
        P("groups", None),
        P(),
        P(None, "mp"),
        P("mp", None),
        P("groups"),
        P("groups"),
        P("groups"),
    )
    return jax.shard_map(
        per_device,
        mesh=mesh,
        in_specs=placed,
        out_specs=(P(("groups", "mp", "psg"), None), P(("groups", "mp"), None)),
        check_vma=False,
    )
```

```python
import functools

import jax
import jax.numpy as jnp
from jax import lax
from jax.experimental import pallas as pl
from jax.experimental.pallas import tpu as pltpu
from jax.sharding import PartitionSpec as P


DH = 128
P_SLOT = 16


eps = 1e-06


def norm_rows(states, gain):
    wide = states.astype(jnp.float32)
    factor = lax.rsqrt(jnp.mean(wide * wide, axis=-1, keepdims=True) + eps)
    return wide * factor * gain


def key_mask(token_index, answer_index, passage_lengths, passage_owner, answer_lengths):
    passage = token_index // P_SLOT
    place = token_index % P_SLOT
    count = passage_lengths.shape[0]
    match = passage[:, None] == jnp.arange(count, dtype=jnp.int32)[None, :]
    token_length = jnp.sum(jnp.where(match, passage_lengths[None, :], 0), axis=1)
    token_owner = jnp.sum(jnp.where(match, passage_owner[None, :], 0), axis=1)
    number = answer_lengths.shape[0]
    order = jnp.arange(number, dtype=jnp.int32)
    ends = jnp.sum(jnp.where(order[:, None] <= order[None, :], answer_lengths[:, None], 0), axis=0)
    question = jnp.sum((answer_index[:, None] >= ends[None, :]).astype(jnp.int32), axis=1)
    return (place < token_length)[None, :] & (token_owner[None, :] == question[:, None])


def spread_out(x, mp):
    quarter = mp // 4
    patterns = [0]
    blocks = [x[None]]
    for k in (3, 2, 1):
        blocks.append(lax.ppermute(x[None], "mp", [(j, j ^ (k * quarter)) for j in range(mp)]))
        patterns.append(k * quarter)
    held = jnp.concatenate(blocks, axis=0)
    step = quarter // 2
    while step > 0:
        got = lax.ppermute(held, "mp", [(j, j ^ step) for j in range(mp)])
        patterns = patterns + [p ^ step for p in patterns]
        if step > 1:
            held = jnp.concatenate([held, got], axis=0)
        step //= 2
    return held, got, patterns


def swap_psg(x):
    return lax.ppermute(x, "psg", [(0, 1), (1, 0)])


BF16 = jnp.bfloat16
F32 = jnp.float32
SMEM_SPEC = pl.BlockSpec(memory_space=pltpu.SMEM)
VMEM_SPEC = pl.BlockSpec(memory_space=pltpu.VMEM)
HBM_SPEC = pl.BlockSpec(memory_space=pltpu.HBM)


def limit(mib):
    return pltpu.CompilerParams(vmem_limit_bytes=mib << 20)


def ask_kernel(half, states, gain, w_query, value, query, first_value, last_value, scr, sems, *, mp):
    inner = query.shape[1]
    part = first_value.shape[1]
    size = scr.shape[2]
    chunks = inner // size
    start = pl.multiple_of(half[0] * inner, 128)
    copies = [
        pltpu.make_async_copy(
            w_query.at[:, pl.ds(pl.multiple_of(start + c * size, 128), size)],
            scr.at[c],
            sems.at[c],
        )
        for c in range(chunks)
    ]
    others = [
        pltpu.make_async_copy(value.at[:, pl.ds(0, part)], first_value, sems.at[chunks]),
        pltpu.make_async_copy(value.at[:, pl.ds(part, part)], last_value, sems.at[chunks + 1]),
    ]
    for copy in copies + others:
        copy.start()
    normed = norm_rows(states[...], gain[...]).astype(BF16)
    count = states.shape[0]
    small = count // mp // 2
    row = lax.broadcasted_iota(jnp.int32, (count, count), 0)
    column = lax.broadcasted_iota(jnp.int32, (count, count), 1)
    side = half[0] ^ lax.div(row, mp * small)
    source = lax.rem(lax.div(row, small), mp) * (2 * small) + side * small + lax.rem(row, small)
    pick = jnp.where(column == source, 1.0, 0.0).astype(BF16)
    normed = jnp.dot(pick, normed, preferred_element_type=F32).astype(BF16)
    for c in range(chunks):
        copies[c].wait()
        query[:, pl.ds(c * size, size)] = jnp.dot(
            normed, scr[c], preferred_element_type=F32
        ).astype(BF16)
    for copy in others:
        copy.wait()


def ask(half, states, gain, w_query, value, mp):
    count, width = states.shape
    inner = value.shape[1]
    size = min(256, inner)
    return pl.pallas_call(
        functools.partial(ask_kernel, mp=mp),
        out_shape=(
            jax.ShapeDtypeStruct((count, inner), BF16),
            jax.ShapeDtypeStruct((width, inner // 2), BF16),
            jax.ShapeDtypeStruct((width, inner // 2), BF16),
        ),
        in_specs=[SMEM_SPEC, VMEM_SPEC, VMEM_SPEC, HBM_SPEC, HBM_SPEC],
        out_specs=(VMEM_SPEC,) * 3,
        scratch_shapes=[
            pltpu.VMEM((inner // size, width, size), BF16),
            pltpu.SemaphoreType.DMA((inner // size + 2,)),
        ],
        compiler_params=limit(50),
        cost_estimate=pl.CostEstimate(
            flops=1 << 30, bytes_accessed=4 * width * inner, transcendentals=0
        ),
        name="ask",
    )(half, states, gain.reshape(1, width), w_query, value)


def prepare_kernel(half, w_keyval, first_key, last_key, w_value, scr, sems):
    inner = w_value.shape[1]
    blocks = scr.shape[0]
    start = pl.multiple_of(half[0] * inner, 128)
    copies = [
        pltpu.make_async_copy(
            w_keyval.at[pl.ds(b * 128, 128), :, pl.ds(start, inner)], scr.at[b], sems.at[b]
        )
        for b in range(blocks)
    ]
    for copy in copies:
        copy.start()
    row = lax.broadcasted_iota(jnp.int32, (256, 256), 0)
    column = lax.broadcasted_iota(jnp.int32, (256, 256), 1)
    source = jnp.where(row < 128, 2 * row, 2 * (row - 128) + 1)
    pick = jnp.where(column == source, 1.0, 0.0).astype(BF16)
    for b in range(blocks):
        rows = pl.ds(b * 128, 128)
        copies[b].wait()
        for s in range(0, inner, 128):
            mixed = scr[b, :, :, pl.ds(s, 128)].reshape(256, 128)
            apart = jnp.dot(pick, mixed, preferred_element_type=F32).astype(BF16)
            if s < inner // 2:
                first_key[rows, pl.ds(s, 128)] = apart[:128]
            else:
                last_key[rows, pl.ds(s - inner // 2, 128)] = apart[:128]
            w_value[rows, pl.ds(s, 128)] = apart[128:]


def prepare(half, w_keyval, inner):
    width = w_keyval.shape[0]
    return pl.pallas_call(
        prepare_kernel,
        out_shape=(
            jax.ShapeDtypeStruct((width, inner // 2), BF16),
            jax.ShapeDtypeStruct((width, inner // 2), BF16),
            jax.ShapeDtypeStruct((width, inner), BF16),
        ),
        in_specs=[SMEM_SPEC, HBM_SPEC],
        out_specs=(VMEM_SPEC,) * 3,
        scratch_shapes=[
            pltpu.VMEM((width // 128, 128, 2, inner), BF16),
            pltpu.SemaphoreType.DMA((width // 128,)),
        ],
        compiler_params=limit(51),
        cost_estimate=pl.CostEstimate(
            flops=4 * width * 256 * inner, bytes_accessed=8 * width * inner, transcendentals=0
        ),
        name="prepare",
    )(half, w_keyval)


def stage_kernel(after, whole, first, last, sems, *, axis):
    del after
    size = first.shape[axis]
    number = sems.shape[0] // 2
    step = size // number
    copies = []
    for half, out in enumerate((first, last)):
        for k in range(number):
            if axis == 0:
                source = whole.at[pl.ds(half * size + k * step, step)]
                target = out.at[pl.ds(k * step, step)]
            else:
                source = whole.at[:, pl.ds(half * size + k * step, step)]
                target = out.at[:, pl.ds(k * step, step)]
            copies.append(pltpu.make_async_copy(source, target, sems.at[half * number + k]))
    for copy in copies:
        copy.start()
    for copy in copies:
        copy.wait()


def stage(after, whole, axis):
    shape = list(whole.shape)
    shape[axis] //= 2
    part = jax.ShapeDtypeStruct(tuple(shape), BF16)
    return pl.pallas_call(
        functools.partial(stage_kernel, axis=axis),
        out_shape=(part, part),
        in_specs=[SMEM_SPEC, HBM_SPEC],
        out_specs=(VMEM_SPEC, VMEM_SPEC),
        scratch_shapes=[pltpu.SemaphoreType.DMA((8,))],
        compiler_params=limit(42),
        cost_estimate=pl.CostEstimate(
            flops=1 << 30, bytes_accessed=8 * shape[0] * shape[1], transcendentals=0
        ),
        name="stage",
    )(after, whole)


def feed_kernel(index, mine, theirs, gain, *refs, patterns):
    *weights, out, normed, hidden = refs
    half = len(weights) // 2
    pairs, rows, width = mine.shape
    units = weights[0].shape[1]
    size = min(256, units)
    weight = gain[...]
    for k in range(2 * pairs):
        place = pl.multiple_of((index[0] ^ patterns[k]) * rows, rows)
        states = mine[k] if k < pairs else theirs[k - pairs]
        normed[pl.ds(place, rows)] = norm_rows(states, weight).astype(BF16)
    for part in range(half):
        for c in range(units // size):
            columns = pl.ds(c * size, size)
            hidden[part, :, columns] = jnp.maximum(
                jnp.dot(normed[...], weights[part][:, columns], preferred_element_type=F32), 0.0
            ).astype(BF16)
    for c in range(width // 256):
        columns = pl.ds(c * 256, 256)
        total = jnp.dot(hidden[0], weights[half][:, columns], preferred_element_type=F32)
        for part in range(1, half):
            total = total + jnp.dot(
                hidden[part], weights[half + part][:, columns], preferred_element_type=F32
            )
        out[:, columns] = total.astype(BF16)


def feed(index, mine, theirs, gain, weights, patterns):
    pairs, rows, width = mine.shape
    count = 2 * pairs * rows
    units = weights[0].shape[1] * len(weights) // 2
    return pl.pallas_call(
        functools.partial(feed_kernel, patterns=patterns),
        out_shape=jax.ShapeDtypeStruct((count, width), BF16),
        in_specs=[SMEM_SPEC] + [VMEM_SPEC] * (3 + len(weights)),
        out_specs=VMEM_SPEC,
        scratch_shapes=[
            pltpu.VMEM((count, width), BF16),
            pltpu.VMEM((len(weights) // 2, count, weights[0].shape[1]), BF16),
        ],
        compiler_params=limit(24),
        cost_estimate=pl.CostEstimate(
            flops=4 * count * width * units, bytes_accessed=4 * width * units, transcendentals=0
        ),
        name="feed",
    )(index, mine, theirs, gain.reshape(1, width), *weights)


def settle_kernel(parts, tokens, gain, after, encoded, memory):
    del after
    total = tokens[...].astype(F32)
    for k in range(parts.shape[0]):
        total = total + parts[k].astype(F32)
    rounded = total.astype(BF16)
    encoded[...] = rounded
    memory[...] = norm_rows(rounded, gain[...]).astype(BF16)


def settle(parts, tokens, gain, after):
    _, rows, width = parts.shape
    return pl.pallas_call(
        settle_kernel,
        out_shape=(
            jax.ShapeDtypeStruct((rows, width), BF16),
            jax.ShapeDtypeStruct((rows, width), BF16),
        ),
        in_specs=[VMEM_SPEC] * 3 + [HBM_SPEC],
        out_specs=(VMEM_SPEC, VMEM_SPEC),
        compiler_params=limit(8),
        name="settle",
    )(parts, tokens, gain.reshape(1, width), after)


def project_kernel(half, mine, theirs, first_key, last_key, first_value, last_value, w_out, keys, values, w_last, sems):
    inner = keys.shape[1]
    part = inner // 2
    start = pl.multiple_of(half[0] * inner, 128)
    number = sems.shape[0]
    step = inner // number
    copies = [
        pltpu.make_async_copy(
            w_out.at[pl.ds(pl.multiple_of(start + k * step, 64), step)],
            w_last.at[pl.ds(k * step, step)],
            sems.at[k],
        )
        for k in range(number)
    ]
    for copy in copies:
        copy.start()
    rows = jnp.concatenate([mine[...], theirs[...]], axis=0)
    size = min(256, part)
    for k, w_key in enumerate((first_key, last_key)):
        for c in range(part // size):
            keys[:, pl.ds(k * part + c * size, size)] = jnp.dot(
                rows, w_key[:, pl.ds(c * size, size)], preferred_element_type=F32
            ).astype(BF16)
    for k, w_value in enumerate((first_value, last_value)):
        for c in range(part // size):
            values[:, pl.ds(k * part + c * size, size)] = jnp.dot(
                rows, w_value[:, pl.ds(c * size, size)], preferred_element_type=F32
            ).astype(BF16)
    for copy in copies:
        copy.wait()


def project(half, mine, theirs, weights, w_attn_out):
    rows, width = mine.shape
    inner = 2 * weights[0].shape[1]
    return pl.pallas_call(
        project_kernel,
        out_shape=(
            jax.ShapeDtypeStruct((2 * rows, inner), BF16),
            jax.ShapeDtypeStruct((2 * rows, inner), BF16),
            jax.ShapeDtypeStruct((inner, width), BF16),
        ),
        in_specs=[SMEM_SPEC] + [VMEM_SPEC] * 6 + [HBM_SPEC],
        out_specs=(VMEM_SPEC,) * 3,
        scratch_shapes=[pltpu.SemaphoreType.DMA((4,))],
        compiler_params=limit(46),
        cost_estimate=pl.CostEstimate(
            flops=8 * rows * width * inner, bytes_accessed=6 * width * inner, transcendentals=0
        ),
        name="project",
    )(half, mine, theirs, *weights, w_attn_out)


def attend_kernel(near_keys, near_values, mine, theirs, query, allowed, first_key, last_key, first_value, last_value, w_last, keep, give, context):
    rows, inner = near_keys.shape
    width = keep.shape[1]
    part = inner // 2
    size = min(256, part)
    late = jnp.concatenate([mine[...], theirs[...]], axis=0)
    near = allowed[:, :rows] > 0
    far = allowed[:, rows:] > 0
    for c in range(inner // size):
        columns = pl.ds(c * size, size)
        w_key = first_key if c * size < part else last_key
        w_value = first_value if c * size < part else last_value
        local = pl.ds(c * size % part, size)
        far_keys = jnp.dot(late, w_key[:, local], preferred_element_type=F32).astype(BF16)
        far_values = jnp.dot(late, w_value[:, local], preferred_element_type=F32).astype(BF16)
        keys = jnp.concatenate([near_keys[:, columns], far_keys], axis=0)
        values = jnp.concatenate([near_values[:, columns], far_values], axis=0)
        for h in range(size // DH):
            lanes = slice(h * DH, (h + 1) * DH)
            place = pl.ds(c * size + h * DH, DH)
            scores = lax.dot_general(
                query[:, place],
                keys[:, lanes],
                (((1,), (1,)), ((), ())),
                preferred_element_type=F32,
            ) * DH ** (-0.5)
            near_scores = jnp.where(near, scores[:, :rows], -1e30)
            far_scores = jnp.where(far, scores[:, rows:], -1e30)
            top = jnp.max(jnp.maximum(near_scores, far_scores), axis=1, keepdims=True)
            near_weights = jnp.where(near, jnp.exp(near_scores - top), 0.0)
            far_weights = jnp.where(far, jnp.exp(far_scores - top), 0.0)
            total = jnp.sum(near_weights + far_weights, axis=1, keepdims=True)
            weights = jnp.concatenate([near_weights, far_weights], axis=1).astype(BF16)
            summed = jnp.dot(weights, values[:, lanes], preferred_element_type=F32)
            context[:, place] = (summed * (1.0 / total)).astype(BF16)
    for c in range(width // 256):
        columns = pl.ds(c * 256, 256)
        result = jnp.dot(context[...], w_last[:, columns], preferred_element_type=F32)
        keep[:, columns] = result[: keep.shape[0]]
        give[:, columns] = result[keep.shape[0] :]


def attend(near_keys, near_values, mine, theirs, query, allowed, weights, w_last):
    rows = near_keys.shape[0]
    width = mine.shape[1]
    count, inner = query.shape
    return pl.pallas_call(
        attend_kernel,
        out_shape=(jax.ShapeDtypeStruct((count // 2, width), F32),) * 2,
        in_specs=[VMEM_SPEC] * 11,
        out_specs=(VMEM_SPEC, VMEM_SPEC),
        scratch_shapes=[pltpu.VMEM((count, inner), BF16)],
        compiler_params=limit(24),
        cost_estimate=pl.CostEstimate(
            flops=4 * rows * width * inner + 8 * count * rows * inner + 2 * count * inner * width,
            bytes_accessed=6 * width * inner,
            transcendentals=2 * count * rows * inner // DH,
        ),
        name="attend",
    )(near_keys, near_values, mine, theirs, query, allowed, *weights, w_last)


def finish_kernel(index, half, parts, states, piece):
    mp, small, _ = parts.shape
    start = index[0] * (2 * small) + half[0] * small
    row = lax.broadcasted_iota(jnp.int32, (small, states.shape[0]), 0)
    column = lax.broadcasted_iota(jnp.int32, (small, states.shape[0]), 1)
    pick = jnp.where(column == row + start, 1.0, 0.0).astype(BF16)
    total = jnp.dot(pick, states[...], preferred_element_type=F32)
    for k in range(mp):
        total = total + parts[k].astype(F32)
    piece[...] = total.astype(BF16)


def finish(index, half, parts, states):
    return pl.pallas_call(
        finish_kernel,
        out_shape=jax.ShapeDtypeStruct(parts.shape[1:], BF16),
        in_specs=[SMEM_SPEC, SMEM_SPEC, VMEM_SPEC, VMEM_SPEC],
        out_specs=VMEM_SPEC,
        compiler_params=limit(8),
        name="finish",
    )(index, half, parts, states)


def join_kernel(half, piece, other, out):
    first = jnp.where(half[0] == 0, piece[...].astype(F32), other[...].astype(F32))
    second = jnp.where(half[0] == 0, other[...].astype(F32), piece[...].astype(F32))
    out[...] = jnp.concatenate([first, second], axis=0).astype(BF16)


def join(half, piece, other):
    small, width = piece.shape
    return pl.pallas_call(
        join_kernel,
        out_shape=jax.ShapeDtypeStruct((2 * small, width), BF16),
        in_specs=[SMEM_SPEC, VMEM_SPEC, VMEM_SPEC],
        out_specs=VMEM_SPEC,
        compiler_params=limit(8),
        name="join",
    )(half, piece, other)


def per_device(
    tokens,
    enc_gain,
    w_in,
    w_out,
    final_gain,
    w_keyval,
    answer_states,
    dec_gain,
    w_query,
    w_attn_out,
    passage_lengths,
    passage_owner,
    answer_lengths,
):
    row_count = tokens.shape[0]
    width = tokens.shape[1]
    answer_count = answer_states.shape[0]
    mp = lax.axis_size("mp")
    psg = lax.axis_size("psg")
    mp_index = lax.axis_index("mp")
    psg_index = lax.axis_index("psg")
    heads = w_query.shape[1] // DH // psg
    inner = heads * DH

    half = jnp.reshape(psg_index, (1,)).astype(jnp.int32)
    index = jnp.reshape(mp_index, (1,)).astype(jnp.int32)
    held, got, patterns = spread_out(tokens, mp)
    first_in, last_in = stage(index, w_in, 1)
    first_out, last_out = stage(index, w_out, 0)
    partial_sums = feed(
        index, held, got, enc_gain, [first_in, last_in, first_out, last_out], patterns
    )
    parts = lax.all_to_all(partial_sums.reshape(mp, row_count, width), "mp", 0, 0)
    first_key, last_key, value = prepare(half, w_keyval, inner)

    runs = mp * row_count // 2
    slots = jnp.arange(4 * runs, dtype=jnp.int32)
    run = slots // runs
    order = jnp.array(patterns, jnp.int32).reshape(2, 1, mp // 2, 1)
    order = jnp.broadcast_to(order, (2, 2, mp // 2, row_count)).reshape(-1)
    block = jnp.bitwise_xor(mp_index, order)
    core = jnp.bitwise_xor(psg_index, run % 2)
    token_index = (block * psg + core) * row_count + slots % row_count
    out_count = answer_count // mp
    small = out_count // psg
    rows = jnp.arange(answer_count, dtype=jnp.int32)
    side = jnp.bitwise_xor(psg_index, rows // (mp * small))
    answer_index = rows // small % mp * out_count + side * small + rows % small
    allowed = key_mask(
        token_index, answer_index, passage_lengths, passage_owner, answer_lengths
    ).astype(jnp.int32)

    encoded, memory = settle(parts, tokens, final_gain, allowed)
    held, got, _ = spread_out(memory, mp)
    query, first_value, last_value = ask(half, answer_states, dec_gain, w_query, value, mp)
    held = held.reshape(runs, width)
    got = got.reshape(runs, width)
    held_theirs = swap_psg(held)
    weights = (first_key, last_key, first_value, last_value)
    near_keys, near_values, w_last = project(half, held, held_theirs, weights, w_attn_out)
    got_theirs = swap_psg(got)
    keep, give = attend(
        near_keys, near_values, got, got_theirs, query, allowed, weights, w_last
    )
    chip_sum = (keep + swap_psg(give)).astype(BF16).reshape(mp, small, width)
    answer_parts = lax.all_to_all(chip_sum, "mp", 0, 0)
    piece = finish(index, half, answer_parts, answer_states)
    return (encoded, join(half, piece, swap_psg(piece)))


def solution(mesh):
    placed = (
        P(("groups", "mp", "psg"), None),
        P(),
        P(None, "mp"),
        P("mp", None),
        P(),
        P(None, None, "mp"),
        P("groups", None),
        P(),
        P(None, "mp"),
        P("mp", None),
        P("groups"),
        P("groups"),
        P("groups"),
    )
    return jax.shard_map(
        per_device,
        mesh=mesh,
        in_specs=placed,
        out_specs=(P(("groups", "mp", "psg"), None), P(("groups", "mp"), None)),
        check_vma=False,
    )
```

```python
import functools

import jax
import jax.numpy as jnp
from jax import lax
from jax.experimental import pallas as pl
from jax.experimental.pallas import tpu as pltpu
from jax.sharding import PartitionSpec as P


DH = 128
P_SLOT = 16


eps = 1e-06


def norm_rows(states, gain):
    wide = states.astype(jnp.float32)
    factor = lax.rsqrt(jnp.mean(wide * wide, axis=-1, keepdims=True) + eps)
    return wide * factor * gain


def mask_rows(index, half, lengths, owners, answers, shape, patterns, mp, row_count):
    count, keys = shape
    psg = 2
    slot = lax.broadcasted_iota(jnp.int32, (1, keys), 1)
    run = lax.div(slot, keys // 4)
    hop = lax.div(lax.rem(slot, keys // 4), row_count) + lax.div(run, 2) * (mp // 2)
    pattern = jnp.zeros((1, keys), jnp.int32)
    for k, value in enumerate(patterns):
        pattern = jnp.where(hop == k, value, pattern)
    block = index[0] ^ pattern
    core = half[0] ^ lax.rem(run, 2)
    token = (block * psg + core) * row_count + lax.rem(slot, row_count)
    passage = lax.div(token, P_SLOT)
    place = lax.rem(token, P_SLOT)
    length = jnp.zeros((1, keys), jnp.int32)
    owner = jnp.zeros((1, keys), jnp.int32)
    for k in range(lengths.shape[0]):
        length = jnp.where(passage == k, lengths[k], length)
        owner = jnp.where(passage == k, owners[k], owner)
    owner = jnp.where(place < length, owner, -1)
    small = count // mp // psg
    row = lax.broadcasted_iota(jnp.int32, (count, 1), 0)
    side = half[0] ^ lax.div(row, mp * small)
    answer = lax.rem(lax.div(row, small), mp) * (psg * small) + side * small + lax.rem(row, small)
    question = jnp.zeros((count, 1), jnp.int32)
    end = 0
    for k in range(answers.shape[0]):
        end = end + answers[k]
        question = question + jnp.where(answer >= end, 1, 0)
    return jnp.where(owner == question, 1, 0)


def spread_out(x, mp):
    quarter = mp // 4
    patterns = [0]
    blocks = [x[None]]
    for k in (3, 2, 1):
        blocks.append(lax.ppermute(x[None], "mp", [(j, j ^ (k * quarter)) for j in range(mp)]))
        patterns.append(k * quarter)
    held = jnp.concatenate(blocks, axis=0)
    step = quarter // 2
    while step > 0:
        got = lax.ppermute(held, "mp", [(j, j ^ step) for j in range(mp)])
        patterns = patterns + [p ^ step for p in patterns]
        if step > 1:
            held = jnp.concatenate([held, got], axis=0)
        step //= 2
    return held, got, patterns


def swap_psg(x):
    return lax.ppermute(x, "psg", [(0, 1), (1, 0)])


BF16 = jnp.bfloat16
F32 = jnp.float32
SMEM_SPEC = pl.BlockSpec(memory_space=pltpu.SMEM)
VMEM_SPEC = pl.BlockSpec(memory_space=pltpu.VMEM)
HBM_SPEC = pl.BlockSpec(memory_space=pltpu.HBM)


def limit(mib):
    return pltpu.CompilerParams(vmem_limit_bytes=mib << 20)


def ask_kernel(half, states, gain, w_query, value, query, first_value, last_value, scr, sems, *, mp):
    inner = query.shape[1]
    part = first_value.shape[1]
    size = scr.shape[2]
    chunks = inner // size
    start = pl.multiple_of(half[0] * inner, 128)
    copies = [
        pltpu.make_async_copy(
            w_query.at[:, pl.ds(pl.multiple_of(start + c * size, 128), size)],
            scr.at[c],
            sems.at[c],
        )
        for c in range(chunks)
    ]
    others = [
        pltpu.make_async_copy(value.at[:, pl.ds(0, part)], first_value, sems.at[chunks]),
        pltpu.make_async_copy(value.at[:, pl.ds(part, part)], last_value, sems.at[chunks + 1]),
    ]
    for copy in copies + others:
        copy.start()
    normed = norm_rows(states[...], gain[...]).astype(BF16)
    count = states.shape[0]
    small = count // mp // 2
    row = lax.broadcasted_iota(jnp.int32, (count, count), 0)
    column = lax.broadcasted_iota(jnp.int32, (count, count), 1)
    side = half[0] ^ lax.div(row, mp * small)
    source = lax.rem(lax.div(row, small), mp) * (2 * small) + side * small + lax.rem(row, small)
    pick = jnp.where(column == source, 1.0, 0.0).astype(BF16)
    normed = jnp.dot(pick, normed, preferred_element_type=F32).astype(BF16)
    for c in range(chunks):
        copies[c].wait()
        query[:, pl.ds(c * size, size)] = jnp.dot(
            normed, scr[c], preferred_element_type=F32
        ).astype(BF16)
    for copy in others:
        copy.wait()


def ask(half, states, gain, w_query, value, mp):
    count, width = states.shape
    inner = value.shape[1]
    size = min(256, inner)
    return pl.pallas_call(
        functools.partial(ask_kernel, mp=mp),
        out_shape=(
            jax.ShapeDtypeStruct((count, inner), BF16),
            jax.ShapeDtypeStruct((width, inner // 2), BF16),
            jax.ShapeDtypeStruct((width, inner // 2), BF16),
        ),
        in_specs=[SMEM_SPEC, VMEM_SPEC, VMEM_SPEC, HBM_SPEC, HBM_SPEC],
        out_specs=(VMEM_SPEC,) * 3,
        scratch_shapes=[
            pltpu.VMEM((inner // size, width, size), BF16),
            pltpu.SemaphoreType.DMA((inner // size + 2,)),
        ],
        compiler_params=limit(50),
        cost_estimate=pl.CostEstimate(
            flops=1 << 30, bytes_accessed=4 * width * inner, transcendentals=0
        ),
        name="ask",
    )(half, states, gain.reshape(1, width), w_query, value)


def prepare_kernel(half, w_keyval, first_key, last_key, w_value, scr, made, sems):
    inner = made.shape[1]
    part = inner // 2
    blocks = scr.shape[0]
    start = pl.multiple_of(half[0] * inner, 128)
    copies = [
        pltpu.make_async_copy(
            w_keyval.at[pl.ds(b * 128, 128), :, pl.ds(start, inner)], scr.at[b], sems.at[0, b]
        )
        for b in range(blocks)
    ]
    for copy in copies:
        copy.start()
    row = lax.broadcasted_iota(jnp.int32, (256, 256), 0)
    column = lax.broadcasted_iota(jnp.int32, (256, 256), 1)
    source = jnp.where(row < 128, 2 * row, 2 * (row - 128) + 1)
    pick = jnp.where(column == source, 1.0, 0.0).astype(BF16)
    size = min(256, part)
    sent = []
    for b in range(blocks):
        rows = pl.ds(b * 128, 128)
        copies[b].wait()
        for s in range(0, inner, size):
            mixed = scr[b, :, :, pl.ds(s, size)].reshape(256, size)
            apart = jnp.dot(pick, mixed, preferred_element_type=F32).astype(BF16)
            if s < part:
                first_key[rows, pl.ds(s, size)] = apart[:128]
            else:
                last_key[rows, pl.ds(s - part, size)] = apart[:128]
            made[rows, pl.ds(s, size)] = apart[128:]
        sent.append(pltpu.make_async_copy(made.at[rows], w_value.at[rows], sems.at[1, b]))
        sent[-1].start()
    for copy in sent:
        copy.wait()


def prepare(half, w_keyval, inner):
    width = w_keyval.shape[0]
    return pl.pallas_call(
        prepare_kernel,
        out_shape=(
            jax.ShapeDtypeStruct((width, inner // 2), BF16),
            jax.ShapeDtypeStruct((width, inner // 2), BF16),
            jax.ShapeDtypeStruct((width, inner), BF16),
        ),
        in_specs=[SMEM_SPEC, HBM_SPEC],
        out_specs=(VMEM_SPEC, VMEM_SPEC, HBM_SPEC),
        scratch_shapes=[
            pltpu.VMEM((width // 128, 128, 2, inner), BF16),
            pltpu.VMEM((width, inner), BF16),
            pltpu.SemaphoreType.DMA((2, width // 128)),
        ],
        compiler_params=limit(51),
        cost_estimate=pl.CostEstimate(
            flops=4 * width * 256 * inner, bytes_accessed=8 * width * inner, transcendentals=0
        ),
        name="prepare",
    )(half, w_keyval)


def stage_kernel(after, whole, first, last, sems, *, axis):
    del after
    size = first.shape[axis]
    number = sems.shape[0] // 2
    step = size // number
    copies = []
    for half, out in enumerate((first, last)):
        for k in range(number):
            if axis == 0:
                source = whole.at[pl.ds(half * size + k * step, step)]
                target = out.at[pl.ds(k * step, step)]
            else:
                source = whole.at[:, pl.ds(half * size + k * step, step)]
                target = out.at[:, pl.ds(k * step, step)]
            copies.append(pltpu.make_async_copy(source, target, sems.at[half * number + k]))
    for copy in copies:
        copy.start()
    for copy in copies:
        copy.wait()


def stage(after, whole, axis):
    shape = list(whole.shape)
    shape[axis] //= 2
    part = jax.ShapeDtypeStruct(tuple(shape), BF16)
    return pl.pallas_call(
        functools.partial(stage_kernel, axis=axis),
        out_shape=(part, part),
        in_specs=[SMEM_SPEC, HBM_SPEC],
        out_specs=(VMEM_SPEC, VMEM_SPEC),
        scratch_shapes=[pltpu.SemaphoreType.DMA((8,))],
        compiler_params=limit(42),
        cost_estimate=pl.CostEstimate(
            flops=1 << 30, bytes_accessed=8 * shape[0] * shape[1], transcendentals=0
        ),
        name="stage",
    )(after, whole)


def feed_kernel(index, mine, theirs, gain, *refs, patterns):
    *weights, out, normed, hidden = refs
    half = len(weights) // 2
    pairs, rows, width = mine.shape
    units = weights[0].shape[1]
    size = min(256, units)
    weight = gain[...]
    for k in range(2 * pairs):
        place = pl.multiple_of((index[0] ^ patterns[k]) * rows, rows)
        states = mine[k] if k < pairs else theirs[k - pairs]
        normed[pl.ds(place, rows)] = norm_rows(states, weight).astype(BF16)
    for part in range(half):
        for c in range(units // size):
            columns = pl.ds(c * size, size)
            hidden[part, :, columns] = jnp.maximum(
                jnp.dot(normed[...], weights[part][:, columns], preferred_element_type=F32), 0.0
            ).astype(BF16)
    for c in range(width // 256):
        columns = pl.ds(c * 256, 256)
        total = jnp.dot(hidden[0], weights[half][:, columns], preferred_element_type=F32)
        for part in range(1, half):
            total = total + jnp.dot(
                hidden[part], weights[half + part][:, columns], preferred_element_type=F32
            )
        out[:, columns] = total.astype(BF16)


def feed(index, mine, theirs, gain, weights, patterns):
    pairs, rows, width = mine.shape
    count = 2 * pairs * rows
    units = weights[0].shape[1] * len(weights) // 2
    return pl.pallas_call(
        functools.partial(feed_kernel, patterns=patterns),
        out_shape=jax.ShapeDtypeStruct((count, width), BF16),
        in_specs=[SMEM_SPEC] + [VMEM_SPEC] * (3 + len(weights)),
        out_specs=VMEM_SPEC,
        scratch_shapes=[
            pltpu.VMEM((count, width), BF16),
            pltpu.VMEM((len(weights) // 2, count, weights[0].shape[1]), BF16),
        ],
        compiler_params=limit(24),
        cost_estimate=pl.CostEstimate(
            flops=4 * count * width * units, bytes_accessed=4 * width * units, transcendentals=0
        ),
        name="feed",
    )(index, mine, theirs, gain.reshape(1, width), *weights)


def settle_kernel(parts, tokens, gain, encoded, memory):
    total = tokens[...].astype(F32)
    for k in range(parts.shape[0]):
        total = total + parts[k].astype(F32)
    rounded = total.astype(BF16)
    encoded[...] = rounded
    memory[...] = norm_rows(rounded, gain[...]).astype(BF16)


def settle(parts, tokens, gain):
    _, rows, width = parts.shape
    return pl.pallas_call(
        settle_kernel,
        out_shape=(
            jax.ShapeDtypeStruct((rows, width), BF16),
            jax.ShapeDtypeStruct((rows, width), BF16),
        ),
        in_specs=[VMEM_SPEC] * 3,
        out_specs=(VMEM_SPEC, VMEM_SPEC),
        compiler_params=limit(8),
        name="settle",
    )(parts, tokens, gain.reshape(1, width))


def project_kernel(index, half, lengths, owners, answers, mine, theirs, first_key, last_key, first_value, last_value, w_out, keys, values, w_last, allowed, sems, *, patterns, mp):
    inner = keys.shape[1]
    part = inner // 2
    start = pl.multiple_of(half[0] * inner, 128)
    number = sems.shape[0]
    step = inner // number
    copies = [
        pltpu.make_async_copy(
            w_out.at[pl.ds(pl.multiple_of(start + k * step, 64), step)],
            w_last.at[pl.ds(k * step, step)],
            sems.at[k],
        )
        for k in range(number)
    ]
    for copy in copies:
        copy.start()
    row_count = 2 * mine.shape[0] // mp
    allowed[...] = mask_rows(
        index, half, lengths, owners, answers, allowed.shape, patterns, mp, row_count
    )
    rows = jnp.concatenate([mine[...], theirs[...]], axis=0)
    size = min(256, part)
    for k, w_key in enumerate((first_key, last_key)):
        for c in range(part // size):
            keys[:, pl.ds(k * part + c * size, size)] = jnp.dot(
                rows, w_key[:, pl.ds(c * size, size)], preferred_element_type=F32
            ).astype(BF16)
    for k, w_value in enumerate((first_value, last_value)):
        for c in range(part // size):
            values[:, pl.ds(k * part + c * size, size)] = jnp.dot(
                rows, w_value[:, pl.ds(c * size, size)], preferred_element_type=F32
            ).astype(BF16)
    for copy in copies:
        copy.wait()


def project(places, tables, mine, theirs, weights, w_attn_out, patterns, count, mp):
    rows, width = mine.shape
    inner = 2 * weights[0].shape[1]
    return pl.pallas_call(
        functools.partial(project_kernel, patterns=patterns, mp=mp),
        out_shape=(
            jax.ShapeDtypeStruct((2 * rows, inner), BF16),
            jax.ShapeDtypeStruct((2 * rows, inner), BF16),
            jax.ShapeDtypeStruct((inner, width), BF16),
            jax.ShapeDtypeStruct((count, 4 * rows), jnp.int32),
        ),
        in_specs=[SMEM_SPEC] * 5 + [VMEM_SPEC] * 6 + [HBM_SPEC],
        out_specs=(VMEM_SPEC,) * 4,
        scratch_shapes=[pltpu.SemaphoreType.DMA((4,))],
        compiler_params=limit(46),
        cost_estimate=pl.CostEstimate(
            flops=8 * rows * width * inner, bytes_accessed=6 * width * inner, transcendentals=0
        ),
        name="project",
    )(*places, *tables, mine, theirs, *weights, w_attn_out)


def attend_kernel(near_keys, near_values, mine, theirs, query, allowed, first_key, last_key, first_value, last_value, w_last, keep, give, context):
    rows, inner = near_keys.shape
    width = keep.shape[1]
    part = inner // 2
    size = min(256, part)
    late = jnp.concatenate([mine[...], theirs[...]], axis=0)
    near = allowed[:, :rows] > 0
    far = allowed[:, rows:] > 0
    for c in range(inner // size):
        columns = pl.ds(c * size, size)
        w_key = first_key if c * size < part else last_key
        w_value = first_value if c * size < part else last_value
        local = pl.ds(c * size % part, size)
        far_keys = jnp.dot(late, w_key[:, local], preferred_element_type=F32).astype(BF16)
        far_values = jnp.dot(late, w_value[:, local], preferred_element_type=F32).astype(BF16)
        keys = jnp.concatenate([near_keys[:, columns], far_keys], axis=0)
        values = jnp.concatenate([near_values[:, columns], far_values], axis=0)
        for h in range(size // DH):
            lanes = slice(h * DH, (h + 1) * DH)
            place = pl.ds(c * size + h * DH, DH)
            scores = lax.dot_general(
                query[:, place],
                keys[:, lanes],
                (((1,), (1,)), ((), ())),
                preferred_element_type=F32,
            ) * DH ** (-0.5)
            near_scores = jnp.where(near, scores[:, :rows], -1e30)
            far_scores = jnp.where(far, scores[:, rows:], -1e30)
            top = jnp.max(jnp.maximum(near_scores, far_scores), axis=1, keepdims=True)
            near_weights = jnp.where(near, jnp.exp(near_scores - top), 0.0)
            far_weights = jnp.where(far, jnp.exp(far_scores - top), 0.0)
            total = jnp.sum(near_weights + far_weights, axis=1, keepdims=True)
            weights = jnp.concatenate([near_weights, far_weights], axis=1).astype(BF16)
            summed = jnp.dot(weights, values[:, lanes], preferred_element_type=F32)
            context[:, place] = (summed * (1.0 / total)).astype(BF16)
    for c in range(width // 256):
        columns = pl.ds(c * 256, 256)
        result = jnp.dot(context[...], w_last[:, columns], preferred_element_type=F32)
        keep[:, columns] = result[: keep.shape[0]]
        give[:, columns] = result[keep.shape[0] :]


def attend(near_keys, near_values, mine, theirs, query, allowed, weights, w_last):
    rows = near_keys.shape[0]
    width = mine.shape[1]
    count, inner = query.shape
    return pl.pallas_call(
        attend_kernel,
        out_shape=(jax.ShapeDtypeStruct((count // 2, width), F32),) * 2,
        in_specs=[VMEM_SPEC] * 11,
        out_specs=(VMEM_SPEC, VMEM_SPEC),
        scratch_shapes=[pltpu.VMEM((count, inner), BF16)],
        compiler_params=limit(24),
        cost_estimate=pl.CostEstimate(
            flops=4 * rows * width * inner + 8 * count * rows * inner + 2 * count * inner * width,
            bytes_accessed=6 * width * inner,
            transcendentals=2 * count * rows * inner // DH,
        ),
        name="attend",
    )(near_keys, near_values, mine, theirs, query, allowed, *weights, w_last)


def finish_kernel(index, half, parts, states, piece):
    mp, small, _ = parts.shape
    start = index[0] * (2 * small) + half[0] * small
    row = lax.broadcasted_iota(jnp.int32, (small, states.shape[0]), 0)
    column = lax.broadcasted_iota(jnp.int32, (small, states.shape[0]), 1)
    pick = jnp.where(column == row + start, 1.0, 0.0).astype(BF16)
    total = jnp.dot(pick, states[...], preferred_element_type=F32)
    for k in range(mp):
        total = total + parts[k].astype(F32)
    piece[...] = total.astype(BF16)


def finish(index, half, parts, states):
    return pl.pallas_call(
        finish_kernel,
        out_shape=jax.ShapeDtypeStruct(parts.shape[1:], BF16),
        in_specs=[SMEM_SPEC, SMEM_SPEC, VMEM_SPEC, VMEM_SPEC],
        out_specs=VMEM_SPEC,
        compiler_params=limit(8),
        name="finish",
    )(index, half, parts, states)


def join_kernel(half, piece, other, out):
    first = jnp.where(half[0] == 0, piece[...].astype(F32), other[...].astype(F32))
    second = jnp.where(half[0] == 0, other[...].astype(F32), piece[...].astype(F32))
    out[...] = jnp.concatenate([first, second], axis=0).astype(BF16)


def join(half, piece, other):
    small, width = piece.shape
    return pl.pallas_call(
        join_kernel,
        out_shape=jax.ShapeDtypeStruct((2 * small, width), BF16),
        in_specs=[SMEM_SPEC, VMEM_SPEC, VMEM_SPEC],
        out_specs=VMEM_SPEC,
        compiler_params=limit(8),
        name="join",
    )(half, piece, other)


def per_device(
    tokens,
    enc_gain,
    w_in,
    w_out,
    final_gain,
    w_keyval,
    answer_states,
    dec_gain,
    w_query,
    w_attn_out,
    passage_lengths,
    passage_owner,
    answer_lengths,
):
    row_count = tokens.shape[0]
    width = tokens.shape[1]
    answer_count = answer_states.shape[0]
    mp = lax.axis_size("mp")
    psg = lax.axis_size("psg")
    mp_index = lax.axis_index("mp")
    psg_index = lax.axis_index("psg")
    heads = w_query.shape[1] // DH // psg
    inner = heads * DH

    half = jnp.reshape(psg_index, (1,)).astype(jnp.int32)
    index = jnp.reshape(mp_index, (1,)).astype(jnp.int32)
    held, got, patterns = spread_out(tokens, mp)
    first_in, last_in = stage(index, w_in, 1)
    first_out, last_out = stage(index, w_out, 0)
    partial_sums = feed(
        index, held, got, enc_gain, [first_in, last_in, first_out, last_out], patterns
    )
    parts = lax.all_to_all(partial_sums.reshape(mp, row_count, width), "mp", 0, 0)
    first_key, last_key, value = prepare(half, w_keyval, inner)

    runs = mp * row_count // 2
    small = answer_count // mp // psg
    encoded, memory = settle(parts, tokens, final_gain)
    held, got, _ = spread_out(memory, mp)
    query, first_value, last_value = ask(half, answer_states, dec_gain, w_query, value, mp)
    held = held.reshape(runs, width)
    got = got.reshape(runs, width)
    held_theirs = swap_psg(held)
    weights = (first_key, last_key, first_value, last_value)
    near_keys, near_values, w_last, allowed = project(
        (index, half),
        (passage_lengths, passage_owner, answer_lengths),
        held,
        held_theirs,
        weights,
        w_attn_out,
        patterns,
        answer_count,
        mp,
    )
    got_theirs = swap_psg(got)
    keep, give = attend(
        near_keys, near_values, got, got_theirs, query, allowed, weights, w_last
    )
    chip_sum = (keep + swap_psg(give)).astype(BF16).reshape(mp, small, width)
    answer_parts = lax.all_to_all(chip_sum, "mp", 0, 0)
    piece = finish(index, half, answer_parts, answer_states)
    return (encoded, join(half, piece, swap_psg(piece)))


def solution(mesh):
    placed = (
        P(("groups", "mp", "psg"), None),
        P(),
        P(None, "mp"),
        P("mp", None),
        P(),
        P(None, None, "mp"),
        P("groups", None),
        P(),
        P(None, "mp"),
        P("mp", None),
        P("groups"),
        P("groups"),
        P("groups"),
    )
    return jax.shard_map(
        per_device,
        mesh=mesh,
        in_specs=placed,
        out_specs=(P(("groups", "mp", "psg"), None), P(("groups", "mp"), None)),
        check_vma=False,
    )
```

```python
import functools

import jax
import jax.numpy as jnp
from jax import lax
from jax.experimental import pallas as pl
from jax.experimental.pallas import tpu as pltpu
from jax.sharding import PartitionSpec as P


DH = 128
P_SLOT = 16


eps = 1e-06


def norm_rows(states, gain):
    wide = states.astype(jnp.float32)
    factor = lax.rsqrt(jnp.mean(wide * wide, axis=-1, keepdims=True) + eps)
    return wide * factor * gain


def mask_rows(index, half, lengths, owners, answers, shape, patterns, mp, row_count):
    count, keys = shape
    psg = 2
    slot = lax.broadcasted_iota(jnp.int32, (1, keys), 1)
    run = lax.div(slot, keys // 4)
    hop = lax.div(lax.rem(slot, keys // 4), row_count) + lax.div(run, 2) * (mp // 2)
    pattern = jnp.zeros((1, keys), jnp.int32)
    for k, value in enumerate(patterns):
        pattern = jnp.where(hop == k, value, pattern)
    block = index[0] ^ pattern
    core = half[0] ^ lax.rem(run, 2)
    token = (block * psg + core) * row_count + lax.rem(slot, row_count)
    passage = lax.div(token, P_SLOT)
    place = lax.rem(token, P_SLOT)
    length = jnp.zeros((1, keys), jnp.int32)
    owner = jnp.zeros((1, keys), jnp.int32)
    for k in range(lengths.shape[0]):
        length = jnp.where(passage == k, lengths[k], length)
        owner = jnp.where(passage == k, owners[k], owner)
    owner = jnp.where(place < length, owner, -1)
    small = count // mp // psg
    row = lax.broadcasted_iota(jnp.int32, (count, 1), 0)
    side = half[0] ^ lax.div(row, mp * small)
    answer = lax.rem(lax.div(row, small), mp) * (psg * small) + side * small + lax.rem(row, small)
    question = jnp.zeros((count, 1), jnp.int32)
    end = 0
    for k in range(answers.shape[0]):
        end = end + answers[k]
        question = question + jnp.where(answer >= end, 1, 0)
    return jnp.where(owner == question, 1, 0)


def spread_out(x, mp):
    quarter = mp // 4
    patterns = [0]
    blocks = [x[None]]
    for k in (3, 2, 1):
        blocks.append(lax.ppermute(x[None], "mp", [(j, j ^ (k * quarter)) for j in range(mp)]))
        patterns.append(k * quarter)
    held = jnp.concatenate(blocks, axis=0)
    step = quarter // 2
    while step > 0:
        got = lax.ppermute(held, "mp", [(j, j ^ step) for j in range(mp)])
        patterns = patterns + [p ^ step for p in patterns]
        if step > 1:
            held = jnp.concatenate([held, got], axis=0)
        step //= 2
    return held, got, patterns


def swap_psg(x):
    return lax.ppermute(x, "psg", [(0, 1), (1, 0)])


BF16 = jnp.bfloat16
F32 = jnp.float32
SMEM_SPEC = pl.BlockSpec(memory_space=pltpu.SMEM)
VMEM_SPEC = pl.BlockSpec(memory_space=pltpu.VMEM)
HBM_SPEC = pl.BlockSpec(memory_space=pltpu.HBM)


def limit(mib):
    return pltpu.CompilerParams(vmem_limit_bytes=mib << 20)


def ask_kernel(half, states, gain, settled, w_query, value, query, first_value, last_value, encoded, scr, sems, *, mp):
    inner = query.shape[1]
    part = first_value.shape[1]
    size = scr.shape[2]
    chunks = inner // size
    start = pl.multiple_of(half[0] * inner, 128)
    copies = [
        pltpu.make_async_copy(
            w_query.at[:, pl.ds(pl.multiple_of(start + c * size, 128), size)],
            scr.at[c],
            sems.at[c],
        )
        for c in range(chunks)
    ]
    others = [
        pltpu.make_async_copy(value.at[:, pl.ds(0, part)], first_value, sems.at[chunks]),
        pltpu.make_async_copy(value.at[:, pl.ds(part, part)], last_value, sems.at[chunks + 1]),
    ]
    for copy in copies + others:
        copy.start()
    normed = norm_rows(states[...], gain[...]).astype(BF16)
    encoded[...] = settled[...]
    count = states.shape[0]
    small = count // mp // 2
    row = lax.broadcasted_iota(jnp.int32, (count, count), 0)
    column = lax.broadcasted_iota(jnp.int32, (count, count), 1)
    side = half[0] ^ lax.div(row, mp * small)
    source = lax.rem(lax.div(row, small), mp) * (2 * small) + side * small + lax.rem(row, small)
    pick = jnp.where(column == source, 1.0, 0.0).astype(BF16)
    normed = jnp.dot(pick, normed, preferred_element_type=F32).astype(BF16)
    for c in range(chunks):
        copies[c].wait()
        query[:, pl.ds(c * size, size)] = jnp.dot(
            normed, scr[c], preferred_element_type=F32
        ).astype(BF16)
    for copy in others:
        copy.wait()


def ask(half, states, gain, settled, w_query, value, mp):
    count, width = states.shape
    inner = value.shape[1]
    size = min(256, inner)
    return pl.pallas_call(
        functools.partial(ask_kernel, mp=mp),
        out_shape=(
            jax.ShapeDtypeStruct((count, inner), BF16),
            jax.ShapeDtypeStruct((width, inner // 2), BF16),
            jax.ShapeDtypeStruct((width, inner // 2), BF16),
            jax.ShapeDtypeStruct(settled.shape, BF16),
        ),
        in_specs=[SMEM_SPEC] + [VMEM_SPEC] * 3 + [HBM_SPEC, HBM_SPEC],
        out_specs=(VMEM_SPEC,) * 4,
        scratch_shapes=[
            pltpu.VMEM((inner // size, width, size), BF16),
            pltpu.SemaphoreType.DMA((inner // size + 2,)),
        ],
        compiler_params=limit(50),
        cost_estimate=pl.CostEstimate(
            flops=1 << 30, bytes_accessed=4 * width * inner, transcendentals=0
        ),
        name="ask",
    )(half, states, gain.reshape(1, width), settled, w_query, value)


def prepare_kernel(half, w_keyval, first_key, last_key, w_value, scr, made, sems):
    inner = made.shape[1]
    part = inner // 2
    blocks = scr.shape[0]
    start = pl.multiple_of(half[0] * inner, 128)
    copies = [
        pltpu.make_async_copy(
            w_keyval.at[pl.ds(b * 128, 128), :, pl.ds(start, inner)], scr.at[b], sems.at[0, b]
        )
        for b in range(blocks)
    ]
    for copy in copies:
        copy.start()
    row = lax.broadcasted_iota(jnp.int32, (256, 256), 0)
    column = lax.broadcasted_iota(jnp.int32, (256, 256), 1)
    source = jnp.where(row < 128, 2 * row, 2 * (row - 128) + 1)
    pick = jnp.where(column == source, 1.0, 0.0).astype(BF16)
    size = min(256, part)
    sent = []
    for b in range(blocks):
        rows = pl.ds(b * 128, 128)
        copies[b].wait()
        for s in range(0, inner, size):
            mixed = scr[b, :, :, pl.ds(s, size)].reshape(256, size)
            apart = jnp.dot(pick, mixed, preferred_element_type=F32).astype(BF16)
            if s < part:
                first_key[rows, pl.ds(s, size)] = apart[:128]
            else:
                last_key[rows, pl.ds(s - part, size)] = apart[:128]
            made[rows, pl.ds(s, size)] = apart[128:]
        sent.append(pltpu.make_async_copy(made.at[rows], w_value.at[rows], sems.at[1, b]))
        sent[-1].start()
    for copy in sent:
        copy.wait()


def prepare(half, w_keyval, inner):
    width = w_keyval.shape[0]
    return pl.pallas_call(
        prepare_kernel,
        out_shape=(
            jax.ShapeDtypeStruct((width, inner // 2), BF16),
            jax.ShapeDtypeStruct((width, inner // 2), BF16),
            jax.ShapeDtypeStruct((width, inner), BF16),
        ),
        in_specs=[SMEM_SPEC, HBM_SPEC],
        out_specs=(VMEM_SPEC, VMEM_SPEC, HBM_SPEC),
        scratch_shapes=[
            pltpu.VMEM((width // 128, 128, 2, inner), BF16),
            pltpu.VMEM((width, inner), BF16),
            pltpu.SemaphoreType.DMA((2, width // 128)),
        ],
        compiler_params=limit(51),
        cost_estimate=pl.CostEstimate(
            flops=4 * width * 256 * inner, bytes_accessed=8 * width * inner, transcendentals=0
        ),
        name="prepare",
    )(half, w_keyval)


def stage_kernel(after, whole, first, last, sems, *, axis):
    del after
    size = first.shape[axis]
    number = sems.shape[0] // 2
    step = size // number
    copies = []
    for half, out in enumerate((first, last)):
        for k in range(number):
            if axis == 0:
                source = whole.at[pl.ds(half * size + k * step, step)]
                target = out.at[pl.ds(k * step, step)]
            else:
                source = whole.at[:, pl.ds(half * size + k * step, step)]
                target = out.at[:, pl.ds(k * step, step)]
            copies.append(pltpu.make_async_copy(source, target, sems.at[half * number + k]))
    for copy in copies:
        copy.start()
    for copy in copies:
        copy.wait()


def stage(after, whole, axis):
    shape = list(whole.shape)
    shape[axis] //= 2
    part = jax.ShapeDtypeStruct(tuple(shape), BF16)
    return pl.pallas_call(
        functools.partial(stage_kernel, axis=axis),
        out_shape=(part, part),
        in_specs=[SMEM_SPEC, HBM_SPEC],
        out_specs=(VMEM_SPEC, VMEM_SPEC),
        scratch_shapes=[pltpu.SemaphoreType.DMA((8,))],
        compiler_params=limit(42),
        cost_estimate=pl.CostEstimate(
            flops=1 << 30, bytes_accessed=8 * shape[0] * shape[1], transcendentals=0
        ),
        name="stage",
    )(after, whole)


def stage_rows_kernel(after, whole, rows, gain, first, last, normed, sems):
    del after
    size = first.shape[0]
    number = sems.shape[0] // 2
    step = size // number
    copies = []
    for half, out in enumerate((first, last)):
        for k in range(number):
            copies.append(
                pltpu.make_async_copy(
                    whole.at[pl.ds(half * size + k * step, step)],
                    out.at[pl.ds(k * step, step)],
                    sems.at[half * number + k],
                )
            )
    for copy in copies:
        copy.start()
    for k in range(rows.shape[0]):
        normed[k] = norm_rows(rows[k], gain[...]).astype(BF16)
    for copy in copies:
        copy.wait()


def stage_rows(after, whole, rows, gain):
    units, width = whole.shape
    part = jax.ShapeDtypeStruct((units // 2, width), BF16)
    return pl.pallas_call(
        stage_rows_kernel,
        out_shape=(part, part, jax.ShapeDtypeStruct(rows.shape, BF16)),
        in_specs=[SMEM_SPEC, HBM_SPEC, VMEM_SPEC, VMEM_SPEC],
        out_specs=(VMEM_SPEC,) * 3,
        scratch_shapes=[pltpu.SemaphoreType.DMA((8,))],
        compiler_params=limit(42),
        cost_estimate=pl.CostEstimate(
            flops=1 << 30, bytes_accessed=4 * units * width, transcendentals=0
        ),
        name="stage_rows",
    )(after, whole, rows, gain.reshape(1, width))


def feed_kernel(index, mine, theirs, gain, *refs, patterns):
    *weights, out, normed, hidden = refs
    half = len(weights) // 2
    pairs, rows, width = mine.shape
    units = weights[0].shape[1]
    size = min(256, units)
    weight = gain[...]
    for k in range(2 * pairs):
        place = pl.multiple_of((index[0] ^ patterns[k]) * rows, rows)
        if k < pairs:
            normed[pl.ds(place, rows)] = mine[k]
        else:
            normed[pl.ds(place, rows)] = norm_rows(theirs[k - pairs], weight).astype(BF16)
    for part in range(half):
        for c in range(units // size):
            columns = pl.ds(c * size, size)
            hidden[part, :, columns] = jnp.maximum(
                jnp.dot(normed[...], weights[part][:, columns], preferred_element_type=F32), 0.0
            ).astype(BF16)
    for c in range(width // 256):
        columns = pl.ds(c * 256, 256)
        total = jnp.dot(hidden[0], weights[half][:, columns], preferred_element_type=F32)
        for part in range(1, half):
            total = total + jnp.dot(
                hidden[part], weights[half + part][:, columns], preferred_element_type=F32
            )
        out[:, columns] = total.astype(BF16)


def feed(index, mine, theirs, gain, weights, patterns):
    pairs, rows, width = mine.shape
    count = 2 * pairs * rows
    units = weights[0].shape[1] * len(weights) // 2
    return pl.pallas_call(
        functools.partial(feed_kernel, patterns=patterns),
        out_shape=jax.ShapeDtypeStruct((count, width), BF16),
        in_specs=[SMEM_SPEC] + [VMEM_SPEC] * (3 + len(weights)),
        out_specs=VMEM_SPEC,
        scratch_shapes=[
            pltpu.VMEM((count, width), BF16),
            pltpu.VMEM((len(weights) // 2, count, weights[0].shape[1]), BF16),
        ],
        compiler_params=limit(24),
        cost_estimate=pl.CostEstimate(
            flops=4 * count * width * units, bytes_accessed=4 * width * units, transcendentals=0
        ),
        name="feed",
    )(index, mine, theirs, gain.reshape(1, width), *weights)


def settle_kernel(parts, tokens, gain, encoded, memory):
    total = tokens[...].astype(F32)
    for k in range(parts.shape[0]):
        total = total + parts[k].astype(F32)
    rounded = total.astype(BF16)
    encoded[...] = rounded
    memory[...] = norm_rows(rounded, gain[...]).astype(BF16)


def settle(parts, tokens, gain):
    _, rows, width = parts.shape
    return pl.pallas_call(
        settle_kernel,
        out_shape=(
            jax.ShapeDtypeStruct((rows, width), BF16),
            jax.ShapeDtypeStruct((rows, width), BF16),
        ),
        in_specs=[VMEM_SPEC] * 3,
        out_specs=(VMEM_SPEC, VMEM_SPEC),
        compiler_params=limit(8),
        name="settle",
    )(parts, tokens, gain.reshape(1, width))


def project_kernel(index, half, lengths, owners, answers, mine, theirs, first_key, last_key, first_value, last_value, w_out, keys, values, w_last, allowed, sems, *, patterns, mp):
    inner = keys.shape[1]
    part = inner // 2
    start = pl.multiple_of(half[0] * inner, 128)
    number = sems.shape[0]
    step = inner // number
    copies = [
        pltpu.make_async_copy(
            w_out.at[pl.ds(pl.multiple_of(start + k * step, 64), step)],
            w_last.at[pl.ds(k * step, step)],
            sems.at[k],
        )
        for k in range(number)
    ]
    for copy in copies:
        copy.start()
    row_count = 2 * mine.shape[0] // mp
    allowed[...] = mask_rows(
        index, half, lengths, owners, answers, allowed.shape, patterns, mp, row_count
    )
    rows = jnp.concatenate([mine[...], theirs[...]], axis=0)
    size = min(256, part)
    for k, w_key in enumerate((first_key, last_key)):
        for c in range(part // size):
            keys[:, pl.ds(k * part + c * size, size)] = jnp.dot(
                rows, w_key[:, pl.ds(c * size, size)], preferred_element_type=F32
            ).astype(BF16)
    for k, w_value in enumerate((first_value, last_value)):
        for c in range(part // size):
            values[:, pl.ds(k * part + c * size, size)] = jnp.dot(
                rows, w_value[:, pl.ds(c * size, size)], preferred_element_type=F32
            ).astype(BF16)
    for copy in copies:
        copy.wait()


def project(places, tables, mine, theirs, weights, w_attn_out, patterns, count, mp):
    rows, width = mine.shape
    inner = 2 * weights[0].shape[1]
    return pl.pallas_call(
        functools.partial(project_kernel, patterns=patterns, mp=mp),
        out_shape=(
            jax.ShapeDtypeStruct((2 * rows, inner), BF16),
            jax.ShapeDtypeStruct((2 * rows, inner), BF16),
            jax.ShapeDtypeStruct((inner, width), BF16),
            jax.ShapeDtypeStruct((count, 4 * rows), jnp.int32),
        ),
        in_specs=[SMEM_SPEC] * 5 + [VMEM_SPEC] * 6 + [HBM_SPEC],
        out_specs=(VMEM_SPEC,) * 4,
        scratch_shapes=[pltpu.SemaphoreType.DMA((4,))],
        compiler_params=limit(46),
        cost_estimate=pl.CostEstimate(
            flops=8 * rows * width * inner, bytes_accessed=6 * width * inner, transcendentals=0
        ),
        name="project",
    )(*places, *tables, mine, theirs, *weights, w_attn_out)


def attend_kernel(near_keys, near_values, mine, theirs, query, allowed, first_key, last_key, first_value, last_value, w_last, keep, give, context):
    rows, inner = near_keys.shape
    width = keep.shape[1]
    part = inner // 2
    size = min(256, part)
    late = jnp.concatenate([mine[...], theirs[...]], axis=0)
    near = allowed[:, :rows] > 0
    far = allowed[:, rows:] > 0
    for c in range(inner // size):
        columns = pl.ds(c * size, size)
        w_key = first_key if c * size < part else last_key
        w_value = first_value if c * size < part else last_value
        local = pl.ds(c * size % part, size)
        far_keys = jnp.dot(late, w_key[:, local], preferred_element_type=F32).astype(BF16)
        far_values = jnp.dot(late, w_value[:, local], preferred_element_type=F32).astype(BF16)
        keys = jnp.concatenate([near_keys[:, columns], far_keys], axis=0)
        values = jnp.concatenate([near_values[:, columns], far_values], axis=0)
        for h in range(size // DH):
            lanes = slice(h * DH, (h + 1) * DH)
            place = pl.ds(c * size + h * DH, DH)
            scores = lax.dot_general(
                query[:, place],
                keys[:, lanes],
                (((1,), (1,)), ((), ())),
                preferred_element_type=F32,
            ) * DH ** (-0.5)
            near_scores = jnp.where(near, scores[:, :rows], -1e30)
            far_scores = jnp.where(far, scores[:, rows:], -1e30)
            top = jnp.max(jnp.maximum(near_scores, far_scores), axis=1, keepdims=True)
            near_weights = jnp.where(near, jnp.exp(near_scores - top), 0.0)
            far_weights = jnp.where(far, jnp.exp(far_scores - top), 0.0)
            total = jnp.sum(near_weights + far_weights, axis=1, keepdims=True)
            weights = jnp.concatenate([near_weights, far_weights], axis=1).astype(BF16)
            summed = jnp.dot(weights, values[:, lanes], preferred_element_type=F32)
            context[:, place] = (summed * (1.0 / total)).astype(BF16)
    for c in range(width // 256):
        columns = pl.ds(c * 256, 256)
        result = jnp.dot(context[...], w_last[:, columns], preferred_element_type=F32)
        keep[:, columns] = result[: keep.shape[0]]
        give[:, columns] = result[keep.shape[0] :]


def attend(near_keys, near_values, mine, theirs, query, allowed, weights, w_last):
    rows = near_keys.shape[0]
    width = mine.shape[1]
    count, inner = query.shape
    return pl.pallas_call(
        attend_kernel,
        out_shape=(jax.ShapeDtypeStruct((count // 2, width), F32),) * 2,
        in_specs=[VMEM_SPEC] * 11,
        out_specs=(VMEM_SPEC, VMEM_SPEC),
        scratch_shapes=[pltpu.VMEM((count, inner), BF16)],
        compiler_params=limit(24),
        cost_estimate=pl.CostEstimate(
            flops=4 * rows * width * inner + 8 * count * rows * inner + 2 * count * inner * width,
            bytes_accessed=6 * width * inner,
            transcendentals=2 * count * rows * inner // DH,
        ),
        name="attend",
    )(near_keys, near_values, mine, theirs, query, allowed, *weights, w_last)


def finish_kernel(index, half, parts, states, piece):
    mp, small, _ = parts.shape
    start = index[0] * (2 * small) + half[0] * small
    row = lax.broadcasted_iota(jnp.int32, (small, states.shape[0]), 0)
    column = lax.broadcasted_iota(jnp.int32, (small, states.shape[0]), 1)
    pick = jnp.where(column == row + start, 1.0, 0.0).astype(BF16)
    total = jnp.dot(pick, states[...], preferred_element_type=F32)
    for k in range(mp):
        total = total + parts[k].astype(F32)
    piece[...] = total.astype(BF16)


def finish(index, half, parts, states):
    return pl.pallas_call(
        finish_kernel,
        out_shape=jax.ShapeDtypeStruct(parts.shape[1:], BF16),
        in_specs=[SMEM_SPEC, SMEM_SPEC, VMEM_SPEC, VMEM_SPEC],
        out_specs=VMEM_SPEC,
        compiler_params=limit(8),
        name="finish",
    )(index, half, parts, states)


def join_kernel(half, piece, other, out):
    first = jnp.where(half[0] == 0, piece[...].astype(F32), other[...].astype(F32))
    second = jnp.where(half[0] == 0, other[...].astype(F32), piece[...].astype(F32))
    out[...] = jnp.concatenate([first, second], axis=0).astype(BF16)


def join(half, piece, other):
    small, width = piece.shape
    return pl.pallas_call(
        join_kernel,
        out_shape=jax.ShapeDtypeStruct((2 * small, width), BF16),
        in_specs=[SMEM_SPEC, VMEM_SPEC, VMEM_SPEC],
        out_specs=VMEM_SPEC,
        compiler_params=limit(8),
        name="join",
    )(half, piece, other)


def per_device(
    tokens,
    enc_gain,
    w_in,
    w_out,
    final_gain,
    w_keyval,
    answer_states,
    dec_gain,
    w_query,
    w_attn_out,
    passage_lengths,
    passage_owner,
    answer_lengths,
):
    row_count = tokens.shape[0]
    width = tokens.shape[1]
    answer_count = answer_states.shape[0]
    mp = lax.axis_size("mp")
    psg = lax.axis_size("psg")
    mp_index = lax.axis_index("mp")
    psg_index = lax.axis_index("psg")
    heads = w_query.shape[1] // DH // psg
    inner = heads * DH

    half = jnp.reshape(psg_index, (1,)).astype(jnp.int32)
    index = jnp.reshape(mp_index, (1,)).astype(jnp.int32)
    held, got, patterns = spread_out(tokens, mp)
    first_in, last_in = stage(index, w_in, 1)
    first_out, last_out, held = stage_rows(index, w_out, held, enc_gain)
    partial_sums = feed(
        index, held, got, enc_gain, [first_in, last_in, first_out, last_out], patterns
    )
    parts = lax.all_to_all(partial_sums.reshape(mp, row_count, width), "mp", 0, 0)
    first_key, last_key, value = prepare(half, w_keyval, inner)

    runs = mp * row_count // 2
    small = answer_count // mp // psg
    settled, memory = settle(parts, tokens, final_gain)
    held, got, _ = spread_out(memory, mp)
    query, first_value, last_value, encoded = ask(
        half, answer_states, dec_gain, settled, w_query, value, mp
    )
    held = held.reshape(runs, width)
    got = got.reshape(runs, width)
    held_theirs = swap_psg(held)
    weights = (first_key, last_key, first_value, last_value)
    near_keys, near_values, w_last, allowed = project(
        (index, half),
        (passage_lengths, passage_owner, answer_lengths),
        held,
        held_theirs,
        weights,
        w_attn_out,
        patterns,
        answer_count,
        mp,
    )
    got_theirs = swap_psg(got)
    keep, give = attend(
        near_keys, near_values, got, got_theirs, query, allowed, weights, w_last
    )
    chip_sum = (keep + swap_psg(give)).astype(BF16).reshape(mp, small, width)
    answer_parts = lax.all_to_all(chip_sum, "mp", 0, 0)
    piece = finish(index, half, answer_parts, answer_states)
    return (encoded, join(half, piece, swap_psg(piece)))


def solution(mesh):
    placed = (
        P(("groups", "mp", "psg"), None),
        P(),
        P(None, "mp"),
        P("mp", None),
        P(),
        P(None, None, "mp"),
        P("groups", None),
        P(),
        P(None, "mp"),
        P("mp", None),
        P("groups"),
        P("groups"),
        P("groups"),
    )
    return jax.shard_map(
        per_device,
        mesh=mesh,
        in_specs=placed,
        out_specs=(P(("groups", "mp", "psg"), None), P(("groups", "mp"), None)),
        check_vma=False,
    )
```

```python
import functools

import jax
import jax.numpy as jnp
from jax import lax
from jax.experimental import pallas as pl
from jax.experimental.pallas import tpu as pltpu
from jax.sharding import PartitionSpec as P


DH = 128
P_SLOT = 16


eps = 1e-06


def norm_rows(states, gain):
    wide = states.astype(jnp.float32)
    factor = lax.rsqrt(jnp.mean(wide * wide, axis=-1, keepdims=True) + eps)
    return wide * factor * gain


def mask_rows(index, half, lengths, owners, answers, shape, patterns, mp, row_count):
    count, keys = shape
    psg = 2
    slot = lax.broadcasted_iota(jnp.int32, (1, keys), 1)
    run = lax.div(slot, keys // 4)
    hop = lax.div(lax.rem(slot, keys // 4), row_count) + lax.div(run, 2) * (mp // 2)
    pattern = jnp.zeros((1, keys), jnp.int32)
    for k, value in enumerate(patterns):
        pattern = jnp.where(hop == k, value, pattern)
    block = index[0] ^ pattern
    core = half[0] ^ lax.rem(run, 2)
    token = (block * psg + core) * row_count + lax.rem(slot, row_count)
    passage = lax.div(token, P_SLOT)
    place = lax.rem(token, P_SLOT)
    length = jnp.zeros((1, keys), jnp.int32)
    owner = jnp.zeros((1, keys), jnp.int32)
    for k in range(lengths.shape[0]):
        length = jnp.where(passage == k, lengths[k], length)
        owner = jnp.where(passage == k, owners[k], owner)
    owner = jnp.where(place < length, owner, -1)
    small = count // mp // psg
    row = lax.broadcasted_iota(jnp.int32, (count, 1), 0)
    side = half[0] ^ lax.div(row, mp * small)
    answer = lax.rem(lax.div(row, small), mp) * (psg * small) + side * small + lax.rem(row, small)
    question = jnp.zeros((count, 1), jnp.int32)
    end = 0
    for k in range(answers.shape[0]):
        end = end + answers[k]
        question = question + jnp.where(answer >= end, 1, 0)
    return jnp.where(owner == question, 1, 0)


def spread_out(x, mp):
    quarter = mp // 4
    patterns = [0]
    blocks = [x[None]]
    for k in (3, 2, 1):
        blocks.append(lax.ppermute(x[None], "mp", [(j, j ^ (k * quarter)) for j in range(mp)]))
        patterns.append(k * quarter)
    held = jnp.concatenate(blocks, axis=0)
    step = quarter // 2
    while step > 0:
        got = lax.ppermute(held, "mp", [(j, j ^ step) for j in range(mp)])
        patterns = patterns + [p ^ step for p in patterns]
        if step > 1:
            held = jnp.concatenate([held, got], axis=0)
        step //= 2
    return held, got, patterns


def swap_psg(x):
    return lax.ppermute(x, "psg", [(0, 1), (1, 0)])


BF16 = jnp.bfloat16
F32 = jnp.float32
SMEM_SPEC = pl.BlockSpec(memory_space=pltpu.SMEM)
VMEM_SPEC = pl.BlockSpec(memory_space=pltpu.VMEM)
HBM_SPEC = pl.BlockSpec(memory_space=pltpu.HBM)


def limit(mib):
    return pltpu.CompilerParams(vmem_limit_bytes=mib << 20)


def ask_kernel(half, states, gain, w_query, value, query, first_value, last_value, scr, sems, *, mp):
    inner = query.shape[1]
    part = first_value.shape[1]
    size = scr.shape[2]
    chunks = inner // size
    start = pl.multiple_of(half[0] * inner, 128)
    copies = [
        pltpu.make_async_copy(
            w_query.at[:, pl.ds(pl.multiple_of(start + c * size, 128), size)],
            scr.at[c],
            sems.at[c],
        )
        for c in range(chunks)
    ]
    others = [
        pltpu.make_async_copy(value.at[:, pl.ds(0, part)], first_value, sems.at[chunks]),
        pltpu.make_async_copy(value.at[:, pl.ds(part, part)], last_value, sems.at[chunks + 1]),
    ]
    for copy in copies + others:
        copy.start()
    normed = norm_rows(states[...], gain[...]).astype(BF16)
    count = states.shape[0]
    small = count // mp // 2
    row = lax.broadcasted_iota(jnp.int32, (count, count), 0)
    column = lax.broadcasted_iota(jnp.int32, (count, count), 1)
    side = half[0] ^ lax.div(row, mp * small)
    source = lax.rem(lax.div(row, small), mp) * (2 * small) + side * small + lax.rem(row, small)
    pick = jnp.where(column == source, 1.0, 0.0).astype(BF16)
    normed = jnp.dot(pick, normed, preferred_element_type=F32).astype(BF16)
    for c in range(chunks):
        copies[c].wait()
        query[:, pl.ds(c * size, size)] = jnp.dot(
            normed, scr[c], preferred_element_type=F32
        ).astype(BF16)
    for copy in others:
        copy.wait()


def ask(half, states, gain, w_query, value, mp):
    count, width = states.shape
    inner = value.shape[1]
    size = min(256, inner)
    return pl.pallas_call(
        functools.partial(ask_kernel, mp=mp),
        out_shape=(
            jax.ShapeDtypeStruct((count, inner), BF16),
            jax.ShapeDtypeStruct((width, inner // 2), BF16),
            jax.ShapeDtypeStruct((width, inner // 2), BF16),
        ),
        in_specs=[SMEM_SPEC, VMEM_SPEC, VMEM_SPEC, HBM_SPEC, HBM_SPEC],
        out_specs=(VMEM_SPEC,) * 3,
        scratch_shapes=[
            pltpu.VMEM((inner // size, width, size), BF16),
            pltpu.SemaphoreType.DMA((inner // size + 2,)),
        ],
        compiler_params=limit(50),
        cost_estimate=pl.CostEstimate(
            flops=1 << 30, bytes_accessed=4 * width * inner, transcendentals=0
        ),
        name="ask",
    )(half, states, gain.reshape(1, width), w_query, value)


def prepare_kernel(half, w_keyval, first_key, last_key, w_value, scr, made, sems):
    inner = made.shape[1]
    part = inner // 2
    blocks = scr.shape[0]
    start = pl.multiple_of(half[0] * inner, 128)
    copies = [
        pltpu.make_async_copy(
            w_keyval.at[pl.ds(b * 128, 128), :, pl.ds(start, inner)], scr.at[b], sems.at[0, b]
        )
        for b in range(blocks)
    ]
    for copy in copies:
        copy.start()
    row = lax.broadcasted_iota(jnp.int32, (256, 256), 0)
    column = lax.broadcasted_iota(jnp.int32, (256, 256), 1)
    source = jnp.where(row < 128, 2 * row, 2 * (row - 128) + 1)
    pick = jnp.where(column == source, 1.0, 0.0).astype(BF16)
    size = min(256, part)
    sent = []
    for b in range(blocks):
        rows = pl.ds(b * 128, 128)
        copies[b].wait()
        for s in range(0, inner, size):
            mixed = scr[b, :, :, pl.ds(s, size)].reshape(256, size)
            apart = jnp.dot(pick, mixed, preferred_element_type=F32).astype(BF16)
            if s < part:
                first_key[rows, pl.ds(s, size)] = apart[:128]
            else:
                last_key[rows, pl.ds(s - part, size)] = apart[:128]
            made[rows, pl.ds(s, size)] = apart[128:]
        sent.append(pltpu.make_async_copy(made.at[rows], w_value.at[rows], sems.at[1, b]))
        sent[-1].start()
    for copy in sent:
        copy.wait()


def prepare(half, w_keyval, inner):
    width = w_keyval.shape[0]
    return pl.pallas_call(
        prepare_kernel,
        out_shape=(
            jax.ShapeDtypeStruct((width, inner // 2), BF16),
            jax.ShapeDtypeStruct((width, inner // 2), BF16),
            jax.ShapeDtypeStruct((width, inner), BF16),
        ),
        in_specs=[SMEM_SPEC, HBM_SPEC],
        out_specs=(VMEM_SPEC, VMEM_SPEC, HBM_SPEC),
        scratch_shapes=[
            pltpu.VMEM((width // 128, 128, 2, inner), BF16),
            pltpu.VMEM((width, inner), BF16),
            pltpu.SemaphoreType.DMA((2, width // 128)),
        ],
        compiler_params=limit(51),
        cost_estimate=pl.CostEstimate(
            flops=4 * width * 256 * inner, bytes_accessed=8 * width * inner, transcendentals=0
        ),
        name="prepare",
    )(half, w_keyval)


def stage_kernel(after, whole, first, last, sems, *, axis):
    del after
    size = first.shape[axis]
    number = sems.shape[0] // 2
    step = size // number
    copies = []
    for half, out in enumerate((first, last)):
        for k in range(number):
            if axis == 0:
                source = whole.at[pl.ds(half * size + k * step, step)]
                target = out.at[pl.ds(k * step, step)]
            else:
                source = whole.at[:, pl.ds(half * size + k * step, step)]
                target = out.at[:, pl.ds(k * step, step)]
            copies.append(pltpu.make_async_copy(source, target, sems.at[half * number + k]))
    for copy in copies:
        copy.start()
    for copy in copies:
        copy.wait()


def stage(after, whole, axis):
    shape = list(whole.shape)
    shape[axis] //= 2
    part = jax.ShapeDtypeStruct(tuple(shape), BF16)
    return pl.pallas_call(
        functools.partial(stage_kernel, axis=axis),
        out_shape=(part, part),
        in_specs=[SMEM_SPEC, HBM_SPEC],
        out_specs=(VMEM_SPEC, VMEM_SPEC),
        scratch_shapes=[pltpu.SemaphoreType.DMA((8,))],
        compiler_params=limit(42),
        cost_estimate=pl.CostEstimate(
            flops=1 << 30, bytes_accessed=8 * shape[0] * shape[1], transcendentals=0
        ),
        name="stage",
    )(after, whole)


def stage_rows_kernel(after, whole, rows, gain, first, last, normed, sems):
    del after
    size = first.shape[0]
    number = sems.shape[0] // 2
    step = size // number
    copies = []
    for half, out in enumerate((first, last)):
        for k in range(number):
            copies.append(
                pltpu.make_async_copy(
                    whole.at[pl.ds(half * size + k * step, step)],
                    out.at[pl.ds(k * step, step)],
                    sems.at[half * number + k],
                )
            )
    for copy in copies:
        copy.start()
    for k in range(rows.shape[0]):
        normed[k] = norm_rows(rows[k], gain[...]).astype(BF16)
    for copy in copies:
        copy.wait()


def stage_rows(after, whole, rows, gain):
    units, width = whole.shape
    part = jax.ShapeDtypeStruct((units // 2, width), BF16)
    return pl.pallas_call(
        stage_rows_kernel,
        out_shape=(part, part, jax.ShapeDtypeStruct(rows.shape, BF16)),
        in_specs=[SMEM_SPEC, HBM_SPEC, VMEM_SPEC, VMEM_SPEC],
        out_specs=(VMEM_SPEC,) * 3,
        scratch_shapes=[pltpu.SemaphoreType.DMA((8,))],
        compiler_params=limit(42),
        cost_estimate=pl.CostEstimate(
            flops=1 << 30, bytes_accessed=4 * units * width, transcendentals=0
        ),
        name="stage_rows",
    )(after, whole, rows, gain.reshape(1, width))


def feed_kernel(index, mine, theirs, gain, *refs, patterns):
    *weights, out, normed, hidden = refs
    half = len(weights) // 2
    pairs, rows, width = mine.shape
    units = weights[0].shape[1]
    size = min(256, units)
    weight = gain[...]
    for k in range(2 * pairs):
        place = pl.multiple_of((index[0] ^ patterns[k]) * rows, rows)
        if k < pairs:
            normed[pl.ds(place, rows)] = mine[k]
        else:
            normed[pl.ds(place, rows)] = norm_rows(theirs[k - pairs], weight).astype(BF16)
    for part in range(half):
        for c in range(units // size):
            columns = pl.ds(c * size, size)
            hidden[part, :, columns] = jnp.maximum(
                jnp.dot(normed[...], weights[part][:, columns], preferred_element_type=F32), 0.0
            ).astype(BF16)
    for c in range(width // 256):
        columns = pl.ds(c * 256, 256)
        total = jnp.dot(hidden[0], weights[half][:, columns], preferred_element_type=F32)
        for part in range(1, half):
            total = total + jnp.dot(
                hidden[part], weights[half + part][:, columns], preferred_element_type=F32
            )
        out[:, columns] = total.astype(BF16)


def feed(index, mine, theirs, gain, weights, patterns):
    pairs, rows, width = mine.shape
    count = 2 * pairs * rows
    units = weights[0].shape[1] * len(weights) // 2
    return pl.pallas_call(
        functools.partial(feed_kernel, patterns=patterns),
        out_shape=jax.ShapeDtypeStruct((count, width), BF16),
        in_specs=[SMEM_SPEC] + [VMEM_SPEC] * (3 + len(weights)),
        out_specs=VMEM_SPEC,
        scratch_shapes=[
            pltpu.VMEM((count, width), BF16),
            pltpu.VMEM((len(weights) // 2, count, weights[0].shape[1]), BF16),
        ],
        compiler_params=limit(24),
        cost_estimate=pl.CostEstimate(
            flops=4 * count * width * units, bytes_accessed=4 * width * units, transcendentals=0
        ),
        name="feed",
    )(index, mine, theirs, gain.reshape(1, width), *weights)


def settle_kernel(parts, tokens, gain, encoded, memory):
    total = tokens[...].astype(F32)
    for k in range(parts.shape[0]):
        total = total + parts[k].astype(F32)
    rounded = total.astype(BF16)
    encoded[...] = rounded
    memory[...] = norm_rows(rounded, gain[...]).astype(BF16)


def settle(parts, tokens, gain):
    _, rows, width = parts.shape
    return pl.pallas_call(
        settle_kernel,
        out_shape=(
            jax.ShapeDtypeStruct((rows, width), BF16),
            jax.ShapeDtypeStruct((rows, width), BF16),
        ),
        in_specs=[VMEM_SPEC] * 3,
        out_specs=(VMEM_SPEC, VMEM_SPEC),
        compiler_params=limit(8),
        name="settle",
    )(parts, tokens, gain.reshape(1, width))


def masked_scores(query, keys, live):
    scores = lax.dot_general(
        query, keys, (((1,), (1,)), ((), ())), preferred_element_type=F32
    ) * DH ** (-0.5)
    return jnp.where(live, scores, -1e30)


def project_kernel(index, half, lengths, owners, answers, settled, query, mine, theirs, first_key, last_key, first_value, last_value, w_out, tops, totals, sums, w_last, allowed, encoded, sems, *, patterns, mp):
    inner = query.shape[1]
    part = inner // 2
    start = pl.multiple_of(half[0] * inner, 128)
    number = sems.shape[0]
    step = inner // number
    copies = [
        pltpu.make_async_copy(
            w_out.at[pl.ds(pl.multiple_of(start + k * step, 64), step)],
            w_last.at[pl.ds(k * step, step)],
            sems.at[k],
        )
        for k in range(number)
    ]
    for copy in copies:
        copy.start()
    encoded[...] = settled[...]
    count = query.shape[0]
    keys_here = 2 * mine.shape[0]
    mask = mask_rows(
        index,
        half,
        lengths,
        owners,
        answers,
        (count, 2 * keys_here),
        patterns,
        mp,
        keys_here // mp,
    )
    allowed[...] = mask[:, keys_here:]
    live = mask[:, :keys_here] > 0
    rows = jnp.concatenate([mine[...], theirs[...]], axis=0)
    size = min(256, part)
    for c in range(inner // size):
        w_key = first_key if c * size < part else last_key
        w_value = first_value if c * size < part else last_value
        local = pl.ds(c * size % part, size)
        keys = jnp.dot(rows, w_key[:, local], preferred_element_type=F32).astype(BF16)
        values = jnp.dot(rows, w_value[:, local], preferred_element_type=F32).astype(BF16)
        for h in range(size // DH):
            lanes = slice(h * DH, (h + 1) * DH)
            place = pl.ds(c * size + h * DH, DH)
            scores = masked_scores(query[:, place], keys[:, lanes], live)
            top = jnp.max(scores, axis=1, keepdims=True)
            weights = jnp.where(live, jnp.exp(scores - top), 0.0)
            total = jnp.sum(weights, axis=1, keepdims=True)
            tops[:, place] = jnp.broadcast_to(top, (count, DH))
            totals[:, place] = jnp.broadcast_to(total, (count, DH))
            sums[:, place] = jnp.dot(
                weights.astype(BF16), values[:, lanes], preferred_element_type=F32
            )
    for copy in copies:
        copy.wait()


def project(places, tables, settled, query, mine, theirs, weights, w_attn_out, patterns, mp):
    rows, width = mine.shape
    count, inner = query.shape
    return pl.pallas_call(
        functools.partial(project_kernel, patterns=patterns, mp=mp),
        out_shape=(
            jax.ShapeDtypeStruct((count, inner), F32),
            jax.ShapeDtypeStruct((count, inner), F32),
            jax.ShapeDtypeStruct((count, inner), F32),
            jax.ShapeDtypeStruct((inner, width), BF16),
            jax.ShapeDtypeStruct((count, 2 * rows), jnp.int32),
            jax.ShapeDtypeStruct(settled.shape, BF16),
        ),
        in_specs=[SMEM_SPEC] * 5 + [VMEM_SPEC] * 8 + [HBM_SPEC],
        out_specs=(VMEM_SPEC,) * 6,
        scratch_shapes=[pltpu.SemaphoreType.DMA((4,))],
        compiler_params=limit(45),
        cost_estimate=pl.CostEstimate(
            flops=8 * rows * width * inner, bytes_accessed=6 * width * inner, transcendentals=0
        ),
        name="project",
    )(*places, *tables, settled, query, mine, theirs, *weights, w_attn_out)


def attend_kernel(tops, totals, sums, mine, theirs, query, allowed, first_key, last_key, first_value, last_value, w_last, keep, give, context):
    inner = query.shape[1]
    width = keep.shape[1]
    part = inner // 2
    size = min(256, part)
    late = jnp.concatenate([mine[...], theirs[...]], axis=0)
    live = allowed[...] > 0
    for c in range(inner // size):
        w_key = first_key if c * size < part else last_key
        w_value = first_value if c * size < part else last_value
        local = pl.ds(c * size % part, size)
        keys = jnp.dot(late, w_key[:, local], preferred_element_type=F32).astype(BF16)
        values = jnp.dot(late, w_value[:, local], preferred_element_type=F32).astype(BF16)
        for h in range(size // DH):
            lanes = slice(h * DH, (h + 1) * DH)
            place = pl.ds(c * size + h * DH, DH)
            scores = masked_scores(query[:, place], keys[:, lanes], live)
            near_top = tops[:, place]
            top = jnp.maximum(near_top, jnp.max(scores, axis=1, keepdims=True))
            weights = jnp.where(live, jnp.exp(scores - top[:, :1]), 0.0)
            factor = jnp.exp(near_top - top)
            total = totals[:, place] * factor + jnp.sum(weights, axis=1, keepdims=True)
            summed = sums[:, place] * factor + jnp.dot(
                weights.astype(BF16), values[:, lanes], preferred_element_type=F32
            )
            context[:, place] = (summed * (1.0 / total)).astype(BF16)
    for c in range(width // 256):
        columns = pl.ds(c * 256, 256)
        result = jnp.dot(context[...], w_last[:, columns], preferred_element_type=F32)
        keep[:, columns] = result[: keep.shape[0]]
        give[:, columns] = result[keep.shape[0] :]


def attend(near, mine, theirs, query, allowed, weights, w_last):
    rows, width = mine.shape
    count, inner = query.shape
    return pl.pallas_call(
        attend_kernel,
        out_shape=(jax.ShapeDtypeStruct((count // 2, width), F32),) * 2,
        in_specs=[VMEM_SPEC] * 12,
        out_specs=(VMEM_SPEC, VMEM_SPEC),
        scratch_shapes=[pltpu.VMEM((count, inner), BF16)],
        compiler_params=limit(24),
        cost_estimate=pl.CostEstimate(
            flops=8 * rows * width * inner + 8 * count * rows * inner + 2 * count * inner * width,
            bytes_accessed=6 * width * inner,
            transcendentals=2 * count * rows * inner // DH,
        ),
        name="attend",
    )(*near, mine, theirs, query, allowed, *weights, w_last)


def finish_kernel(index, half, parts, states, piece):
    mp, small, _ = parts.shape
    start = index[0] * (2 * small) + half[0] * small
    row = lax.broadcasted_iota(jnp.int32, (small, states.shape[0]), 0)
    column = lax.broadcasted_iota(jnp.int32, (small, states.shape[0]), 1)
    pick = jnp.where(column == row + start, 1.0, 0.0).astype(BF16)
    total = jnp.dot(pick, states[...], preferred_element_type=F32)
    for k in range(mp):
        total = total + parts[k].astype(F32)
    piece[...] = total.astype(BF16)


def finish(index, half, parts, states):
    return pl.pallas_call(
        finish_kernel,
        out_shape=jax.ShapeDtypeStruct(parts.shape[1:], BF16),
        in_specs=[SMEM_SPEC, SMEM_SPEC, VMEM_SPEC, VMEM_SPEC],
        out_specs=VMEM_SPEC,
        compiler_params=limit(8),
        name="finish",
    )(index, half, parts, states)


def join_kernel(half, piece, other, out):
    first = jnp.where(half[0] == 0, piece[...].astype(F32), other[...].astype(F32))
    second = jnp.where(half[0] == 0, other[...].astype(F32), piece[...].astype(F32))
    out[...] = jnp.concatenate([first, second], axis=0).astype(BF16)


def join(half, piece, other):
    small, width = piece.shape
    return pl.pallas_call(
        join_kernel,
        out_shape=jax.ShapeDtypeStruct((2 * small, width), BF16),
        in_specs=[SMEM_SPEC, VMEM_SPEC, VMEM_SPEC],
        out_specs=VMEM_SPEC,
        compiler_params=limit(8),
        name="join",
    )(half, piece, other)


def per_device(
    tokens,
    enc_gain,
    w_in,
    w_out,
    final_gain,
    w_keyval,
    answer_states,
    dec_gain,
    w_query,
    w_attn_out,
    passage_lengths,
    passage_owner,
    answer_lengths,
):
    row_count = tokens.shape[0]
    width = tokens.shape[1]
    answer_count = answer_states.shape[0]
    mp = lax.axis_size("mp")
    psg = lax.axis_size("psg")
    mp_index = lax.axis_index("mp")
    psg_index = lax.axis_index("psg")
    heads = w_query.shape[1] // DH // psg
    inner = heads * DH

    half = jnp.reshape(psg_index, (1,)).astype(jnp.int32)
    index = jnp.reshape(mp_index, (1,)).astype(jnp.int32)
    held, got, patterns = spread_out(tokens, mp)
    first_in, last_in = stage(index, w_in, 1)
    first_out, last_out, held = stage_rows(index, w_out, held, enc_gain)
    partial_sums = feed(
        index, held, got, enc_gain, [first_in, last_in, first_out, last_out], patterns
    )
    parts = lax.all_to_all(partial_sums.reshape(mp, row_count, width), "mp", 0, 0)
    first_key, last_key, value = prepare(half, w_keyval, inner)

    runs = mp * row_count // 2
    small = answer_count // mp // psg
    settled, memory = settle(parts, tokens, final_gain)
    held, got, _ = spread_out(memory, mp)
    query, first_value, last_value = ask(half, answer_states, dec_gain, w_query, value, mp)
    held = held.reshape(runs, width)
    got = got.reshape(runs, width)
    held_theirs = swap_psg(held)
    weights = (first_key, last_key, first_value, last_value)
    *near, w_last, allowed, encoded = project(
        (index, half),
        (passage_lengths, passage_owner, answer_lengths),
        settled,
        query,
        held,
        held_theirs,
        weights,
        w_attn_out,
        patterns,
        mp,
    )
    got_theirs = swap_psg(got)
    keep, give = attend(near, got, got_theirs, query, allowed, weights, w_last)
    chip_sum = (keep + swap_psg(give)).astype(BF16).reshape(mp, small, width)
    answer_parts = lax.all_to_all(chip_sum, "mp", 0, 0)
    piece = finish(index, half, answer_parts, answer_states)
    return (encoded, join(half, piece, swap_psg(piece)))


def solution(mesh):
    placed = (
        P(("groups", "mp", "psg"), None),
        P(),
        P(None, "mp"),
        P("mp", None),
        P(),
        P(None, None, "mp"),
        P("groups", None),
        P(),
        P(None, "mp"),
        P("mp", None),
        P("groups"),
        P("groups"),
        P("groups"),
    )
    return jax.shard_map(
        per_device,
        mesh=mesh,
        in_specs=placed,
        out_specs=(P(("groups", "mp", "psg"), None), P(("groups", "mp"), None)),
        check_vma=False,
    )
```

```python
import functools

import jax
import jax.numpy as jnp
from jax import lax
from jax.experimental import pallas as pl
from jax.experimental.pallas import tpu as pltpu
from jax.sharding import PartitionSpec as P


DH = 128
P_SLOT = 16


eps = 1e-06


def norm_rows(states, gain):
    wide = states.astype(jnp.float32)
    factor = lax.rsqrt(jnp.mean(wide * wide, axis=-1, keepdims=True) + eps)
    return wide * factor * gain


def mask_rows(index, half, lengths, owners, answers, shape, patterns, mp, row_count):
    count, keys = shape
    psg = 2
    slot = lax.broadcasted_iota(jnp.int32, (1, keys), 1)
    run = lax.div(slot, keys // 4)
    hop = lax.div(lax.rem(slot, keys // 4), row_count) + lax.div(run, 2) * (mp // 2)
    pattern = jnp.zeros((1, keys), jnp.int32)
    for k, value in enumerate(patterns):
        pattern = jnp.where(hop == k, value, pattern)
    block = index[0] ^ pattern
    core = half[0] ^ lax.rem(run, 2)
    token = (block * psg + core) * row_count + lax.rem(slot, row_count)
    passage = lax.div(token, P_SLOT)
    place = lax.rem(token, P_SLOT)
    length = jnp.zeros((1, keys), jnp.int32)
    owner = jnp.zeros((1, keys), jnp.int32)
    for k in range(lengths.shape[0]):
        length = jnp.where(passage == k, lengths[k], length)
        owner = jnp.where(passage == k, owners[k], owner)
    owner = jnp.where(place < length, owner, -1)
    small = count // mp // psg
    row = lax.broadcasted_iota(jnp.int32, (count, 1), 0)
    side = half[0] ^ lax.div(row, mp * small)
    answer = lax.rem(lax.div(row, small), mp) * (psg * small) + side * small + lax.rem(row, small)
    question = jnp.zeros((count, 1), jnp.int32)
    end = 0
    for k in range(answers.shape[0]):
        end = end + answers[k]
        question = question + jnp.where(answer >= end, 1, 0)
    return jnp.where(owner == question, 1, 0)


def spread_out(x, mp):
    quarter = mp // 4
    patterns = [0]
    blocks = [x[None]]
    for k in (3, 2, 1):
        blocks.append(lax.ppermute(x[None], "mp", [(j, j ^ (k * quarter)) for j in range(mp)]))
        patterns.append(k * quarter)
    held = jnp.concatenate(blocks, axis=0)
    step = quarter // 2
    while step > 0:
        got = lax.ppermute(held, "mp", [(j, j ^ step) for j in range(mp)])
        patterns = patterns + [p ^ step for p in patterns]
        if step > 1:
            held = jnp.concatenate([held, got], axis=0)
        step //= 2
    return held, got, patterns


def swap_psg(x):
    return lax.ppermute(x, "psg", [(0, 1), (1, 0)])


BF16 = jnp.bfloat16
F32 = jnp.float32
SMEM_SPEC = pl.BlockSpec(memory_space=pltpu.SMEM)
VMEM_SPEC = pl.BlockSpec(memory_space=pltpu.VMEM)
HBM_SPEC = pl.BlockSpec(memory_space=pltpu.HBM)


def limit(mib):
    return pltpu.CompilerParams(vmem_limit_bytes=mib << 20)


def ask_kernel(half, states, gain, w_query, value, query, first_value, last_value, scr, sems, *, mp):
    inner = query.shape[1]
    part = first_value.shape[1]
    size = scr.shape[2]
    chunks = inner // size
    start = pl.multiple_of(half[0] * inner, 128)
    copies = [
        pltpu.make_async_copy(
            w_query.at[:, pl.ds(pl.multiple_of(start + c * size, 128), size)],
            scr.at[c],
            sems.at[c],
        )
        for c in range(chunks)
    ]
    others = [
        pltpu.make_async_copy(value.at[:, pl.ds(0, part)], first_value, sems.at[chunks]),
        pltpu.make_async_copy(value.at[:, pl.ds(part, part)], last_value, sems.at[chunks + 1]),
    ]
    for copy in copies + others:
        copy.start()
    normed = norm_rows(states[...], gain[...]).astype(BF16)
    count = states.shape[0]
    small = count // mp // 2
    row = lax.broadcasted_iota(jnp.int32, (count, count), 0)
    column = lax.broadcasted_iota(jnp.int32, (count, count), 1)
    side = half[0] ^ lax.div(row, mp * small)
    source = lax.rem(lax.div(row, small), mp) * (2 * small) + side * small + lax.rem(row, small)
    pick = jnp.where(column == source, 1.0, 0.0).astype(BF16)
    normed = jnp.dot(pick, normed, preferred_element_type=F32).astype(BF16)
    for c in range(chunks):
        copies[c].wait()
        query[:, pl.ds(c * size, size)] = jnp.dot(
            normed, scr[c], preferred_element_type=F32
        ).astype(BF16)
    for copy in others:
        copy.wait()


def ask(half, states, gain, w_query, value, mp):
    count, width = states.shape
    inner = value.shape[1]
    size = min(256, inner)
    return pl.pallas_call(
        functools.partial(ask_kernel, mp=mp),
        out_shape=(
            jax.ShapeDtypeStruct((count, inner), BF16),
            jax.ShapeDtypeStruct((width, inner // 2), BF16),
            jax.ShapeDtypeStruct((width, inner // 2), BF16),
        ),
        in_specs=[SMEM_SPEC, VMEM_SPEC, VMEM_SPEC, HBM_SPEC, HBM_SPEC],
        out_specs=(VMEM_SPEC,) * 3,
        scratch_shapes=[
            pltpu.VMEM((inner // size, width, size), BF16),
            pltpu.SemaphoreType.DMA((inner // size + 2,)),
        ],
        compiler_params=limit(50),
        cost_estimate=pl.CostEstimate(
            flops=1 << 30, bytes_accessed=4 * width * inner, transcendentals=0
        ),
        name="ask",
    )(half, states, gain.reshape(1, width), w_query, value)


def prepare_kernel(half, w_keyval, first_key, last_key, w_value, scr, made, sems):
    inner = made.shape[1]
    part = inner // 2
    blocks = scr.shape[0]
    start = pl.multiple_of(half[0] * inner, 128)
    copies = [
        pltpu.make_async_copy(
            w_keyval.at[pl.ds(b * 128, 128), :, pl.ds(start, inner)], scr.at[b], sems.at[0, b]
        )
        for b in range(blocks)
    ]
    for copy in copies:
        copy.start()
    row = lax.broadcasted_iota(jnp.int32, (256, 256), 0)
    column = lax.broadcasted_iota(jnp.int32, (256, 256), 1)
    source = jnp.where(row < 128, 2 * row, 2 * (row - 128) + 1)
    pick = jnp.where(column == source, 1.0, 0.0).astype(BF16)
    size = min(256, part)
    sent = []
    for b in range(blocks):
        rows = pl.ds(b * 128, 128)
        copies[b].wait()
        for s in range(0, inner, size):
            mixed = scr[b, :, :, pl.ds(s, size)].reshape(256, size)
            apart = jnp.dot(pick, mixed, preferred_element_type=F32).astype(BF16)
            if s < part:
                first_key[rows, pl.ds(s, size)] = apart[:128]
            else:
                last_key[rows, pl.ds(s - part, size)] = apart[:128]
            made[rows, pl.ds(s, size)] = apart[128:]
        sent.append(pltpu.make_async_copy(made.at[rows], w_value.at[rows], sems.at[1, b]))
        sent[-1].start()
    for copy in sent:
        copy.wait()


def prepare(half, w_keyval, inner):
    width = w_keyval.shape[0]
    return pl.pallas_call(
        prepare_kernel,
        out_shape=(
            jax.ShapeDtypeStruct((width, inner // 2), BF16),
            jax.ShapeDtypeStruct((width, inner // 2), BF16),
            jax.ShapeDtypeStruct((width, inner), BF16),
        ),
        in_specs=[SMEM_SPEC, HBM_SPEC],
        out_specs=(VMEM_SPEC, VMEM_SPEC, HBM_SPEC),
        scratch_shapes=[
            pltpu.VMEM((width // 128, 128, 2, inner), BF16),
            pltpu.VMEM((width, inner), BF16),
            pltpu.SemaphoreType.DMA((2, width // 128)),
        ],
        compiler_params=limit(51),
        cost_estimate=pl.CostEstimate(
            flops=4 * width * 256 * inner, bytes_accessed=8 * width * inner, transcendentals=0
        ),
        name="prepare",
    )(half, w_keyval)


def stage_kernel(after, whole, first, last, sems, *, axis):
    del after
    size = first.shape[axis]
    number = sems.shape[0] // 2
    step = size // number
    copies = []
    for half, out in enumerate((first, last)):
        for k in range(number):
            if axis == 0:
                source = whole.at[pl.ds(half * size + k * step, step)]
                target = out.at[pl.ds(k * step, step)]
            else:
                source = whole.at[:, pl.ds(half * size + k * step, step)]
                target = out.at[:, pl.ds(k * step, step)]
            copies.append(pltpu.make_async_copy(source, target, sems.at[half * number + k]))
    for copy in copies:
        copy.start()
    for copy in copies:
        copy.wait()


def stage(after, whole, axis):
    shape = list(whole.shape)
    shape[axis] //= 2
    part = jax.ShapeDtypeStruct(tuple(shape), BF16)
    return pl.pallas_call(
        functools.partial(stage_kernel, axis=axis),
        out_shape=(part, part),
        in_specs=[SMEM_SPEC, HBM_SPEC],
        out_specs=(VMEM_SPEC, VMEM_SPEC),
        scratch_shapes=[pltpu.SemaphoreType.DMA((8,))],
        compiler_params=limit(42),
        cost_estimate=pl.CostEstimate(
            flops=1 << 30, bytes_accessed=8 * shape[0] * shape[1], transcendentals=0
        ),
        name="stage",
    )(after, whole)


def stage_rows_kernel(after, whole, rows, gain, first, last, normed, sems):
    del after
    size = first.shape[0]
    number = sems.shape[0] // 2
    step = size // number
    copies = []
    for half, out in enumerate((first, last)):
        for k in range(number):
            copies.append(
                pltpu.make_async_copy(
                    whole.at[pl.ds(half * size + k * step, step)],
                    out.at[pl.ds(k * step, step)],
                    sems.at[half * number + k],
                )
            )
    for copy in copies:
        copy.start()
    for k in range(rows.shape[0]):
        normed[k] = norm_rows(rows[k], gain[...]).astype(BF16)
    for copy in copies:
        copy.wait()


def stage_rows(after, whole, rows, gain):
    units, width = whole.shape
    part = jax.ShapeDtypeStruct((units // 2, width), BF16)
    return pl.pallas_call(
        stage_rows_kernel,
        out_shape=(part, part, jax.ShapeDtypeStruct(rows.shape, BF16)),
        in_specs=[SMEM_SPEC, HBM_SPEC, VMEM_SPEC, VMEM_SPEC],
        out_specs=(VMEM_SPEC,) * 3,
        scratch_shapes=[pltpu.SemaphoreType.DMA((8,))],
        compiler_params=limit(42),
        cost_estimate=pl.CostEstimate(
            flops=1 << 30, bytes_accessed=4 * units * width, transcendentals=0
        ),
        name="stage_rows",
    )(after, whole, rows, gain.reshape(1, width))


def feed_kernel(index, mine, theirs, gain, *refs, patterns):
    *weights, out, normed, hidden = refs
    half = len(weights) // 2
    pairs, rows, width = mine.shape
    units = weights[0].shape[1]
    size = min(256, units)
    weight = gain[...]
    for k in range(2 * pairs):
        place = pl.multiple_of((index[0] ^ patterns[k]) * rows, rows)
        if k < pairs:
            normed[pl.ds(place, rows)] = mine[k]
        else:
            normed[pl.ds(place, rows)] = norm_rows(theirs[k - pairs], weight).astype(BF16)
    for part in range(half):
        for c in range(units // size):
            columns = pl.ds(c * size, size)
            hidden[part, :, columns] = jnp.maximum(
                jnp.dot(normed[...], weights[part][:, columns], preferred_element_type=F32), 0.0
            ).astype(BF16)
    for c in range(width // 256):
        columns = pl.ds(c * 256, 256)
        total = jnp.dot(hidden[0], weights[half][:, columns], preferred_element_type=F32)
        for part in range(1, half):
            total = total + jnp.dot(
                hidden[part], weights[half + part][:, columns], preferred_element_type=F32
            )
        out[:, columns] = total.astype(BF16)


def feed(index, mine, theirs, gain, weights, patterns):
    pairs, rows, width = mine.shape
    count = 2 * pairs * rows
    units = weights[0].shape[1] * len(weights) // 2
    return pl.pallas_call(
        functools.partial(feed_kernel, patterns=patterns),
        out_shape=jax.ShapeDtypeStruct((count, width), BF16),
        in_specs=[SMEM_SPEC] + [VMEM_SPEC] * (3 + len(weights)),
        out_specs=VMEM_SPEC,
        scratch_shapes=[
            pltpu.VMEM((count, width), BF16),
            pltpu.VMEM((len(weights) // 2, count, weights[0].shape[1]), BF16),
        ],
        compiler_params=limit(24),
        cost_estimate=pl.CostEstimate(
            flops=4 * count * width * units, bytes_accessed=4 * width * units, transcendentals=0
        ),
        name="feed",
    )(index, mine, theirs, gain.reshape(1, width), *weights)


def settle_kernel(parts, tokens, gain, encoded, memory):
    total = tokens[...].astype(F32)
    for k in range(parts.shape[0]):
        total = total + parts[k].astype(F32)
    rounded = total.astype(BF16)
    encoded[...] = rounded
    memory[...] = norm_rows(rounded, gain[...]).astype(BF16)


def settle(parts, tokens, gain):
    _, rows, width = parts.shape
    return pl.pallas_call(
        settle_kernel,
        out_shape=(
            jax.ShapeDtypeStruct((rows, width), BF16),
            jax.ShapeDtypeStruct((rows, width), BF16),
        ),
        in_specs=[VMEM_SPEC] * 3,
        out_specs=(VMEM_SPEC, VMEM_SPEC),
        compiler_params=limit(8),
        name="settle",
    )(parts, tokens, gain.reshape(1, width))


def project_kernel(index, half, lengths, owners, answers, settled, mine, theirs, first_key, last_key, first_value, last_value, w_out, keys, values, w_last, allowed, encoded, sems, *, patterns, mp):
    inner = keys.shape[1]
    part = inner // 2
    start = pl.multiple_of(half[0] * inner, 128)
    number = sems.shape[0]
    step = inner // number
    copies = [
        pltpu.make_async_copy(
            w_out.at[pl.ds(pl.multiple_of(start + k * step, 64), step)],
            w_last.at[pl.ds(k * step, step)],
            sems.at[k],
        )
        for k in range(number)
    ]
    for copy in copies:
        copy.start()
    encoded[...] = settled[...]
    row_count = 2 * mine.shape[0] // mp
    allowed[...] = mask_rows(
        index, half, lengths, owners, answers, allowed.shape, patterns, mp, row_count
    )
    rows = jnp.concatenate([mine[...], theirs[...]], axis=0)
    size = min(256, part)
    for k, w_key in enumerate((first_key, last_key)):
        for c in range(part // size):
            keys[:, pl.ds(k * part + c * size, size)] = jnp.dot(
                rows, w_key[:, pl.ds(c * size, size)], preferred_element_type=F32
            ).astype(BF16)
    for k, w_value in enumerate((first_value, last_value)):
        for c in range(part // size):
            values[:, pl.ds(k * part + c * size, size)] = jnp.dot(
                rows, w_value[:, pl.ds(c * size, size)], preferred_element_type=F32
            ).astype(BF16)
    for copy in copies:
        copy.wait()


def project(places, tables, settled, mine, theirs, weights, w_attn_out, patterns, count, mp):
    rows, width = mine.shape
    inner = 2 * weights[0].shape[1]
    return pl.pallas_call(
        functools.partial(project_kernel, patterns=patterns, mp=mp),
        out_shape=(
            jax.ShapeDtypeStruct((2 * rows, inner), BF16),
            jax.ShapeDtypeStruct((2 * rows, inner), BF16),
            jax.ShapeDtypeStruct((inner, width), BF16),
            jax.ShapeDtypeStruct((count, 4 * rows), jnp.int32),
            jax.ShapeDtypeStruct(settled.shape, BF16),
        ),
        in_specs=[SMEM_SPEC] * 5 + [VMEM_SPEC] * 7 + [HBM_SPEC],
        out_specs=(VMEM_SPEC,) * 5,
        scratch_shapes=[pltpu.SemaphoreType.DMA((4,))],
        compiler_params=limit(46),
        cost_estimate=pl.CostEstimate(
            flops=8 * rows * width * inner, bytes_accessed=6 * width * inner, transcendentals=0
        ),
        name="project",
    )(*places, *tables, settled, mine, theirs, *weights, w_attn_out)


def attend_kernel(near_keys, near_values, mine, theirs, query, allowed, first_key, last_key, first_value, last_value, w_last, keep, give, context):
    rows, inner = near_keys.shape
    width = keep.shape[1]
    part = inner // 2
    size = min(256, part)
    late = jnp.concatenate([mine[...], theirs[...]], axis=0)
    near = allowed[:, :rows] > 0
    far = allowed[:, rows:] > 0
    for c in range(inner // size):
        columns = pl.ds(c * size, size)
        w_key = first_key if c * size < part else last_key
        w_value = first_value if c * size < part else last_value
        local = pl.ds(c * size % part, size)
        far_keys = jnp.dot(late, w_key[:, local], preferred_element_type=F32).astype(BF16)
        far_values = jnp.dot(late, w_value[:, local], preferred_element_type=F32).astype(BF16)
        keys = jnp.concatenate([near_keys[:, columns], far_keys], axis=0)
        values = jnp.concatenate([near_values[:, columns], far_values], axis=0)
        for h in range(size // DH):
            lanes = slice(h * DH, (h + 1) * DH)
            place = pl.ds(c * size + h * DH, DH)
            scores = lax.dot_general(
                query[:, place],
                keys[:, lanes],
                (((1,), (1,)), ((), ())),
                preferred_element_type=F32,
            ) * DH ** (-0.5)
            near_scores = jnp.where(near, scores[:, :rows], -1e30)
            far_scores = jnp.where(far, scores[:, rows:], -1e30)
            top = jnp.max(jnp.maximum(near_scores, far_scores), axis=1, keepdims=True)
            near_weights = jnp.where(near, jnp.exp(near_scores - top), 0.0)
            far_weights = jnp.where(far, jnp.exp(far_scores - top), 0.0)
            total = jnp.sum(near_weights + far_weights, axis=1, keepdims=True)
            weights = jnp.concatenate([near_weights, far_weights], axis=1).astype(BF16)
            summed = jnp.dot(weights, values[:, lanes], preferred_element_type=F32)
            context[:, place] = (summed * (1.0 / total)).astype(BF16)
    for c in range(width // 256):
        columns = pl.ds(c * 256, 256)
        result = jnp.dot(context[...], w_last[:, columns], preferred_element_type=F32)
        keep[:, columns] = result[: keep.shape[0]]
        give[:, columns] = result[keep.shape[0] :]


def attend(near_keys, near_values, mine, theirs, query, allowed, weights, w_last):
    rows = near_keys.shape[0]
    width = mine.shape[1]
    count, inner = query.shape
    return pl.pallas_call(
        attend_kernel,
        out_shape=(jax.ShapeDtypeStruct((count // 2, width), F32),) * 2,
        in_specs=[VMEM_SPEC] * 11,
        out_specs=(VMEM_SPEC, VMEM_SPEC),
        scratch_shapes=[pltpu.VMEM((count, inner), BF16)],
        compiler_params=limit(24),
        cost_estimate=pl.CostEstimate(
            flops=4 * rows * width * inner + 8 * count * rows * inner + 2 * count * inner * width,
            bytes_accessed=6 * width * inner,
            transcendentals=2 * count * rows * inner // DH,
        ),
        name="attend",
    )(near_keys, near_values, mine, theirs, query, allowed, *weights, w_last)


def finish_kernel(index, half, parts, states, piece):
    mp, small, _ = parts.shape
    start = index[0] * (2 * small) + half[0] * small
    row = lax.broadcasted_iota(jnp.int32, (small, states.shape[0]), 0)
    column = lax.broadcasted_iota(jnp.int32, (small, states.shape[0]), 1)
    pick = jnp.where(column == row + start, 1.0, 0.0).astype(BF16)
    total = jnp.dot(pick, states[...], preferred_element_type=F32)
    for k in range(mp):
        total = total + parts[k].astype(F32)
    piece[...] = total.astype(BF16)


def finish(index, half, parts, states):
    return pl.pallas_call(
        finish_kernel,
        out_shape=jax.ShapeDtypeStruct(parts.shape[1:], BF16),
        in_specs=[SMEM_SPEC, SMEM_SPEC, VMEM_SPEC, VMEM_SPEC],
        out_specs=VMEM_SPEC,
        compiler_params=limit(8),
        name="finish",
    )(index, half, parts, states)


def join_kernel(half, piece, other, out):
    first = jnp.where(half[0] == 0, piece[...].astype(F32), other[...].astype(F32))
    second = jnp.where(half[0] == 0, other[...].astype(F32), piece[...].astype(F32))
    out[...] = jnp.concatenate([first, second], axis=0).astype(BF16)


def join(half, piece, other):
    small, width = piece.shape
    return pl.pallas_call(
        join_kernel,
        out_shape=jax.ShapeDtypeStruct((2 * small, width), BF16),
        in_specs=[SMEM_SPEC, VMEM_SPEC, VMEM_SPEC],
        out_specs=VMEM_SPEC,
        compiler_params=limit(8),
        name="join",
    )(half, piece, other)


def per_device(
    tokens,
    enc_gain,
    w_in,
    w_out,
    final_gain,
    w_keyval,
    answer_states,
    dec_gain,
    w_query,
    w_attn_out,
    passage_lengths,
    passage_owner,
    answer_lengths,
):
    row_count = tokens.shape[0]
    width = tokens.shape[1]
    answer_count = answer_states.shape[0]
    mp = lax.axis_size("mp")
    psg = lax.axis_size("psg")
    mp_index = lax.axis_index("mp")
    psg_index = lax.axis_index("psg")
    heads = w_query.shape[1] // DH // psg
    inner = heads * DH

    half = jnp.reshape(psg_index, (1,)).astype(jnp.int32)
    index = jnp.reshape(mp_index, (1,)).astype(jnp.int32)
    held, got, patterns = spread_out(tokens, mp)
    first_in, last_in = stage(index, w_in, 1)
    first_out, last_out, held = stage_rows(index, w_out, held, enc_gain)
    partial_sums = feed(
        index, held, got, enc_gain, [first_in, last_in, first_out, last_out], patterns
    )
    parts = lax.all_to_all(partial_sums.reshape(mp, row_count, width), "mp", 0, 0)
    first_key, last_key, value = prepare(half, w_keyval, inner)

    runs = mp * row_count // 2
    small = answer_count // mp // psg
    settled, memory = settle(parts, tokens, final_gain)
    held, got, _ = spread_out(memory, mp)
    query, first_value, last_value = ask(half, answer_states, dec_gain, w_query, value, mp)
    held = held.reshape(runs, width)
    got = got.reshape(runs, width)
    held_theirs = swap_psg(held)
    weights = (first_key, last_key, first_value, last_value)
    near_keys, near_values, w_last, allowed, encoded = project(
        (index, half),
        (passage_lengths, passage_owner, answer_lengths),
        settled,
        held,
        held_theirs,
        weights,
        w_attn_out,
        patterns,
        answer_count,
        mp,
    )
    got_theirs = swap_psg(got)
    keep, give = attend(
        near_keys, near_values, got, got_theirs, query, allowed, weights, w_last
    )
    chip_sum = (keep + swap_psg(give)).astype(BF16).reshape(mp, small, width)
    answer_parts = lax.all_to_all(chip_sum, "mp", 0, 0)
    piece = finish(index, half, answer_parts, answer_states)
    return (encoded, join(half, piece, swap_psg(piece)))


def solution(mesh):
    placed = (
        P(("groups", "mp", "psg"), None),
        P(),
        P(None, "mp"),
        P("mp", None),
        P(),
        P(None, None, "mp"),
        P("groups", None),
        P(),
        P(None, "mp"),
        P("mp", None),
        P("groups"),
        P("groups"),
        P("groups"),
    )
    return jax.shard_map(
        per_device,
        mesh=mesh,
        in_specs=placed,
        out_specs=(P(("groups", "mp", "psg"), None), P(("groups", "mp"), None)),
        check_vma=False,
    )
```

```python
import functools

import jax
import jax.numpy as jnp
from jax import lax
from jax.experimental import pallas as pl
from jax.experimental.pallas import tpu as pltpu
from jax.sharding import PartitionSpec as P


DH = 128
P_SLOT = 16


eps = 1e-06


def norm_rows(states, gain):
    wide = states.astype(jnp.float32)
    factor = lax.rsqrt(jnp.mean(wide * wide, axis=-1, keepdims=True) + eps)
    return wide * factor * gain


def mask_rows(index, half, lengths, owners, answers, shape, patterns, mp, row_count):
    count, keys = shape
    psg = 2
    slot = lax.broadcasted_iota(jnp.int32, (1, keys), 1)
    run = lax.div(slot, keys // 4)
    hop = lax.div(lax.rem(slot, keys // 4), row_count) + lax.div(run, 2) * (mp // 2)
    pattern = jnp.zeros((1, keys), jnp.int32)
    for k, value in enumerate(patterns):
        pattern = jnp.where(hop == k, value, pattern)
    block = index[0] ^ pattern
    core = half[0] ^ lax.rem(run, 2)
    token = (block * psg + core) * row_count + lax.rem(slot, row_count)
    passage = lax.div(token, P_SLOT)
    place = lax.rem(token, P_SLOT)
    length = jnp.zeros((1, keys), jnp.int32)
    owner = jnp.zeros((1, keys), jnp.int32)
    for k in range(lengths.shape[0]):
        length = jnp.where(passage == k, lengths[k], length)
        owner = jnp.where(passage == k, owners[k], owner)
    owner = jnp.where(place < length, owner, -1)
    small = count // mp // psg
    row = lax.broadcasted_iota(jnp.int32, (count, 1), 0)
    side = half[0] ^ lax.div(row, mp * small)
    answer = lax.rem(lax.div(row, small), mp) * (psg * small) + side * small + lax.rem(row, small)
    question = jnp.zeros((count, 1), jnp.int32)
    end = 0
    for k in range(answers.shape[0]):
        end = end + answers[k]
        question = question + jnp.where(answer >= end, 1, 0)
    return jnp.where(owner == question, 1, 0)


def spread_out(x, mp):
    quarter = mp // 4
    patterns = [0]
    blocks = [x[None]]
    for k in (3, 2, 1):
        blocks.append(lax.ppermute(x[None], "mp", [(j, j ^ (k * quarter)) for j in range(mp)]))
        patterns.append(k * quarter)
    held = jnp.concatenate(blocks, axis=0)
    step = quarter // 2
    while step > 0:
        got = lax.ppermute(held, "mp", [(j, j ^ step) for j in range(mp)])
        patterns = patterns + [p ^ step for p in patterns]
        if step > 1:
            held = jnp.concatenate([held, got], axis=0)
        step //= 2
    return held, got, patterns


def swap_psg(x):
    return lax.ppermute(x, "psg", [(0, 1), (1, 0)])


BF16 = jnp.bfloat16
F32 = jnp.float32
SMEM_SPEC = pl.BlockSpec(memory_space=pltpu.SMEM)
VMEM_SPEC = pl.BlockSpec(memory_space=pltpu.VMEM)
HBM_SPEC = pl.BlockSpec(memory_space=pltpu.HBM)


def limit(mib):
    return pltpu.CompilerParams(vmem_limit_bytes=mib << 20)


def ask_kernel(half, states, gain, w_query, value, query, first_value, last_value, scr, sems, *, mp):
    inner = query.shape[1]
    part = first_value.shape[1]
    size = scr.shape[2]
    chunks = inner // size
    start = pl.multiple_of(half[0] * inner, 128)
    copies = [
        pltpu.make_async_copy(
            w_query.at[:, pl.ds(pl.multiple_of(start + c * size, 128), size)],
            scr.at[c],
            sems.at[c],
        )
        for c in range(chunks)
    ]
    others = [
        pltpu.make_async_copy(value.at[:, pl.ds(0, part)], first_value, sems.at[chunks]),
        pltpu.make_async_copy(value.at[:, pl.ds(part, part)], last_value, sems.at[chunks + 1]),
    ]
    for copy in copies + others:
        copy.start()
    normed = norm_rows(states[...], gain[...]).astype(BF16)
    count = states.shape[0]
    small = count // mp // 2
    row = lax.broadcasted_iota(jnp.int32, (count, count), 0)
    column = lax.broadcasted_iota(jnp.int32, (count, count), 1)
    side = half[0] ^ lax.div(row, mp * small)
    source = lax.rem(lax.div(row, small), mp) * (2 * small) + side * small + lax.rem(row, small)
    pick = jnp.where(column == source, 1.0, 0.0).astype(BF16)
    normed = jnp.dot(pick, normed, preferred_element_type=F32).astype(BF16)
    for c in range(chunks):
        copies[c].wait()
        query[:, pl.ds(c * size, size)] = jnp.dot(
            normed, scr[c], preferred_element_type=F32
        ).astype(BF16)
    for copy in others:
        copy.wait()


def ask(half, states, gain, w_query, value, mp):
    count, width = states.shape
    inner = value.shape[1]
    size = min(256, inner)
    return pl.pallas_call(
        functools.partial(ask_kernel, mp=mp),
        out_shape=(
            jax.ShapeDtypeStruct((count, inner), BF16),
            jax.ShapeDtypeStruct((width, inner // 2), BF16),
            jax.ShapeDtypeStruct((width, inner // 2), BF16),
        ),
        in_specs=[SMEM_SPEC, VMEM_SPEC, VMEM_SPEC, HBM_SPEC, HBM_SPEC],
        out_specs=(VMEM_SPEC,) * 3,
        scratch_shapes=[
            pltpu.VMEM((inner // size, width, size), BF16),
            pltpu.SemaphoreType.DMA((inner // size + 2,)),
        ],
        compiler_params=limit(50),
        cost_estimate=pl.CostEstimate(
            flops=1 << 30, bytes_accessed=4 * width * inner, transcendentals=0
        ),
        name="ask",
    )(half, states, gain.reshape(1, width), w_query, value)


def prepare_kernel(half, w_keyval, first_key, last_key, w_value, scr, made, sems):
    inner = made.shape[1]
    part = inner // 2
    blocks = scr.shape[0]
    start = pl.multiple_of(half[0] * inner, 128)
    copies = [
        pltpu.make_async_copy(
            w_keyval.at[pl.ds(b * 128, 128), :, pl.ds(start, inner)], scr.at[b], sems.at[0, b]
        )
        for b in range(blocks)
    ]
    for copy in copies:
        copy.start()
    row = lax.broadcasted_iota(jnp.int32, (256, 256), 0)
    column = lax.broadcasted_iota(jnp.int32, (256, 256), 1)
    source = jnp.where(row < 128, 2 * row, 2 * (row - 128) + 1)
    pick = jnp.where(column == source, 1.0, 0.0).astype(BF16)
    size = min(256, part)
    sent = []
    for b in range(blocks):
        rows = pl.ds(b * 128, 128)
        copies[b].wait()
        for s in range(0, inner, size):
            mixed = scr[b, :, :, pl.ds(s, size)].reshape(256, size)
            apart = jnp.dot(pick, mixed, preferred_element_type=F32).astype(BF16)
            if s < part:
                first_key[rows, pl.ds(s, size)] = apart[:128]
            else:
                last_key[rows, pl.ds(s - part, size)] = apart[:128]
            made[rows, pl.ds(s, size)] = apart[128:]
        sent.append(pltpu.make_async_copy(made.at[rows], w_value.at[rows], sems.at[1, b]))
        sent[-1].start()
    for copy in sent:
        copy.wait()


def prepare(half, w_keyval, inner):
    width = w_keyval.shape[0]
    return pl.pallas_call(
        prepare_kernel,
        out_shape=(
            jax.ShapeDtypeStruct((width, inner // 2), BF16),
            jax.ShapeDtypeStruct((width, inner // 2), BF16),
            jax.ShapeDtypeStruct((width, inner), BF16),
        ),
        in_specs=[SMEM_SPEC, HBM_SPEC],
        out_specs=(VMEM_SPEC, VMEM_SPEC, HBM_SPEC),
        scratch_shapes=[
            pltpu.VMEM((width // 128, 128, 2, inner), BF16),
            pltpu.VMEM((width, inner), BF16),
            pltpu.SemaphoreType.DMA((2, width // 128)),
        ],
        compiler_params=limit(51),
        cost_estimate=pl.CostEstimate(
            flops=4 * width * 256 * inner, bytes_accessed=8 * width * inner, transcendentals=0
        ),
        name="prepare",
    )(half, w_keyval)


def stage_kernel(after, whole, first, last, sems, *, axis):
    del after
    size = first.shape[axis]
    number = sems.shape[0] // 2
    step = size // number
    copies = []
    for half, out in enumerate((first, last)):
        for k in range(number):
            if axis == 0:
                source = whole.at[pl.ds(half * size + k * step, step)]
                target = out.at[pl.ds(k * step, step)]
            else:
                source = whole.at[:, pl.ds(half * size + k * step, step)]
                target = out.at[:, pl.ds(k * step, step)]
            copies.append(pltpu.make_async_copy(source, target, sems.at[half * number + k]))
    for copy in copies:
        copy.start()
    for copy in copies:
        copy.wait()


def stage(after, whole, axis):
    shape = list(whole.shape)
    shape[axis] //= 2
    part = jax.ShapeDtypeStruct(tuple(shape), BF16)
    return pl.pallas_call(
        functools.partial(stage_kernel, axis=axis),
        out_shape=(part, part),
        in_specs=[SMEM_SPEC, HBM_SPEC],
        out_specs=(VMEM_SPEC, VMEM_SPEC),
        scratch_shapes=[pltpu.SemaphoreType.DMA((8,))],
        compiler_params=limit(42),
        cost_estimate=pl.CostEstimate(
            flops=1 << 30, bytes_accessed=8 * shape[0] * shape[1], transcendentals=0
        ),
        name="stage",
    )(after, whole)


def stage_rows_kernel(after, whole, rows, gain, first, last, normed, sems):
    del after
    size = first.shape[0]
    number = sems.shape[0] // 2
    step = size // number
    copies = []
    for half, out in enumerate((first, last)):
        for k in range(number):
            copies.append(
                pltpu.make_async_copy(
                    whole.at[pl.ds(half * size + k * step, step)],
                    out.at[pl.ds(k * step, step)],
                    sems.at[half * number + k],
                )
            )
    for copy in copies:
        copy.start()
    for k in range(rows.shape[0]):
        normed[k] = norm_rows(rows[k], gain[...]).astype(BF16)
    for copy in copies:
        copy.wait()


def stage_rows(after, whole, rows, gain):
    units, width = whole.shape
    part = jax.ShapeDtypeStruct((units // 2, width), BF16)
    return pl.pallas_call(
        stage_rows_kernel,
        out_shape=(part, part, jax.ShapeDtypeStruct(rows.shape, BF16)),
        in_specs=[SMEM_SPEC, HBM_SPEC, VMEM_SPEC, VMEM_SPEC],
        out_specs=(VMEM_SPEC,) * 3,
        scratch_shapes=[pltpu.SemaphoreType.DMA((8,))],
        compiler_params=limit(42),
        cost_estimate=pl.CostEstimate(
            flops=1 << 30, bytes_accessed=4 * units * width, transcendentals=0
        ),
        name="stage_rows",
    )(after, whole, rows, gain.reshape(1, width))


def feed_kernel(index, mine, theirs, gain, *refs, patterns):
    *weights, out, normed, hidden = refs
    half = len(weights) // 2
    pairs, rows, width = mine.shape
    units = weights[0].shape[1]
    size = min(256, units)
    weight = gain[...]
    for k in range(2 * pairs):
        place = pl.multiple_of((index[0] ^ patterns[k]) * rows, rows)
        if k < pairs:
            normed[pl.ds(place, rows)] = mine[k]
        else:
            normed[pl.ds(place, rows)] = norm_rows(theirs[k - pairs], weight).astype(BF16)
    for part in range(half):
        for c in range(units // size):
            columns = pl.ds(c * size, size)
            hidden[part, :, columns] = jnp.maximum(
                jnp.dot(normed[...], weights[part][:, columns], preferred_element_type=F32), 0.0
            ).astype(BF16)
    for c in range(width // 256):
        columns = pl.ds(c * 256, 256)
        total = jnp.dot(hidden[0], weights[half][:, columns], preferred_element_type=F32)
        for part in range(1, half):
            total = total + jnp.dot(
                hidden[part], weights[half + part][:, columns], preferred_element_type=F32
            )
        out[:, columns] = total.astype(BF16)


def feed(index, mine, theirs, gain, weights, patterns):
    pairs, rows, width = mine.shape
    count = 2 * pairs * rows
    units = weights[0].shape[1] * len(weights) // 2
    return pl.pallas_call(
        functools.partial(feed_kernel, patterns=patterns),
        out_shape=jax.ShapeDtypeStruct((count, width), BF16),
        in_specs=[SMEM_SPEC] + [VMEM_SPEC] * (3 + len(weights)),
        out_specs=VMEM_SPEC,
        scratch_shapes=[
            pltpu.VMEM((count, width), BF16),
            pltpu.VMEM((len(weights) // 2, count, weights[0].shape[1]), BF16),
        ],
        compiler_params=limit(24),
        cost_estimate=pl.CostEstimate(
            flops=4 * count * width * units, bytes_accessed=4 * width * units, transcendentals=0
        ),
        name="feed",
    )(index, mine, theirs, gain.reshape(1, width), *weights)


def settle_kernel(parts, tokens, gain, encoded, memory):
    total = tokens[...].astype(F32)
    for k in range(parts.shape[0]):
        total = total + parts[k].astype(F32)
    rounded = total.astype(BF16)
    encoded[...] = rounded
    memory[...] = norm_rows(rounded, gain[...]).astype(BF16)


def settle(parts, tokens, gain):
    _, rows, width = parts.shape
    return pl.pallas_call(
        settle_kernel,
        out_shape=(
            jax.ShapeDtypeStruct((rows, width), BF16),
            jax.ShapeDtypeStruct((rows, width), BF16),
        ),
        in_specs=[VMEM_SPEC] * 3,
        out_specs=(VMEM_SPEC, VMEM_SPEC),
        compiler_params=limit(8),
        name="settle",
    )(parts, tokens, gain.reshape(1, width))


def project_kernel(index, half, lengths, owners, answers, settled, mine, theirs, first_key, last_key, first_value, last_value, w_out, keys, values, w_last, allowed, encoded, sems, *, patterns, mp):
    inner = keys.shape[1]
    part = inner // 2
    start = pl.multiple_of(half[0] * inner, 128)
    number = sems.shape[0]
    step = inner // number
    copies = [
        pltpu.make_async_copy(
            w_out.at[pl.ds(pl.multiple_of(start + k * step, 64), step)],
            w_last.at[pl.ds(k * step, step)],
            sems.at[k],
        )
        for k in range(number)
    ]
    for copy in copies:
        copy.start()
    encoded[...] = settled[...]
    row_count = 2 * mine.shape[0] // mp
    allowed[...] = mask_rows(
        index, half, lengths, owners, answers, allowed.shape, patterns, mp, row_count
    )
    rows = jnp.concatenate([mine[...], theirs[...]], axis=0)
    size = min(256, part)
    for k, w_key in enumerate((first_key, last_key)):
        for c in range(part // size):
            keys[:, pl.ds(k * part + c * size, size)] = jnp.dot(
                rows, w_key[:, pl.ds(c * size, size)], preferred_element_type=F32
            ).astype(BF16)
    for k, w_value in enumerate((first_value, last_value)):
        for c in range(part // size):
            values[:, pl.ds(k * part + c * size, size)] = jnp.dot(
                rows, w_value[:, pl.ds(c * size, size)], preferred_element_type=F32
            ).astype(BF16)
    for copy in copies:
        copy.wait()


def project(places, tables, settled, mine, theirs, weights, w_attn_out, patterns, count, mp):
    rows, width = mine.shape
    inner = 2 * weights[0].shape[1]
    return pl.pallas_call(
        functools.partial(project_kernel, patterns=patterns, mp=mp),
        out_shape=(
            jax.ShapeDtypeStruct((2 * rows, inner), BF16),
            jax.ShapeDtypeStruct((2 * rows, inner), BF16),
            jax.ShapeDtypeStruct((inner, width), BF16),
            jax.ShapeDtypeStruct((count, 4 * rows), jnp.int32),
            jax.ShapeDtypeStruct(settled.shape, BF16),
        ),
        in_specs=[SMEM_SPEC] * 5 + [VMEM_SPEC] * 7 + [HBM_SPEC],
        out_specs=(VMEM_SPEC,) * 5,
        scratch_shapes=[pltpu.SemaphoreType.DMA((4,))],
        compiler_params=limit(46),
        cost_estimate=pl.CostEstimate(
            flops=8 * rows * width * inner, bytes_accessed=6 * width * inner, transcendentals=0
        ),
        name="project",
    )(*places, *tables, settled, mine, theirs, *weights, w_attn_out)


def attend_kernel(near_keys, near_values, mine, theirs, query, allowed, first_key, last_key, first_value, last_value, w_last, keep, give, context):
    rows, inner = near_keys.shape
    width = keep.shape[1]
    part = inner // 2
    size = min(256, part)
    late = jnp.concatenate([mine[...], theirs[...]], axis=0)
    near = allowed[:, :rows] > 0
    far = allowed[:, rows:] > 0
    for c in range(inner // size):
        columns = pl.ds(c * size, size)
        w_key = first_key if c * size < part else last_key
        w_value = first_value if c * size < part else last_value
        local = pl.ds(c * size % part, size)
        far_keys = jnp.dot(late, w_key[:, local], preferred_element_type=F32).astype(BF16)
        far_values = jnp.dot(late, w_value[:, local], preferred_element_type=F32).astype(BF16)
        keys = jnp.concatenate([near_keys[:, columns], far_keys], axis=0)
        values = jnp.concatenate([near_values[:, columns], far_values], axis=0)
        for h in range(size // DH):
            lanes = slice(h * DH, (h + 1) * DH)
            place = pl.ds(c * size + h * DH, DH)
            scores = lax.dot_general(
                query[:, place],
                keys[:, lanes],
                (((1,), (1,)), ((), ())),
                preferred_element_type=F32,
            ) * DH ** (-0.5)
            near_scores = jnp.where(near, scores[:, :rows], -1e30)
            far_scores = jnp.where(far, scores[:, rows:], -1e30)
            top = jnp.max(jnp.maximum(near_scores, far_scores), axis=1, keepdims=True)
            near_weights = jnp.where(near, jnp.exp(near_scores - top), 0.0)
            far_weights = jnp.where(far, jnp.exp(far_scores - top), 0.0)
            total = jnp.sum(near_weights + far_weights, axis=1, keepdims=True)
            weights = jnp.concatenate([near_weights, far_weights], axis=1).astype(BF16)
            summed = jnp.dot(weights, values[:, lanes], preferred_element_type=F32)
            context[:, place] = (summed * (1.0 / total)).astype(BF16)
    for c in range(width // 256):
        columns = pl.ds(c * 256, 256)
        result = jnp.dot(context[...], w_last[:, columns], preferred_element_type=F32)
        keep[:, columns] = result[: keep.shape[0]]
        give[:, columns] = result[keep.shape[0] :].astype(BF16)


def attend(near_keys, near_values, mine, theirs, query, allowed, weights, w_last):
    rows = near_keys.shape[0]
    width = mine.shape[1]
    count, inner = query.shape
    return pl.pallas_call(
        attend_kernel,
        out_shape=(
            jax.ShapeDtypeStruct((count // 2, width), F32),
            jax.ShapeDtypeStruct((count // 2, width), BF16),
        ),
        in_specs=[VMEM_SPEC] * 11,
        out_specs=(VMEM_SPEC, VMEM_SPEC),
        scratch_shapes=[pltpu.VMEM((count, inner), BF16)],
        compiler_params=limit(24),
        cost_estimate=pl.CostEstimate(
            flops=4 * rows * width * inner + 8 * count * rows * inner + 2 * count * inner * width,
            bytes_accessed=6 * width * inner,
            transcendentals=2 * count * rows * inner // DH,
        ),
        name="attend",
    )(near_keys, near_values, mine, theirs, query, allowed, *weights, w_last)


def finish_kernel(index, half, parts, states, piece):
    mp, small, _ = parts.shape
    start = index[0] * (2 * small) + half[0] * small
    row = lax.broadcasted_iota(jnp.int32, (small, states.shape[0]), 0)
    column = lax.broadcasted_iota(jnp.int32, (small, states.shape[0]), 1)
    pick = jnp.where(column == row + start, 1.0, 0.0).astype(BF16)
    total = jnp.dot(pick, states[...], preferred_element_type=F32)
    for k in range(mp):
        total = total + parts[k].astype(F32)
    piece[...] = total.astype(BF16)


def finish(index, half, parts, states):
    return pl.pallas_call(
        finish_kernel,
        out_shape=jax.ShapeDtypeStruct(parts.shape[1:], BF16),
        in_specs=[SMEM_SPEC, SMEM_SPEC, VMEM_SPEC, VMEM_SPEC],
        out_specs=VMEM_SPEC,
        compiler_params=limit(8),
        name="finish",
    )(index, half, parts, states)


def join_kernel(half, piece, other, out):
    first = jnp.where(half[0] == 0, piece[...].astype(F32), other[...].astype(F32))
    second = jnp.where(half[0] == 0, other[...].astype(F32), piece[...].astype(F32))
    out[...] = jnp.concatenate([first, second], axis=0).astype(BF16)


def join(half, piece, other):
    small, width = piece.shape
    return pl.pallas_call(
        join_kernel,
        out_shape=jax.ShapeDtypeStruct((2 * small, width), BF16),
        in_specs=[SMEM_SPEC, VMEM_SPEC, VMEM_SPEC],
        out_specs=VMEM_SPEC,
        compiler_params=limit(8),
        name="join",
    )(half, piece, other)


def per_device(
    tokens,
    enc_gain,
    w_in,
    w_out,
    final_gain,
    w_keyval,
    answer_states,
    dec_gain,
    w_query,
    w_attn_out,
    passage_lengths,
    passage_owner,
    answer_lengths,
):
    row_count = tokens.shape[0]
    width = tokens.shape[1]
    answer_count = answer_states.shape[0]
    mp = lax.axis_size("mp")
    psg = lax.axis_size("psg")
    mp_index = lax.axis_index("mp")
    psg_index = lax.axis_index("psg")
    heads = w_query.shape[1] // DH // psg
    inner = heads * DH

    half = jnp.reshape(psg_index, (1,)).astype(jnp.int32)
    index = jnp.reshape(mp_index, (1,)).astype(jnp.int32)
    held, got, patterns = spread_out(tokens, mp)
    first_in, last_in = stage(index, w_in, 1)
    first_out, last_out, held = stage_rows(index, w_out, held, enc_gain)
    partial_sums = feed(
        index, held, got, enc_gain, [first_in, last_in, first_out, last_out], patterns
    )
    parts = lax.all_to_all(partial_sums.reshape(mp, row_count, width), "mp", 0, 0)
    first_key, last_key, value = prepare(half, w_keyval, inner)

    runs = mp * row_count // 2
    small = answer_count // mp // psg
    settled, memory = settle(parts, tokens, final_gain)
    held, got, _ = spread_out(memory, mp)
    query, first_value, last_value = ask(half, answer_states, dec_gain, w_query, value, mp)
    held = held.reshape(runs, width)
    got = got.reshape(runs, width)
    held_theirs = swap_psg(held)
    weights = (first_key, last_key, first_value, last_value)
    near_keys, near_values, w_last, allowed, encoded = project(
        (index, half),
        (passage_lengths, passage_owner, answer_lengths),
        settled,
        held,
        held_theirs,
        weights,
        w_attn_out,
        patterns,
        answer_count,
        mp,
    )
    got_theirs = swap_psg(got)
    keep, give = attend(
        near_keys, near_values, got, got_theirs, query, allowed, weights, w_last
    )
    chip_sum = (keep + swap_psg(give).astype(F32)).astype(BF16).reshape(mp, small, width)
    answer_parts = lax.all_to_all(chip_sum, "mp", 0, 0)
    piece = finish(index, half, answer_parts, answer_states)
    return (encoded, join(half, piece, swap_psg(piece)))


def solution(mesh):
    placed = (
        P(("groups", "mp", "psg"), None),
        P(),
        P(None, "mp"),
        P("mp", None),
        P(),
        P(None, None, "mp"),
        P("groups", None),
        P(),
        P(None, "mp"),
        P("mp", None),
        P("groups"),
        P("groups"),
        P("groups"),
    )
    return jax.shard_map(
        per_device,
        mesh=mesh,
        in_specs=placed,
        out_specs=(P(("groups", "mp", "psg"), None), P(("groups", "mp"), None)),
        check_vma=False,
    )
```
